32 devices in a mesh: pole: 2 (over y), prow: 4 (over z), pcol: 4 (over x, core).
Axes of the slice: x: 2, y: 2, z: 4, core: 2. Of those that a mesh axis runs over, the one named last changes fastest.
Arguments:
- ainv_anc: bfloat16 [2, 4096, 2048], P(None, ('pole', 'prow'), 'pcol'), parts along dimension 1, may hold values from -6 to 6
- panel: bfloat16 [2, 8, 1024, 256], P(None, 'pole', ('pcol', 'prow')), parts along dimension 1, may hold values from -6 to 6
- u_inv: bfloat16 [2, 8, 256, 256], P(None, 'pole'), parts along dimension 1, may hold values from -0.01171875 to 0.01171875
- k_inv: float32 [2, 8, 256, 256], P(None, ('pole', 'pcol')), parts along dimension 1, may hold values from -6 to 6
- structure: int32 [4, 4], replicated, may hold values from -1 to 7, as said below
Outputs:
- sel_inv: float32 [2, 4096, 1024], P(None, ('pole', 'prow'), 'pcol'), parts along dimension 1
- diag_inv: float32 [2, 8, 256, 256], P(None, ('pole', 'pcol')), parts along dimension 1
The draws below stay inside these ranges and needn't reach their ends.
There are 2 independent parts, one for each index of `pole`. The reference program is written for one: setup_inputs(seed, part) draws one part's arguments, and reference() takes and returns one part's arrays. A program takes and returns all parts, laid end to end along the dimension named above; an argument that names none is the same for every part. Nothing has to cross between parts.
Inputs may be any that keep to these rules, and one draw needn't show every extreme that they name: `structure`: slots g * 1 to (g + 1) * 1 - 1 of row k hold distinct blocks of g * 2 to (g + 1) * 2 - 1 in rising order, followed by -1 for empty slots; each such group of each row holds at least one block, and for every g some row fills all 1 slots of group g.
All inputs are finite; a program needn't handle non-finite values.
Results may differ from the reference program's by a relative error of at most 0.005.
Values may be sent and summed in bfloat16 or wider, within the bound.
A program may use at most 128 MiB of HBM per device.

```python
import jax
import jax.numpy as jnp
from jax import lax

B = 256
NS = 8
GROUPB = 2
M = 4
GSLOT = 1
NK = 4


def draw_structure(key, part):
    groups = NS // GROUPB
    key_count = jax.random.fold_in(key, 11)
    key_full = jax.random.fold_in(key, 12)
    key_score = jax.random.fold_in(key, 13)
    counts = jax.random.randint(key_count, (NK, groups), 1, GSLOT + 1)
    full_row = jax.random.randint(key_full, (groups,), 0, NK)
    counts = jnp.where(jnp.arange(NK)[:, None] == full_row[None, :], GSLOT, counts)
    scores = jax.random.randint(key_score, (NK, groups, GROUPB), 0, 1 << 20) * GROUPB + jnp.arange(GROUPB)[None, None, :]
    order = jnp.argsort(scores, axis=-1)
    chosen = order[:, :, :GSLOT]
    slot_index = jnp.arange(GSLOT)
    live_slot = slot_index[None, None, :] < counts[:, :, None]
    keyed = jnp.where(live_slot, chosen, GROUPB + slot_index[None, None, :])
    ranked = jnp.sort(keyed, axis=-1)
    offset = jnp.arange(groups)[None, :, None] * GROUPB
    result = jnp.where(ranked < GROUPB, ranked + offset, -1)
    return result.reshape(NK, groups * GSLOT).astype(jnp.int32)


def block_levels(key, shape, cuts, least, high):
    gain = 1.0
    for position, parts in cuts:
        steps = jax.random.uniform(jax.random.fold_in(jax.random.fold_in(key, 6), position), (parts,), jnp.float32, least / len(cuts), high / len(cuts))
        gain = gain * jnp.repeat(jnp.exp(steps), shape[position] // parts).reshape((-1,) + (1,) * (len(shape) - 1 - position))
    return gain


def noise(stream_key, shape, deviation, reach, pieces=(), kind=jnp.bfloat16):
    gain = block_levels(stream_key, shape, pieces, -0.22, 0.18) if pieces else 1.0
    values = jax.random.normal(stream_key, shape, jnp.float32) * deviation * gain
    return jnp.minimum(jnp.maximum(values, -reach), reach).astype(kind)


def setup_inputs(seed: int = 0, part: int = 0) -> dict:
    splits = jax.random.split(jax.random.key(seed), 6)
    part_splits = jax.random.split(jax.random.fold_in(splits[5], part), 6)
    return {
        "ainv_anc": noise(part_splits[0], (2, NS * B, NS * B), 1.0, 6.0, ((1, 4), (2, 4))),
        "panel": noise(part_splits[1], (2, NK, M * B, B), 1.0, 6.0, ((2, 16),)),
        "u_inv": noise(part_splits[2], (2, NK, B, B), (B * B * M) ** -0.5, 0.01171875),
        "k_inv": noise(part_splits[3], (2, NK, B, B), 1.0, 6.0, ((1, 4),), jnp.float32),
        "structure": draw_structure(jax.random.fold_in(splits[5], 71), part),
    }


def complex_dot(left, right):
    real = jnp.dot(left[0], right[0], preferred_element_type=jnp.float32) - jnp.dot(left[1], right[1], preferred_element_type=jnp.float32)
    imag = jnp.dot(left[0], right[1], preferred_element_type=jnp.float32) + jnp.dot(left[1], right[0], preferred_element_type=jnp.float32)
    return jnp.stack([real, imag])


def complex_tdot(left, right):
    highest = lax.Precision.HIGHEST
    real = jnp.dot(left[0].T, right[0], precision=highest) - jnp.dot(left[1].T, right[1], precision=highest)
    imag = jnp.dot(left[0].T, right[1], precision=highest) + jnp.dot(left[1].T, right[0], precision=highest)
    return jnp.stack([real, imag])


def reference(ainv_anc, panel, u_inv, k_inv, structure):
    highest = lax.Precision.HIGHEST
    blocks = ainv_anc.reshape(2, NS, B, NS, B)

    def one_node(items):
        panel_k, slot_ids, u_block, k_block = items
        live_slots = slot_ids >= 0
        safe_ids = jnp.where(live_slots, slot_ids, 0).astype(jnp.int32)
        live_rows = jnp.repeat(live_slots, B)
        scaled = complex_dot(panel_k, u_block)
        scaled = jnp.where(live_rows[None, :, None], scaled, 0.0).astype(jnp.bfloat16)
        picked = jnp.take(jnp.take(blocks, safe_ids, axis=1), safe_ids, axis=3).reshape(2, M * B, M * B)
        result = -complex_dot(picked, scaled)
        result = jnp.where(live_rows[None, :, None], result, 0.0)
        diag_k = k_block - complex_tdot(scaled.astype(jnp.float32), result)
        onehot = (slot_ids[:, None] == jnp.arange(NS, dtype=jnp.int32)[None, :]).astype(jnp.float32)
        dense = jnp.einsum("mj,cmab->cjab", onehot, result.reshape(2, M, B, B), precision=highest)
        return dense, diag_k

    items = (jnp.moveaxis(panel, 1, 0), structure, jnp.moveaxis(u_inv, 1, 0), jnp.moveaxis(k_inv, 1, 0))
    dense, diag_inv = lax.map(one_node, items)
    sel_inv = jnp.transpose(dense, (1, 2, 3, 0, 4)).reshape(2, NS * B, NK * B)
    return sel_inv, jnp.moveaxis(diag_inv, 0, 1)
```

```python
import functools

import jax
import jax.numpy as jnp
from jax import lax
from jax.experimental import pallas as pl
from jax.experimental.pallas import tpu as pltpu
from jax.sharding import PartitionSpec as P

BF16 = jnp.bfloat16
F32 = jnp.float32


def cdot(left, right, dims=(((1,), (0,)), ((), ()))):
    def single(x, y):
        return lax.dot_general(x, y, dims, preferred_element_type=F32)

    real = single(left[0], right[0]) - single(left[1], right[1])
    imag = single(left[0], right[1]) + single(left[1], right[0])
    return real, imag


def remote(src, dst, send_sem, recv_sem, where):
    return pltpu.make_async_remote_copy(
        src_ref=src,
        dst_ref=dst,
        send_sem=send_sem,
        recv_sem=recv_sem,
        device_id=where,
        device_id_type=pl.DeviceIdType.MESH,
    )


def kernel(
    n_rows, n_cols, bands, a_hbm, panel_hbm, u_hbm, k_hbm, table_hbm, sel_out, diag_out,
    table, av, pv, uv, pr, gather, pick_out, pick_in, acc, kv, q_out, q_in, tot, q_own,
    local_sem, p_send, p_recv, a_send, a_recv, g_send, g_recv, q_send, q_recv, t_send, t_recv,
):
    row = lax.axis_index("prow")
    col = lax.axis_index("pcol")
    width = u_hbm.shape[-1]
    pairs = n_cols // 2
    row_blocks = a_hbm.shape[1] // width
    col_blocks = a_hbm.shape[2] // width
    half_width = width // 2
    band_rows = width // bands
    mate = row + 1 - 2 * (row % 2)
    is_end = (row == 0) | (row == n_rows - 1)
    end = jnp.where(is_end, row, mate)
    inner = jnp.where(is_end, mate, row)
    over = n_rows - 1 - inner
    far = n_rows - 1 - end

    def peer(unit):
        return ((col // 2 + unit // 2) % pairs) * 2 + (col + unit) % 2

    copy_p = pltpu.make_async_copy(panel_hbm, pv, local_sem.at[0])
    copy_u = pltpu.make_async_copy(u_hbm.at[:, col], uv, local_sem.at[1])
    copy_t = pltpu.make_async_copy(table_hbm, table, local_sem.at[2])
    copy_a = pltpu.make_async_copy(a_hbm, av, local_sem.at[3])
    copy_k = pltpu.make_async_copy(k_hbm, kv, local_sem.at[4])
    copy_p.start()
    copy_u.start()
    copy_t.start()

    barrier = pltpu.get_barrier_semaphore()

    def greet(axis, there):
        pl.semaphore_signal(barrier, inc=1, device_id={axis: there}, device_id_type=pl.DeviceIdType.MESH)

    for unit in range(1, n_cols):
        greet("pcol", peer(unit))
    greet("prow", mate)
    greet("prow", jnp.where(is_end, over, far))

    @pl.when(jnp.logical_not(is_end))
    def _():
        greet("prow", over)

    pl.semaphore_wait(barrier, n_cols + 2 - is_end.astype(jnp.int32))

    def panel_copy(unit, source):
        return remote(
            pv.at[:, peer(unit)], pr.at[source], p_send.at[unit], p_recv.at[source], {"pcol": peer(unit)}
        )

    def pick_copy(unit, source):
        return remote(
            pick_out.at[unit], pick_in.at[source], a_send.at[unit], a_recv.at[source], {"pcol": peer(unit)}
        )

    def chunk_copy(unit, chunk, kind, there):
        block = gather.at[unit, :, chunk]
        return remote(block, block, g_send.at[kind], g_recv.at[unit, chunk], {"prow": there})

    def arrived(unit, chunk):
        chunk_copy(unit, chunk, 0, mate).wait_recv()

    copy_p.wait()
    copy_a.start()
    for unit in range(1, n_cols):
        panel_copy(unit, col).start()
    copy_k.start()
    copy_u.wait()
    copy_t.wait()

    def scale(unit):
        slot = peer(unit)
        if unit == 0:
            left = (pv[0, col], pv[1, col])
        else:
            panel_copy(unit, slot).wait_recv()
            left = (pr[slot, 0], pr[slot, 1])
        real, imag = cdot(left, (uv[0], uv[1]))
        live = (jnp.full((1, width), table[col, slot]) >= 0).astype(F32)
        gather[unit, 0, row] = (real * live).astype(BF16)
        gather[unit, 1, row] = (imag * live).astype(BF16)
        chunk_copy(unit, row, 0, over).start()
        chunk_copy(unit, row, 1, mate).start()

    def pick(unit):
        node = peer(unit)
        top = jnp.full((1, width), table[node, row]) - row * row_blocks
        side = jnp.full((1, width), table[node, col]) - col * col_blocks
        for plane in range(2):
            total = None
            for i in range(row_blocks):
                for j in range(col_blocks):
                    keep = ((top == i) & (side == j)).astype(F32).astype(BF16)
                    block = av[plane, i * width : (i + 1) * width, j * width : (j + 1) * width] * keep
                    total = block if total is None else total + block
            pick_out[unit, plane] = total

    scale(0)
    scale(1)
    copy_a.wait()
    for unit in list(range(2, n_cols)) + [1]:
        pick(unit)
        pick_copy(unit, col).start()
    pick(0)
    late = range(2, n_cols)

    def relay(unit, chunk, kind):
        arrived(unit, chunk)
        chunk_copy(unit, chunk, kind, end).start()

    @pl.when(is_end)
    def _():
        for unit in late:
            scale(unit)

    @pl.when(jnp.logical_not(is_end))
    def _():
        scale(2)
        relay(0, over, 2)
        scale(3)
        relay(1, over, 2)
        relay(0, far, 3)
        relay(1, far, 3)
        for unit in late:
            relay(unit, over, 2)
            relay(unit, far, 3)

    def multiply(unit):
        slot = peer(unit)

        @pl.when(is_end)
        def _():
            arrived(unit, over)
            arrived(unit, far)

        arrived(unit, mate)
        if unit == 0:
            left = (pick_out[0, 0], pick_out[0, 1])
        else:
            pick_copy(unit, slot).wait_recv()
            left = (pick_in[slot, 0], pick_in[slot, 1])
        right = tuple(gather[unit, plane].reshape(width, width) for plane in range(2))
        real, imag = cdot(left, right)
        if unit == 0:
            acc[0] = real
            acc[1] = imag
        else:
            acc[0] += real
            acc[1] += imag

    for unit in range(n_cols):
        multiply(unit)
    live = (jnp.full((1, width), table[col, row]) >= 0).astype(F32)
    unit_here = ((row // 2 - col // 2 + pairs) % pairs) * 2 + (row + col) % 2
    z = tuple(gather[unit_here, plane].reshape(width, width) for plane in range(2))
    r = (acc[0] * live, acc[1] * live)
    low = (r[0].astype(BF16), r[1].astype(BF16))
    named = jnp.full((1, width), table[col, row]) - row * row_blocks

    def owner(half):
        return n_rows // 2 - 1 + half

    def quad_copy(half, band, source):
        return remote(
            q_out.at[half, band], q_in.at[source, band], q_send.at[0], q_recv.at[source, band],
            {"prow": owner(half)},
        )

    def total_copy(half, band, kind, there):
        block = tot.at[half, band]
        return remote(block, block, t_send.at[kind], t_recv.at[half, band], {"prow": there})

    for half in range(2):
        columns = slice(half * half_width, (half + 1) * half_width)
        quad = cdot(z, (low[0][:, columns], low[1][:, columns]), (((0,), (0,)), ((), ())))
        for plane in range(2):
            for band in range(bands):
                block = quad[plane][band * band_rows : (band + 1) * band_rows]
                q_out[half, band, plane] = block.astype(BF16)

                @pl.when(row == owner(half))
                def _():
                    q_own[band, plane] = block

    for band in range(bands):
        for half in range(2):
            @pl.when(row != owner(half))
            def _():
                quad_copy(half, band, row).start()

    for i in range(row_blocks):
        keep = -(named == i).astype(F32)
        for plane in range(2):
            sel_out[plane, i * width : (i + 1) * width, :] = r[plane] * keep
    copy_k.wait()

    def finish(half, band):
        rows = slice(band * band_rows, (band + 1) * band_rows)
        columns = pl.ds(pl.multiple_of(half * half_width, half_width), half_width)
        for plane in range(2):
            diag_out[plane, 0, rows, columns] = kv[plane, 0, rows, columns] + tot[half, band, plane].astype(F32)

    mine = inner - (n_rows // 2 - 1)

    @pl.when(jnp.logical_not(is_end))
    def _():
        for band in range(bands):
            for source in (over, end, far):
                quad_copy(mine, band, source).wait_recv()
            for plane in range(2):
                total = q_own[band, plane]
                for source in (over, end, far):
                    total = total + q_in[source, band, plane].astype(F32)
                tot[mine, band, plane] = total.astype(BF16)
            total_copy(mine, band, 0, far).start()
            total_copy(mine, band, 1, end).start()
            total_copy(mine, band, 2, over).start()
        for band in range(bands):
            finish(mine, band)

    @pl.when(is_end)
    def _():
        for band in range(bands):
            total_copy(mine, band, 0, far).wait_recv()
            finish(mine, band)

    for band in range(bands):
        total_copy(1 - mine, band, 0, far).wait_recv()
        finish(1 - mine, band)

    for unit in range(1, n_cols):
        panel_copy(unit, col).wait_send()
        pick_copy(unit, col).wait_send()

    def drain(view, sem):
        remote(view, view, sem, sem, {"prow": mate}).wait_send()

    drain(gather.at[0], g_send.at[0])
    drain(gather.at[0], g_send.at[1])

    @pl.when(is_end)
    def _():
        drain(q_out, q_send.at[0])

    @pl.when(jnp.logical_not(is_end))
    def _():
        drain(gather.at[0], g_send.at[2])
        drain(gather.at[0], g_send.at[3])
        drain(q_out.at[0], q_send.at[0])
        for kind in range(3):
            drain(tot.at[0], t_send.at[kind])


def place(sel, diag, sel_out, diag_out, out_sem):
    copies = [
        pltpu.make_async_copy(sel, sel_out, out_sem.at[0]),
        pltpu.make_async_copy(diag, diag_out, out_sem.at[1]),
    ]
    for copy in copies:
        copy.start()
    for copy in copies:
        copy.wait()


def compact(ainv_anc, panel, u_inv, k_inv, structure):
    n_rows, n_cols = lax.axis_size("prow"), lax.axis_size("pcol")
    width, part = u_inv.shape[-1], panel.shape[2]
    row_blocks = ainv_anc.shape[1] // width
    bands = n_rows
    hbm = pl.BlockSpec(memory_space=pltpu.HBM)
    vmem = pl.BlockSpec(memory_space=pltpu.VMEM)
    dma = pltpu.SemaphoreType.DMA
    shapes = (
        jax.ShapeDtypeStruct((2, row_blocks * width, width), F32),
        jax.ShapeDtypeStruct(k_inv.shape, F32),
    )
    piece = (2, width // bands, width // 2)
    results = pl.pallas_call(
        functools.partial(kernel, n_rows, n_cols, bands),
        out_shape=tuple(pltpu.VMEM(s.shape, s.dtype) for s in shapes),
        in_specs=[hbm, hbm, hbm, hbm, hbm],
        out_specs=(vmem, vmem),
        scratch_shapes=[
            pltpu.SMEM(structure.shape, jnp.int32),
            pltpu.VMEM(ainv_anc.shape, BF16),
            pltpu.VMEM(panel.shape, BF16),
            pltpu.VMEM((2, width, width), BF16),
            pltpu.VMEM((n_cols, 2, part, width), BF16),
            pltpu.VMEM((n_cols, 2, n_rows, part, width), BF16),
            pltpu.VMEM((n_cols, 2, width, width), BF16),
            pltpu.VMEM((n_cols, 2, width, width), BF16),
            pltpu.VMEM((2, width, width), F32),
            pltpu.VMEM(k_inv.shape, F32),
            pltpu.VMEM((2, bands) + piece, BF16),
            pltpu.VMEM((n_rows, bands) + piece, BF16),
            pltpu.VMEM((2, bands) + piece, BF16),
            pltpu.VMEM((bands,) + piece, F32),
            dma((5,)),
            dma((n_cols,)),
            dma((n_cols,)),
            dma((n_cols,)),
            dma((n_cols,)),
            dma((4,)),
            dma((n_cols, n_rows)),
            dma((1,)),
            dma((n_rows, bands)),
            dma((3,)),
            dma((2, bands)),
        ],
        compiler_params=pltpu.CompilerParams(
            collective_id=0, has_side_effects=True
        ),
    )(ainv_anc, panel, u_inv, k_inv, structure)
    return pl.pallas_call(
        place,
        out_shape=shapes,
        in_specs=[vmem, vmem],
        out_specs=(hbm, hbm),
        scratch_shapes=[dma((2,))],
    )(*[pltpu.with_memory_space_constraint(x, pltpu.VMEM) for x in results])


def complex_quad(z_part, s_part):
    highest = lax.Precision.HIGHEST

    def single(left, right):
        return jnp.einsum("kra,rkb->kab", left, right, precision=highest)

    real = single(z_part[0], s_part[0]) - single(z_part[1], s_part[1])
    imag = single(z_part[0], s_part[1]) + single(z_part[1], s_part[0])
    return jnp.stack([real, imag])


def local(ainv_anc, panel, u_inv, k_inv, structure):
    block_width = u_inv.shape[-1]
    cols = lax.axis_size("pcol")
    if (
        structure.shape[1] == cols
        and lax.axis_size("prow") == cols
        and ainv_anc.shape[1] == ainv_anc.shape[2]
        and u_inv.shape[1] == cols
        and cols // 2 == 2
        and cols % 2 == 0
    ):
        return compact(ainv_anc, panel, u_inv, k_inv, structure)
    total_k = u_inv.shape[1]
    own_k = k_inv.shape[1]
    n_cols = lax.axis_size("pcol")
    row_here = lax.axis_index("prow")
    col_here = lax.axis_index("pcol")
    row_blocks = ainv_anc.shape[1] // block_width
    group_blocks = ainv_anc.shape[2] // block_width
    group_slots = structure.shape[1] // n_cols
    rows_all = row_blocks * block_width
    col_struct = lax.dynamic_slice_in_dim(structure, col_here * group_slots, group_slots, 1)
    slot_live = col_struct >= 0
    slot_pos = col_struct - col_here * group_blocks
    first_block = row_here * row_blocks
    target = first_block + jnp.arange(row_blocks, dtype=jnp.int32)
    rows_in = lax.all_gather(panel, "prow", axis=2, tiled=True)

    def single(left, right):
        return jnp.einsum("knb,kbc->knc", left, right, preferred_element_type=jnp.float32)

    real = single(rows_in[0], u_inv[0]) - single(rows_in[1], u_inv[1])
    imag = single(rows_in[0], u_inv[1]) + single(rows_in[1], u_inv[0])
    placed = jnp.stack([real, imag]).astype(jnp.bfloat16)
    placed = placed.reshape(2, total_k, group_slots, block_width, block_width)
    placed = jnp.where(slot_live[None, :, :, None, None], placed, jnp.zeros((), jnp.bfloat16))
    block_ids = jnp.arange(group_blocks, dtype=jnp.int32)
    pick_table = (slot_pos[:, :, None] == block_ids[None, None, :]).astype(jnp.bfloat16)
    ainv_blocks = ainv_anc.reshape(2, rows_all, group_blocks, block_width)

    def one_node(items):
        table_k, rows_k = items
        picked = jnp.einsum(
            "sg,cigw->cisw", table_k, ainv_blocks, preferred_element_type=jnp.float32
        )
        picked = picked.astype(jnp.bfloat16).reshape(2, rows_all, group_slots * block_width)
        right = rows_k.reshape(2, group_slots * block_width, block_width)
        real = jnp.dot(picked[0], right[0], preferred_element_type=jnp.float32) - jnp.dot(
            picked[1], right[1], preferred_element_type=jnp.float32
        )
        imag = jnp.dot(picked[0], right[1], preferred_element_type=jnp.float32) + jnp.dot(
            picked[1], right[0], preferred_element_type=jnp.float32
        )
        return jnp.stack([real, imag])

    per_node = lax.map(one_node, (pick_table, jnp.moveaxis(placed, 1, 0)))
    partial_value = jnp.transpose(per_node, (1, 2, 0, 3))
    row_table = (col_struct[:, None, :] == target[None, :, None]).astype(jnp.bfloat16)
    z_rows = jnp.einsum("kts,ckswb->cktwb", row_table, placed, preferred_element_type=jnp.float32)
    z_rows = z_rows.astype(jnp.bfloat16).reshape(2, total_k, rows_all, block_width)
    summed = lax.psum_scatter(
        partial_value.reshape(2, rows_all, total_k * block_width),
        "pcol",
        scatter_dimension=2,
        tiled=True,
    )
    own_struct = lax.dynamic_slice_in_dim(structure, col_here * own_k, own_k, 0)
    member = jnp.any(own_struct[:, :, None] == target[None, None, :], axis=1)
    selected = -summed.reshape(2, row_blocks, block_width, own_k, block_width)
    selected = jnp.where(member.T[None, :, None, :, None], selected, 0.0)
    sel_inv = selected.reshape(2, rows_all, own_k * block_width)
    received = lax.all_to_all(z_rows, "pcol", split_axis=1, concat_axis=1, tiled=True)
    z_own = (
        received.astype(jnp.float32).reshape(2, n_cols, own_k, rows_all, block_width).sum(axis=1)
    )
    quad_term = complex_quad(z_own, selected.reshape(2, rows_all, own_k, block_width))
    total_sum = lax.psum(quad_term, "prow")
    diag_inv = k_inv - total_sum
    return (sel_inv, diag_inv)


def solution(mesh):
    placed = (
        P(None, ("pole", "prow"), "pcol"),
        P(None, "pole", ("pcol", "prow"), None),
        P(None, "pole", None, None),
        P(None, ("pole", "pcol"), None, None),
        P(),
    )
    return jax.shard_map(
        local,
        mesh=mesh,
        in_specs=placed,
        out_specs=(P(None, ("pole", "prow"), "pcol"), P(None, ("pole", "pcol"), None, None)),
        check_vma=False,
    )
```

```python
import functools

import jax
import jax.numpy as jnp
from jax import lax
from jax.experimental import pallas as pl
from jax.experimental.pallas import tpu as pltpu
from jax.sharding import PartitionSpec as P

BF16 = jnp.bfloat16
F32 = jnp.float32
scope = jax.named_scope


def cdot(left, right, dims=(((1,), (0,)), ((), ()))):
    def single(x, y):
        return lax.dot_general(x, y, dims, preferred_element_type=F32)

    real = single(left[0], right[0]) - single(left[1], right[1])
    imag = single(left[0], right[1]) + single(left[1], right[0])
    return real, imag


def remote(src, dst, send_sem, recv_sem, where):
    return pltpu.make_async_remote_copy(
        src_ref=src,
        dst_ref=dst,
        send_sem=send_sem,
        recv_sem=recv_sem,
        device_id=where,
        device_id_type=pl.DeviceIdType.MESH,
    )


def kernel(
    n_rows, n_cols, a_hbm, panel_hbm, u_hbm, k_hbm, table_hbm, sel_out, diag_out,
    table, av, pv, uv, pr, gather, pick_out, picks, acc, kv, q_own, q_out, q_in, tot,
    local_sem, p_send, p_recv, a_send, a_recv, g_send, g_recv, q_send, q_recv, t_send, t_recv,
):
    row = lax.axis_index("prow")
    col = lax.axis_index("pcol")
    width = u_hbm.shape[-1]
    pairs = n_cols // 2
    row_blocks = a_hbm.shape[1] // width
    col_blocks = a_hbm.shape[2] // width
    lanes = width // 2
    share = q_in.shape[2]
    band_rows = q_in.shape[3]
    bands = q_out.shape[1]
    mate = row + 1 - 2 * (row % 2)
    is_end = (row == 0) | (row == n_rows - 1)
    is_inner = jnp.logical_not(is_end)
    end = jnp.where(is_end, row, mate)
    inner = jnp.where(is_end, mate, row)
    over = n_rows - 1 - inner
    far = n_rows - 1 - end

    def peer(unit):
        return ((col // 2 + unit // 2) % pairs) * 2 + (col + unit) % 2

    def unit_of(slot):
        return ((slot // 2 - col // 2 + pairs) % pairs) * 2 + (slot + col) % 2

    copy_p = pltpu.make_async_copy(panel_hbm, pv, local_sem.at[0])
    copy_u = pltpu.make_async_copy(u_hbm.at[:, col], uv, local_sem.at[1])
    copy_t = pltpu.make_async_copy(table_hbm, table, local_sem.at[2])
    copy_a = pltpu.make_async_copy(a_hbm, av, local_sem.at[3])
    copy_k = pltpu.make_async_copy(k_hbm, kv, local_sem.at[4])
    copy_p.start()
    copy_u.start()
    copy_t.start()

    barrier = pltpu.get_barrier_semaphore()

    def greet(axis, there):
        pl.semaphore_signal(barrier, inc=1, device_id={axis: there}, device_id_type=pl.DeviceIdType.MESH)

    for unit in range(1, n_cols):
        greet("pcol", peer(unit))
    greet("prow", mate)
    greet("prow", jnp.where(is_end, over, far))

    @pl.when(is_inner)
    def _():
        greet("prow", over)

    with scope("barrier"):
        pl.semaphore_wait(barrier, n_cols + 2 - is_end.astype(jnp.int32))

    def panel_copy(unit, source):
        return remote(
            pv.at[:, peer(unit)], pr.at[source], p_send.at[unit], p_recv.at[source], {"pcol": peer(unit)}
        )

    def pick_copy(unit, source):
        return remote(
            pick_out.at[unit - 1], picks.at[source], a_send.at[unit], a_recv.at[source], {"pcol": peer(unit)}
        )

    def chunk_copy(half, unit, chunk, kind, there):
        block = gather.at[half, unit, chunk]
        return remote(block, block, g_send.at[kind], g_recv.at[half, unit, chunk], {"prow": there})

    def arrived(half, unit, chunk):
        chunk_copy(half, unit, chunk, 0, mate).wait_recv()

    with scope("copy_p"):
        copy_p.wait()
    copy_a.start()
    for unit in range(1, n_cols):
        panel_copy(unit, col).start()
    copy_k.start()
    with scope("copy_u"):
        copy_u.wait()
        copy_t.wait()

    def scale(unit):
        slot = peer(unit)
        if unit == 0:
            left = (pv[0, col], pv[1, col])
        else:
            panel_copy(unit, slot).wait_recv()
            left = (pr[slot, 0], pr[slot, 1])
        value = cdot(left, (uv[0], uv[1]))
        live = (jnp.full((1, lanes), table[col, slot]) >= 0).astype(F32)
        for half in range(2):
            for plane in range(2):
                block = value[plane][:, half * lanes : (half + 1) * lanes]
                gather[half, unit, row, :, plane * lanes : (plane + 1) * lanes] = (block * live).astype(BF16)

    def spread(half, unit):
        chunk_copy(half, unit, row, 0, over).start()
        chunk_copy(half, unit, row, 1, mate).start()

    def pick(unit):
        node = peer(unit)
        top = jnp.full((1, width), table[node, row]) - row * row_blocks
        side = jnp.full((1, width), table[node, col]) - col * col_blocks
        for plane in range(2):
            total = None
            for i in range(row_blocks):
                for j in range(col_blocks):
                    keep = ((top == i) & (side == j)).astype(F32).astype(BF16)
                    block = av[plane, i * width : (i + 1) * width, j * width : (j + 1) * width] * keep
                    total = block if total is None else total + block
            if unit == 0:
                picks[col, plane] = total
            else:
                pick_out[unit - 1, plane] = total

    for unit in range(2):
        with scope(f"scale{unit}"):
            scale(unit)
        for half in range(2):
            spread(half, unit)
    with scope("copy_a"):
        copy_a.wait()
    for unit in list(range(2, n_cols)) + [1]:
        with scope(f"pick{unit}"):
            pick(unit)
        pick_copy(unit, col).start()
    pick(0)
    late = range(2, n_cols)

    def relay(half, unit, chunk, kind):
        arrived(half, unit, chunk)
        chunk_copy(half, unit, chunk, kind, end).start()

    @pl.when(is_end)
    def _():
        for unit in late:
            with scope(f"scale{unit}"):
                scale(unit)
            spread(0, unit)
        for unit in late:
            spread(1, unit)

    @pl.when(is_inner)
    def _():
        with scope("scale2"):
            scale(2)
        spread(0, 2)
        with scope("relay_0o"):
            relay(0, 0, over, 2)
        with scope("relay_1o"):
            relay(0, 1, over, 2)
        with scope("scale3"):
            scale(3)
        spread(0, 3)
        with scope("relay_01f"):
            relay(0, 0, far, 3)
            relay(0, 1, far, 3)
        for unit in late:
            spread(1, unit)
        for unit in late:
            with scope(f"relay_{unit}o"):
                relay(0, unit, over, 2)
            with scope(f"relay_{unit}f"):
                relay(0, unit, far, 3)
        for i in range(n_cols):
            unit = (unit_of(end) + i) % n_cols
            with scope(f"relay_h1_{i}o"):
                relay(1, unit, over, 2)
            with scope(f"relay_h1_{i}f"):
                relay(1, unit, far, 3)

    def ready(half, unit):
        @pl.when(is_end)
        def _():
            arrived(half, unit, over)
            arrived(half, unit, far)

        arrived(half, unit, mate)

    def multiply(half, unit, first):
        right = gather[half, unit].reshape(width, width)
        slot = peer(unit)
        for plane in range(2):
            value = jnp.dot(picks[slot, plane], right, preferred_element_type=F32)
            if first:
                acc[plane] = value
            else:
                acc[plane] += value

    home = unit_of(row)
    live = (jnp.full((1, width), table[col, row]) >= 0).astype(F32)
    named = jnp.full((1, lanes), table[col, row]) - row * row_blocks

    def owner(band):
        return n_rows // 2 - 1 + band // share

    def quad_copy(half, there, part, source):
        band = (there - (n_rows // 2 - 1)) * share + part
        return remote(
            q_out.at[half, band], q_in.at[source, half, part], q_send.at[0], q_recv.at[source, half, part],
            {"prow": there},
        )

    def quad(half):
        real = acc[0, :, :lanes] - acc[1, :, lanes:]
        imag = acc[0, :, lanes:] + acc[1, :, :lanes]
        value = jnp.concatenate([real, imag], axis=1) * live
        low = value.astype(BF16)
        for top in range(2):
            z = gather[top, home].reshape(width, width)
            product = lax.dot_general(z, low, (((0,), (0,)), ((), ())), preferred_element_type=F32)
            real = product[:lanes, :lanes] - product[lanes:, lanes:]
            imag = product[:lanes, lanes:] + product[lanes:, :lanes]
            whole = jnp.concatenate([real, imag], axis=1)
            for i in range(bands // 2):
                block = whole[i * band_rows : (i + 1) * band_rows]
                band = top * (bands // 2) + i
                q_out[half, band] = block.astype(BF16)

                @pl.when(row == owner(band))
                def _():
                    q_own[half, band % share] = block

        for part in range(share):
            quad_copy(half, over, part, row).start()

        @pl.when(is_end)
        def _():
            for part in range(share):
                quad_copy(half, mate, part, row).start()

        columns = slice(half * lanes, (half + 1) * lanes)
        for i in range(row_blocks):
            keep = -(named == i).astype(F32)
            for plane in range(2):
                block = value[:, plane * lanes : (plane + 1) * lanes]
                sel_out[plane, i * width : (i + 1) * width, columns] = block * keep

    for unit in range(n_cols):
        with scope(f"ready_h0_{unit}"):
            ready(0, unit)
        with scope(f"wpick_{unit}"):
            if unit > 0:
                pick_copy(unit, peer(unit)).wait_recv()
        multiply(0, unit, unit == 0)
    with scope("ready_home"):
        ready(1, home)
    with scope("quad0"):
        quad(0)
    for i in range(n_cols):
        unit = (home + i) % n_cols
        if i > 0:
            with scope(f"ready_h1_{i}"):
                ready(1, unit)
        multiply(1, unit, i == 0)
    with scope("quad1"):
        quad(1)
    copy_k.wait()

    def total_copy(half, band, kind, there):
        block = tot.at[half, band]
        return remote(block, block, t_send.at[kind], t_recv.at[half, band], {"prow": there})

    def finish(half, band):
        rows = pl.ds(pl.multiple_of(band * band_rows, band_rows), band_rows)
        columns = slice(half * lanes, (half + 1) * lanes)
        for plane in range(2):
            block = tot[half, band, :, plane * lanes : (plane + 1) * lanes].astype(F32)
            diag_out[plane, 0, rows, columns] = kv[plane, 0, rows, columns] + block

    near_band = (inner - (n_rows // 2 - 1)) * share
    over_band = (over - (n_rows // 2 - 1)) * share

    @pl.when(is_inner)
    def _():
        for half in range(2):
            for part in range(share):
                with scope(f"wq{half}_{part}"):
                    for source in (over, end, far):
                        quad_copy(half, row, part, source).wait_recv()
                total = q_own[half, part]
                for source in (over, end, far):
                    total = total + q_in[source, half, part].astype(F32)
                tot[half, near_band + part] = total.astype(BF16)
                total_copy(half, near_band + part, 0, far).start()
                total_copy(half, near_band + part, 1, end).start()
                total_copy(half, near_band + part, 2, over).start()
        for half in range(2):
            for part in range(share):
                finish(half, near_band + part)

    for half in range(2):
        @pl.when(is_end)
        def _():
            for part in range(share):
                with scope(f"wt_near{half}_{part}"):
                    total_copy(half, near_band + part, 0, mate).wait_recv()
                finish(half, near_band + part)

        for part in range(share):
            with scope(f"wt_over{half}_{part}"):
                total_copy(half, over_band + part, 0, mate).wait_recv()
            finish(half, over_band + part)

    for unit in range(1, n_cols):
        panel_copy(unit, col).wait_send()
        pick_copy(unit, col).wait_send()

    def drain(view, sem):
        remote(view, view, sem, sem, {"prow": mate}).wait_send()

    drain(gather.at[0, 0:2], g_send.at[0])
    drain(gather.at[0, 0:2], g_send.at[1])

    @pl.when(is_end)
    def _():
        drain(q_out, q_send.at[0])

    @pl.when(is_inner)
    def _():
        drain(gather.at[0, 0:2], g_send.at[2])
        drain(gather.at[0, 0:2], g_send.at[3])
        drain(q_out.at[0], q_send.at[0])
        for kind in range(3):
            drain(tot.at[0], t_send.at[kind])


def place(sel, diag, sel_out, diag_out, out_sem):
    copies = [
        pltpu.make_async_copy(sel, sel_out, out_sem.at[0]),
        pltpu.make_async_copy(diag, diag_out, out_sem.at[1]),
    ]
    for copy in copies:
        copy.start()
    for copy in copies:
        copy.wait()


def compact(ainv_anc, panel, u_inv, k_inv, structure):
    n_rows, n_cols = lax.axis_size("prow"), lax.axis_size("pcol")
    width, part = u_inv.shape[-1], panel.shape[2]
    row_blocks = ainv_anc.shape[1] // width
    bands = n_rows
    share = bands // 2
    hbm = pl.BlockSpec(memory_space=pltpu.HBM)
    vmem = pl.BlockSpec(memory_space=pltpu.VMEM)
    dma = pltpu.SemaphoreType.DMA
    shapes = (
        jax.ShapeDtypeStruct((2, row_blocks * width, width), F32),
        jax.ShapeDtypeStruct(k_inv.shape, F32),
    )
    piece = (width // bands, width)
    results = pl.pallas_call(
        functools.partial(kernel, n_rows, n_cols),
        out_shape=tuple(pltpu.VMEM(s.shape, s.dtype) for s in shapes),
        in_specs=[hbm, hbm, hbm, hbm, hbm],
        out_specs=(vmem, vmem),
        scratch_shapes=[
            pltpu.SMEM(structure.shape, jnp.int32),
            pltpu.VMEM(ainv_anc.shape, BF16),
            pltpu.VMEM(panel.shape, BF16),
            pltpu.VMEM((2, width, width), BF16),
            pltpu.VMEM((n_cols, 2, part, width), BF16),
            pltpu.VMEM((2, n_cols, n_rows, part, width), BF16),
            pltpu.VMEM((n_cols - 1, 2, width, width), BF16),
            pltpu.VMEM((n_cols, 2, width, width), BF16),
            pltpu.VMEM((2, width, width), F32),
            pltpu.VMEM(k_inv.shape, F32),
            pltpu.VMEM((2, share) + piece, F32),
            pltpu.VMEM((2, bands) + piece, BF16),
            pltpu.VMEM((n_rows, 2, share) + piece, BF16),
            pltpu.VMEM((2, bands) + piece, BF16),
            dma((5,)),
            dma((n_cols,)),
            dma((n_cols,)),
            dma((n_cols,)),
            dma((n_cols,)),
            dma((4,)),
            dma((2, n_cols, n_rows)),
            dma((1,)),
            dma((n_rows, 2, share)),
            dma((3,)),
            dma((2, bands)),
        ],
        compiler_params=pltpu.CompilerParams(
            collective_id=0, has_side_effects=True
        ),
    )(ainv_anc, panel, u_inv, k_inv, structure)
    return pl.pallas_call(
        place,
        out_shape=shapes,
        in_specs=[vmem, vmem],
        out_specs=(hbm, hbm),
        scratch_shapes=[dma((2,))],
    )(*[pltpu.with_memory_space_constraint(x, pltpu.VMEM) for x in results])


def complex_quad(z_part, s_part):
    highest = lax.Precision.HIGHEST

    def single(left, right):
        return jnp.einsum("kra,rkb->kab", left, right, precision=highest)

    real = single(z_part[0], s_part[0]) - single(z_part[1], s_part[1])
    imag = single(z_part[0], s_part[1]) + single(z_part[1], s_part[0])
    return jnp.stack([real, imag])


def local(ainv_anc, panel, u_inv, k_inv, structure):
    block_width = u_inv.shape[-1]
    cols = lax.axis_size("pcol")
    if (
        structure.shape[1] == cols
        and lax.axis_size("prow") == cols
        and ainv_anc.shape[1] == ainv_anc.shape[2]
        and u_inv.shape[1] == cols
        and cols // 2 == 2
        and cols % 2 == 0
    ):
        return compact(ainv_anc, panel, u_inv, k_inv, structure)
    total_k = u_inv.shape[1]
    own_k = k_inv.shape[1]
    n_cols = lax.axis_size("pcol")
    row_here = lax.axis_index("prow")
    col_here = lax.axis_index("pcol")
    row_blocks = ainv_anc.shape[1] // block_width
    group_blocks = ainv_anc.shape[2] // block_width
    group_slots = structure.shape[1] // n_cols
    rows_all = row_blocks * block_width
    col_struct = lax.dynamic_slice_in_dim(structure, col_here * group_slots, group_slots, 1)
    slot_live = col_struct >= 0
    slot_pos = col_struct - col_here * group_blocks
    first_block = row_here * row_blocks
    target = first_block + jnp.arange(row_blocks, dtype=jnp.int32)
    rows_in = lax.all_gather(panel, "prow", axis=2, tiled=True)

    def single(left, right):
        return jnp.einsum("knb,kbc->knc", left, right, preferred_element_type=jnp.float32)

    real = single(rows_in[0], u_inv[0]) - single(rows_in[1], u_inv[1])
    imag = single(rows_in[0], u_inv[1]) + single(rows_in[1], u_inv[0])
    placed = jnp.stack([real, imag]).astype(jnp.bfloat16)
    placed = placed.reshape(2, total_k, group_slots, block_width, block_width)
    placed = jnp.where(slot_live[None, :, :, None, None], placed, jnp.zeros((), jnp.bfloat16))
    block_ids = jnp.arange(group_blocks, dtype=jnp.int32)
    pick_table = (slot_pos[:, :, None] == block_ids[None, None, :]).astype(jnp.bfloat16)
    ainv_blocks = ainv_anc.reshape(2, rows_all, group_blocks, block_width)

    def one_node(items):
        table_k, rows_k = items
        picked = jnp.einsum(
            "sg,cigw->cisw", table_k, ainv_blocks, preferred_element_type=jnp.float32
        )
        picked = picked.astype(jnp.bfloat16).reshape(2, rows_all, group_slots * block_width)
        right = rows_k.reshape(2, group_slots * block_width, block_width)
        real = jnp.dot(picked[0], right[0], preferred_element_type=jnp.float32) - jnp.dot(
            picked[1], right[1], preferred_element_type=jnp.float32
        )
        imag = jnp.dot(picked[0], right[1], preferred_element_type=jnp.float32) + jnp.dot(
            picked[1], right[0], preferred_element_type=jnp.float32
        )
        return jnp.stack([real, imag])

    per_node = lax.map(one_node, (pick_table, jnp.moveaxis(placed, 1, 0)))
    partial_value = jnp.transpose(per_node, (1, 2, 0, 3))
    row_table = (col_struct[:, None, :] == target[None, :, None]).astype(jnp.bfloat16)
    z_rows = jnp.einsum("kts,ckswb->cktwb", row_table, placed, preferred_element_type=jnp.float32)
    z_rows = z_rows.astype(jnp.bfloat16).reshape(2, total_k, rows_all, block_width)
    summed = lax.psum_scatter(
        partial_value.reshape(2, rows_all, total_k * block_width),
        "pcol",
        scatter_dimension=2,
        tiled=True,
    )
    own_struct = lax.dynamic_slice_in_dim(structure, col_here * own_k, own_k, 0)
    member = jnp.any(own_struct[:, :, None] == target[None, None, :], axis=1)
    selected = -summed.reshape(2, row_blocks, block_width, own_k, block_width)
    selected = jnp.where(member.T[None, :, None, :, None], selected, 0.0)
    sel_inv = selected.reshape(2, rows_all, own_k * block_width)
    received = lax.all_to_all(z_rows, "pcol", split_axis=1, concat_axis=1, tiled=True)
    z_own = (
        received.astype(jnp.float32).reshape(2, n_cols, own_k, rows_all, block_width).sum(axis=1)
    )
    quad_term = complex_quad(z_own, selected.reshape(2, rows_all, own_k, block_width))
    total_sum = lax.psum(quad_term, "prow")
    diag_inv = k_inv - total_sum
    return (sel_inv, diag_inv)


def solution(mesh):
    placed = (
        P(None, ("pole", "prow"), "pcol"),
        P(None, "pole", ("pcol", "prow"), None),
        P(None, "pole", None, None),
        P(None, ("pole", "pcol"), None, None),
        P(),
    )
    return jax.shard_map(
        local,
        mesh=mesh,
        in_specs=placed,
        out_specs=(P(None, ("pole", "prow"), "pcol"), P(None, ("pole", "pcol"), None, None)),
        check_vma=False,
    )
```

```python
import functools

import jax
import jax.numpy as jnp
from jax import lax
from jax.experimental import pallas as pl
from jax.experimental.pallas import tpu as pltpu
from jax.sharding import PartitionSpec as P

BF16 = jnp.bfloat16
F32 = jnp.float32
scope = jax.named_scope


def cdot(left, right, dims=(((1,), (0,)), ((), ()))):
    def single(x, y):
        return lax.dot_general(x, y, dims, preferred_element_type=F32)

    real = single(left[0], right[0]) - single(left[1], right[1])
    imag = single(left[0], right[1]) + single(left[1], right[0])
    return real, imag


def remote(src, dst, send_sem, recv_sem, where):
    return pltpu.make_async_remote_copy(
        src_ref=src,
        dst_ref=dst,
        send_sem=send_sem,
        recv_sem=recv_sem,
        device_id=where,
        device_id_type=pl.DeviceIdType.MESH,
    )


def kernel(
    n_rows, n_cols, a_hbm, panel_hbm, u_hbm, k_hbm, table_hbm, sel_out, diag_out,
    table, av, pv, uv, pr, gather, pick_out, picks, acc, kv, z_t, q_own, q_out, q_in, tot,
    local_sem, p_send, p_recv, a_send, a_recv, g_send, g_recv, d_send, q_recv, t_recv,
):
    row = lax.axis_index("prow")
    col = lax.axis_index("pcol")
    width = u_hbm.shape[-1]
    pairs = n_cols // 2
    row_blocks = a_hbm.shape[1] // width
    col_blocks = a_hbm.shape[2] // width
    lanes = width // 2
    share = q_in.shape[2]
    band_rows = q_in.shape[3]
    bands = q_out.shape[1]
    mate = row + 1 - 2 * (row % 2)
    is_end = (row == 0) | (row == n_rows - 1)
    is_inner = jnp.logical_not(is_end)
    end = jnp.where(is_end, row, mate)
    inner = jnp.where(is_end, mate, row)
    over = n_rows - 1 - inner
    far = n_rows - 1 - end

    def peer(unit):
        return ((col // 2 + unit // 2) % pairs) * 2 + (col + unit) % 2

    def unit_of(slot):
        return ((slot // 2 - col // 2 + pairs) % pairs) * 2 + (slot + col) % 2

    copy_p = pltpu.make_async_copy(panel_hbm, pv, local_sem.at[0])
    copy_u = pltpu.make_async_copy(u_hbm.at[:, col], uv, local_sem.at[1])
    copy_t = pltpu.make_async_copy(table_hbm, table, local_sem.at[2])
    copy_a = pltpu.make_async_copy(a_hbm, av, local_sem.at[3])
    copy_k = pltpu.make_async_copy(k_hbm, kv, local_sem.at[2])
    copy_p.start()
    copy_u.start()
    copy_t.start()
    copy_a.start()

    barrier = pltpu.get_barrier_semaphore()

    def greet(axis, there):
        pl.semaphore_signal(barrier, inc=1, device_id={axis: there}, device_id_type=pl.DeviceIdType.MESH)

    for unit in range(1, n_cols):
        greet("pcol", peer(unit))
    greet("prow", mate)
    greet("prow", jnp.where(is_end, over, far))

    @pl.when(is_inner)
    def _():
        greet("prow", over)

    def panel_copy(unit, source):
        return remote(
            pv.at[:, peer(unit)], pr.at[source], p_send.at[0], p_recv.at[unit - 1], {"pcol": peer(unit)}
        )

    def pick_copy(unit, source):
        return remote(
            pick_out.at[unit - 1], picks.at[source], a_send.at[0], a_recv.at[unit - 1], {"pcol": peer(unit)}
        )

    second, whole = 2 * n_cols, 3 * n_cols

    def chunk_copy(half, unit, chunk, index, there):
        block = gather.at[half, unit, chunk]
        return remote(block, block, g_send.at[0], g_recv.at[index], {"prow": there})

    def arrived(view, sem):
        remote(view, view, sem, sem, {"prow": mate}).wait_recv()

    def scale(unit):
        slot = peer(unit)
        if unit == 0:
            left = (pv[0, col], pv[1, col])
        else:
            panel_copy(unit, slot).wait_recv()
            left = (pr[slot, 0], pr[slot, 1])
        value = cdot(left, (uv[0], uv[1]))
        live = (jnp.full((1, lanes), table[col, slot]) >= 0).astype(F32)
        for half in range(2):
            for plane in range(2):
                block = value[plane][:, half * lanes : (half + 1) * lanes]
                gather[half, unit, row, :, plane * lanes : (plane + 1) * lanes] = (block * live).astype(BF16)

    def send_over(half, unit):
        index = second + unit if half else unit + jnp.where(is_end, n_cols, 0)
        chunk_copy(half, unit, row, index, over).start()

    def send_mate(half, unit):
        index = jnp.where(is_end, whole + half, second * half + unit)
        chunk_copy(half, unit, row, index, mate).start()

    def pick(unit):
        node = peer(unit)
        top = jnp.full((1, width), table[node, row]) - row * row_blocks
        side = jnp.full((1, width), table[node, col]) - col * col_blocks
        for plane in range(2):
            total = None
            for i in range(row_blocks):
                for j in range(col_blocks):
                    keep = ((top == i) & (side == j)).astype(F32).astype(BF16)
                    block = av[plane, i * width : (i + 1) * width, j * width : (j + 1) * width] * keep
                    total = block if total is None else total + block
            if unit == 0:
                picks[col, plane] = total
            else:
                pick_out[unit - 1, plane] = total

    with scope("copies"):
        copy_p.wait()
        copy_u.wait()
        copy_t.wait()
    copy_k.start()
    with scope("scale0"):
        scale(0)
    with scope("barrier"):
        pl.semaphore_wait(barrier, n_cols + 2 - is_end.astype(jnp.int32))
    for unit in range(1, n_cols):
        panel_copy(unit, col).start()
    send_over(0, 0)
    send_mate(0, 0)
    with scope("scale1"):
        scale(1)
    send_over(0, 1)
    send_mate(0, 1)
    far_home = unit_of(far)
    early = jnp.where(far_home < 2, far_home, 0)
    send_over(1, early)

    @pl.when(is_end)
    def _():
        send_mate(1, early)

    @pl.when(is_inner)
    def _():
        send_mate(1, 0)
        send_mate(1, 1)

    with scope("copy_a"):
        copy_a.wait()
    for unit in list(range(2, n_cols)) + [1]:
        with scope(f"pick{unit}"):
            pick(unit)
        pick_copy(unit, col).start()
    pick(0)
    late = range(2, n_cols)

    def relay(unit, chunk, index):
        arrived(gather.at[0, unit, chunk], g_recv.at[index])
        chunk_copy(0, unit, chunk, unit, end).start()

    @pl.when(is_end)
    def _():
        for unit in late:
            with scope(f"scale{unit}"):
                scale(unit)
            send_over(0, unit)
            send_mate(0, unit)
        for i in range(n_cols):
            unit = (far_home + i) % n_cols

            @pl.when(unit != early)
            def _():
                send_over(1, unit)
                send_mate(1, unit)

    @pl.when(is_inner)
    def _():
        with scope("scale2"):
            scale(2)
        send_over(0, 2)
        send_mate(0, 2)
        with scope("relay_0o"):
            relay(0, over, 0)
        with scope("relay_1o"):
            relay(1, over, 1)
        with scope("scale3"):
            scale(3)
        send_over(0, 3)
        send_mate(0, 3)
        with scope("relay_01f"):
            relay(0, far, n_cols)
            relay(1, far, n_cols + 1)
        for i in range(n_cols):
            unit = (far_home + i) % n_cols

            @pl.when(unit != early)
            def _():
                send_over(1, unit)

        home = unit_of(end)

        @pl.when(home >= 2)
        def _():
            send_mate(1, home)

        for unit in late:
            with scope(f"relay_{unit}o"):
                relay(unit, over, unit)
            with scope(f"relay_{unit}f"):
                relay(unit, far, n_cols + unit)
        for i in range(n_cols):
            if i == 1:
                for unit in late:

                    @pl.when(unit != home)
                    def _():
                        send_mate(1, unit)

            unit = (home + i) % n_cols
            with scope(f"relay_h1_{i}"):
                arrived(gather.at[1, unit, 0:2], g_recv.at[second + unit])
            chunk_copy(1, unit, over, second + unit, end).start()
            chunk_copy(1, unit, far, second + unit, end).start()

    def ready(half, unit):
        @pl.when(is_end)
        def _():
            arrived(gather.at[half, unit, 0 : n_rows - 1], g_recv.at[second * half + unit])

    def multiply(half, unit, first):
        right = gather[half, unit].reshape(width, width)
        slot = peer(unit)
        for plane in range(2):
            value = jnp.dot(picks[slot, plane], right, preferred_element_type=F32)
            if first:
                acc[plane] = value
            else:
                acc[plane] += value

    @pl.when(is_inner)
    def _():
        for half in range(2):
            with scope(f"mate{half}"):
                arrived(gather.at[half, 0], g_recv.at[whole + half])

    home = unit_of(row)
    live = (jnp.full((1, width), table[col, row]) >= 0).astype(F32)
    named = jnp.full((1, lanes), table[col, row]) - row * row_blocks

    first = n_rows // 2 - 1

    def quad_copy(half, there, part, source):
        return remote(
            q_out.at[half, (there - first) * share + part], q_in.at[source, half, part],
            d_send.at[0], q_recv.at[half, part], {"prow": there},
        )

    def quad(half):
        real = acc[0, :, :lanes] - acc[1, :, lanes:]
        imag = acc[0, :, lanes:] + acc[1, :, :lanes]
        value = jnp.concatenate([real, imag], axis=1) * live
        low = value.astype(BF16)
        for there in (over, inner):
            top = there - first
            product = jnp.dot(z_t[top], low, preferred_element_type=F32)
            real = product[:lanes, :lanes] - product[lanes:, lanes:]
            imag = product[:lanes, lanes:] + product[lanes:, :lanes]
            both = jnp.concatenate([real, imag], axis=1)
            for part in range(share):
                block = both[part * band_rows : (part + 1) * band_rows]
                q_out[half, top * share + part] = block.astype(BF16)
                if there is inner:
                    q_own[half, part] = block

            @pl.when(row != there)
            def _():
                for part in range(share):
                    quad_copy(half, there, part, row).start()

        columns = slice(half * lanes, (half + 1) * lanes)
        for i in range(row_blocks):
            keep = -(named == i).astype(F32)
            for plane in range(2):
                block = value[:, plane * lanes : (plane + 1) * lanes]
                sel_out[plane, i * width : (i + 1) * width, columns] = block * keep

    for unit in range(n_cols):
        with scope(f"ready_h0_{unit}"):
            ready(0, unit)
        with scope(f"wpick_{unit}"):
            if unit > 0:
                pick_copy(unit, peer(unit)).wait_recv()
        multiply(0, unit, unit == 0)
    with scope("ready_home"):
        ready(1, home)
    for top in range(2):
        z_t[top] = gather[top, home].reshape(width, width).T
    with scope("quad0"):
        quad(0)
    for i in range(n_cols):
        unit = (home + i) % n_cols
        if i > 0:
            with scope(f"ready_h1_{i}"):
                ready(1, unit)
        multiply(1, unit, i == 0)
    with scope("quad1"):
        quad(1)
    copy_k.wait()

    def drain(view, sem):
        remote(view, view, sem, sem, {"prow": mate}).wait_send()

    drain(pr.at[0 : n_cols - 1], p_send.at[0])
    drain(pick_out, a_send.at[0])

    @pl.when(is_inner)
    def _():
        drain(gather, g_send.at[0])

    @pl.when(is_end)
    def _():
        drain(gather.at[0], g_send.at[0])
        drain(q_out, d_send.at[0])

    def total_copy(half, part, there):
        block = tot.at[half, (row - first) * share + part]
        return remote(block, block, d_send.at[0], t_recv.at[half, row - first], {"prow": there})

    def finish(half, group):
        columns = slice(half * lanes, (half + 1) * lanes)
        for part in range(share):
            band = group * share + part
            rows = pl.ds(pl.multiple_of(band * band_rows, band_rows), band_rows)
            for plane in range(2):
                block = tot[half, band, :, plane * lanes : (plane + 1) * lanes].astype(F32)
                diag_out[plane, 0, rows, columns] = kv[plane, 0, rows, columns] + block

    @pl.when(is_inner)
    def _():
        for half in range(2):
            for part in range(share):
                with scope(f"wq{half}_{part}"):
                    arrived(q_in.at[0 : n_rows - 1, half, part], q_recv.at[half, part])
                total = q_own[half, part]
                for source in (over, end, far):
                    total = total + q_in[source, half, part].astype(F32)
                tot[half, (row - first) * share + part] = total.astype(BF16)
                total_copy(half, part, far).start()
                total_copy(half, part, end).start()
            for part in range(share):
                total_copy(half, part, over).start()
        for half in range(2):
            finish(half, row - first)

    for half in range(2):
        @pl.when(is_end)
        def _():
            with scope(f"wt_near{half}"):
                arrived(tot.at[half, 0:share], t_recv.at[half, inner - first])
            finish(half, inner - first)

        with scope(f"wt_over{half}"):
            arrived(tot.at[half, 0:share], t_recv.at[half, over - first])
        finish(half, over - first)

    @pl.when(is_inner)
    def _():
        drain(q_in, d_send.at[0])


def place(sel, diag, sel_out, diag_out, out_sem):
    copies = [
        pltpu.make_async_copy(sel, sel_out, out_sem.at[0]),
        pltpu.make_async_copy(diag, diag_out, out_sem.at[1]),
    ]
    for copy in copies:
        copy.start()
    for copy in copies:
        copy.wait()


def compact(ainv_anc, panel, u_inv, k_inv, structure):
    n_rows, n_cols = lax.axis_size("prow"), lax.axis_size("pcol")
    width, part = u_inv.shape[-1], panel.shape[2]
    row_blocks = ainv_anc.shape[1] // width
    bands = n_rows
    share = bands // 2
    hbm = pl.BlockSpec(memory_space=pltpu.HBM)
    vmem = pl.BlockSpec(memory_space=pltpu.VMEM)
    dma = pltpu.SemaphoreType.DMA
    shapes = (
        jax.ShapeDtypeStruct((2, row_blocks * width, width), F32),
        jax.ShapeDtypeStruct(k_inv.shape, F32),
    )
    piece = (width // bands, width)
    results = pl.pallas_call(
        functools.partial(kernel, n_rows, n_cols),
        out_shape=tuple(pltpu.VMEM(s.shape, s.dtype) for s in shapes),
        in_specs=[hbm, hbm, hbm, hbm, hbm],
        out_specs=(vmem, vmem),
        scratch_shapes=[
            pltpu.SMEM(structure.shape, jnp.int32),
            pltpu.VMEM(ainv_anc.shape, BF16),
            pltpu.VMEM(panel.shape, BF16),
            pltpu.VMEM((2, width, width), BF16),
            pltpu.VMEM((n_cols, 2, part, width), BF16),
            pltpu.VMEM((2, n_cols, n_rows, part, width), BF16),
            pltpu.VMEM((n_cols - 1, 2, width, width), BF16),
            pltpu.VMEM((n_cols, 2, width, width), BF16),
            pltpu.VMEM((2, width, width), F32),
            pltpu.VMEM(k_inv.shape, F32),
            pltpu.VMEM((2, width, width), BF16),
            pltpu.VMEM((2, share) + piece, F32),
            pltpu.VMEM((2, bands) + piece, BF16),
            pltpu.VMEM((n_rows, 2, share) + piece, BF16),
            pltpu.VMEM((2, bands) + piece, BF16),
            dma((4,)),
            dma((1,)),
            dma((n_cols - 1,)),
            dma((1,)),
            dma((n_cols - 1,)),
            dma((1,)),
            dma((3 * n_cols + 2,)),
            dma((1,)),
            dma((2, share)),
            dma((2, 2)),
        ],
        compiler_params=pltpu.CompilerParams(
            collective_id=0, has_side_effects=True
        ),
    )(ainv_anc, panel, u_inv, k_inv, structure)
    return pl.pallas_call(
        place,
        out_shape=shapes,
        in_specs=[vmem, vmem],
        out_specs=(hbm, hbm),
        scratch_shapes=[dma((2,))],
    )(*[pltpu.with_memory_space_constraint(x, pltpu.VMEM) for x in results])


def complex_quad(z_part, s_part):
    highest = lax.Precision.HIGHEST

    def single(left, right):
        return jnp.einsum("kra,rkb->kab", left, right, precision=highest)

    real = single(z_part[0], s_part[0]) - single(z_part[1], s_part[1])
    imag = single(z_part[0], s_part[1]) + single(z_part[1], s_part[0])
    return jnp.stack([real, imag])


def local(ainv_anc, panel, u_inv, k_inv, structure):
    block_width = u_inv.shape[-1]
    cols = lax.axis_size("pcol")
    if (
        structure.shape[1] == cols
        and lax.axis_size("prow") == cols
        and ainv_anc.shape[1] == ainv_anc.shape[2]
        and u_inv.shape[1] == cols
        and cols // 2 == 2
        and cols % 2 == 0
    ):
        return compact(ainv_anc, panel, u_inv, k_inv, structure)
    total_k = u_inv.shape[1]
    own_k = k_inv.shape[1]
    n_cols = lax.axis_size("pcol")
    row_here = lax.axis_index("prow")
    col_here = lax.axis_index("pcol")
    row_blocks = ainv_anc.shape[1] // block_width
    group_blocks = ainv_anc.shape[2] // block_width
    group_slots = structure.shape[1] // n_cols
    rows_all = row_blocks * block_width
    col_struct = lax.dynamic_slice_in_dim(structure, col_here * group_slots, group_slots, 1)
    slot_live = col_struct >= 0
    slot_pos = col_struct - col_here * group_blocks
    first_block = row_here * row_blocks
    target = first_block + jnp.arange(row_blocks, dtype=jnp.int32)
    rows_in = lax.all_gather(panel, "prow", axis=2, tiled=True)

    def single(left, right):
        return jnp.einsum("knb,kbc->knc", left, right, preferred_element_type=jnp.float32)

    real = single(rows_in[0], u_inv[0]) - single(rows_in[1], u_inv[1])
    imag = single(rows_in[0], u_inv[1]) + single(rows_in[1], u_inv[0])
    placed = jnp.stack([real, imag]).astype(jnp.bfloat16)
    placed = placed.reshape(2, total_k, group_slots, block_width, block_width)
    placed = jnp.where(slot_live[None, :, :, None, None], placed, jnp.zeros((), jnp.bfloat16))
    block_ids = jnp.arange(group_blocks, dtype=jnp.int32)
    pick_table = (slot_pos[:, :, None] == block_ids[None, None, :]).astype(jnp.bfloat16)
    ainv_blocks = ainv_anc.reshape(2, rows_all, group_blocks, block_width)

    def one_node(items):
        table_k, rows_k = items
        picked = jnp.einsum(
            "sg,cigw->cisw", table_k, ainv_blocks, preferred_element_type=jnp.float32
        )
        picked = picked.astype(jnp.bfloat16).reshape(2, rows_all, group_slots * block_width)
        right = rows_k.reshape(2, group_slots * block_width, block_width)
        real = jnp.dot(picked[0], right[0], preferred_element_type=jnp.float32) - jnp.dot(
            picked[1], right[1], preferred_element_type=jnp.float32
        )
        imag = jnp.dot(picked[0], right[1], preferred_element_type=jnp.float32) + jnp.dot(
            picked[1], right[0], preferred_element_type=jnp.float32
        )
        return jnp.stack([real, imag])

    per_node = lax.map(one_node, (pick_table, jnp.moveaxis(placed, 1, 0)))
    partial_value = jnp.transpose(per_node, (1, 2, 0, 3))
    row_table = (col_struct[:, None, :] == target[None, :, None]).astype(jnp.bfloat16)
    z_rows = jnp.einsum("kts,ckswb->cktwb", row_table, placed, preferred_element_type=jnp.float32)
    z_rows = z_rows.astype(jnp.bfloat16).reshape(2, total_k, rows_all, block_width)
    summed = lax.psum_scatter(
        partial_value.reshape(2, rows_all, total_k * block_width),
        "pcol",
        scatter_dimension=2,
        tiled=True,
    )
    own_struct = lax.dynamic_slice_in_dim(structure, col_here * own_k, own_k, 0)
    member = jnp.any(own_struct[:, :, None] == target[None, None, :], axis=1)
    selected = -summed.reshape(2, row_blocks, block_width, own_k, block_width)
    selected = jnp.where(member.T[None, :, None, :, None], selected, 0.0)
    sel_inv = selected.reshape(2, rows_all, own_k * block_width)
    received = lax.all_to_all(z_rows, "pcol", split_axis=1, concat_axis=1, tiled=True)
    z_own = (
        received.astype(jnp.float32).reshape(2, n_cols, own_k, rows_all, block_width).sum(axis=1)
    )
    quad_term = complex_quad(z_own, selected.reshape(2, rows_all, own_k, block_width))
    total_sum = lax.psum(quad_term, "prow")
    diag_inv = k_inv - total_sum
    return (sel_inv, diag_inv)


def solution(mesh):
    placed = (
        P(None, ("pole", "prow"), "pcol"),
        P(None, "pole", ("pcol", "prow"), None),
        P(None, "pole", None, None),
        P(None, ("pole", "pcol"), None, None),
        P(),
    )
    return jax.shard_map(
        local,
        mesh=mesh,
        in_specs=placed,
        out_specs=(P(None, ("pole", "prow"), "pcol"), P(None, ("pole", "pcol"), None, None)),
        check_vma=False,
    )
```

```python
import functools

import jax
import jax.numpy as jnp
from jax import lax
from jax.experimental import pallas as pl
from jax.experimental.pallas import tpu as pltpu
from jax.sharding import PartitionSpec as P

BF16 = jnp.bfloat16
F32 = jnp.float32
scope = jax.named_scope


def cdot(left, right, dims=(((1,), (0,)), ((), ()))):
    def single(x, y):
        return lax.dot_general(x, y, dims, preferred_element_type=F32)

    real = single(left[0], right[0]) - single(left[1], right[1])
    imag = single(left[0], right[1]) + single(left[1], right[0])
    return real, imag


def remote(src, dst, send_sem, recv_sem, where):
    return pltpu.make_async_remote_copy(
        src_ref=src,
        dst_ref=dst,
        send_sem=send_sem,
        recv_sem=recv_sem,
        device_id=where,
        device_id_type=pl.DeviceIdType.MESH,
    )


def kernel(
    n_rows, n_cols, a_hbm, panel_hbm, u_hbm, k_hbm, table_hbm, sel_out, diag_out,
    table, av, pv, uv, pr, gather, pick_out, picks, acc, kv, z_t, q_own, q_out, q_in, tot,
    local_sem, p_send, p_recv, a_send, a_recv, g_send, g_recv, d_send, q_recv, t_recv,
):
    row = lax.axis_index("prow")
    col = lax.axis_index("pcol")
    width = u_hbm.shape[-1]
    pairs = n_cols // 2
    row_blocks = a_hbm.shape[1] // width
    col_blocks = a_hbm.shape[2] // width
    lanes = width // 2
    share = q_in.shape[2]
    band_rows = q_in.shape[3]
    bands = q_out.shape[1]
    mate = row + 1 - 2 * (row % 2)
    is_end = (row == 0) | (row == n_rows - 1)
    is_inner = jnp.logical_not(is_end)
    end = jnp.where(is_end, row, mate)
    inner = jnp.where(is_end, mate, row)
    over = n_rows - 1 - inner
    far = n_rows - 1 - end

    def peer(unit):
        return ((col // 2 + unit // 2) % pairs) * 2 + (col + unit) % 2

    def unit_of(slot):
        return ((slot // 2 - col // 2 + pairs) % pairs) * 2 + (slot + col) % 2

    copy_p = pltpu.make_async_copy(panel_hbm, pv, local_sem.at[0])
    copy_u = pltpu.make_async_copy(u_hbm.at[:, col], uv, local_sem.at[1])
    copy_t = pltpu.make_async_copy(table_hbm, table, local_sem.at[2])
    copy_a = pltpu.make_async_copy(a_hbm, av, local_sem.at[3])
    copy_k = pltpu.make_async_copy(k_hbm, kv, local_sem.at[2])
    copy_p.start()
    copy_u.start()
    copy_t.start()
    copy_a.start()

    barrier = pltpu.get_barrier_semaphore()

    def greet(axis, there):
        pl.semaphore_signal(barrier, inc=1, device_id={axis: there}, device_id_type=pl.DeviceIdType.MESH)

    for unit in range(1, n_cols):
        greet("pcol", peer(unit))
    greet("prow", mate)
    greet("prow", jnp.where(is_end, over, far))

    @pl.when(is_inner)
    def _():
        greet("prow", over)

    def panel_copy(unit, source):
        return remote(
            pv.at[:, peer(unit)], pr.at[source], p_send.at[0], p_recv.at[unit - 1], {"pcol": peer(unit)}
        )

    def pick_copy(unit, source):
        return remote(
            pick_out.at[unit - 1], picks.at[source], a_send.at[0], a_recv.at[unit - 1], {"pcol": peer(unit)}
        )

    second, whole = 2 * n_cols, 3 * n_cols

    def chunk_copy(half, unit, chunk, index, there):
        block = gather.at[half, unit, chunk]
        return remote(block, block, g_send.at[0], g_recv.at[index], {"prow": there})

    def arrived(view, sem):
        remote(view, view, sem, sem, {"prow": mate}).wait_recv()

    def scale(unit):
        slot = peer(unit)
        if unit == 0:
            left = (pv[0, col], pv[1, col])
        else:
            panel_copy(unit, slot).wait_recv()
            left = (pr[slot, 0], pr[slot, 1])
        value = cdot(left, (uv[0], uv[1]))
        live = (jnp.full((1, lanes), table[col, slot]) >= 0).astype(F32)
        for half in range(2):
            for plane in range(2):
                block = value[plane][:, half * lanes : (half + 1) * lanes]
                gather[half, unit, row, :, plane * lanes : (plane + 1) * lanes] = (block * live).astype(BF16)

    def send_over(half, unit):
        index = second + unit if half else unit + jnp.where(is_end, n_cols, 0)
        chunk_copy(half, unit, row, index, over).start()

    def send_mate(half, unit):
        index = jnp.where(is_end, whole + half, second * half + unit)
        chunk_copy(half, unit, row, index, mate).start()

    def pick(unit):
        node = peer(unit)
        top = jnp.full((1, width), table[node, row]) - row * row_blocks
        side = jnp.full((1, width), table[node, col]) - col * col_blocks
        for plane in range(2):
            total = None
            for i in range(row_blocks):
                for j in range(col_blocks):
                    keep = ((top == i) & (side == j)).astype(F32).astype(BF16)
                    block = av[plane, i * width : (i + 1) * width, j * width : (j + 1) * width] * keep
                    total = block if total is None else total + block
            if unit == 0:
                picks[col, plane] = total
            else:
                pick_out[unit - 1, plane] = total

    with scope("copies"):
        copy_p.wait()
        copy_u.wait()
        copy_t.wait()
    copy_k.start()
    with scope("scale0"):
        scale(0)
    with scope("barrier"):
        pl.semaphore_wait(barrier, n_cols + 2 - is_end.astype(jnp.int32))
    for unit in range(1, n_cols):
        panel_copy(unit, col).start()
    send_over(0, 0)
    send_mate(0, 0)
    with scope("scale1"):
        scale(1)
    send_over(0, 1)
    send_mate(0, 1)
    far_home = unit_of(far)
    early = jnp.where(far_home < 2, far_home, 0)
    send_over(1, early)

    @pl.when(is_end)
    def _():
        send_mate(1, early)

    @pl.when(is_inner)
    def _():
        send_mate(1, 0)
        send_mate(1, 1)

    with scope("copy_a"):
        copy_a.wait()
    for unit in list(range(2, n_cols)) + [1]:
        with scope(f"pick{unit}"):
            pick(unit)
        pick_copy(unit, col).start()
    pick(0)
    late = range(2, n_cols)

    def relay(unit, chunk, index):
        arrived(gather.at[0, unit, chunk], g_recv.at[index])
        chunk_copy(0, unit, chunk, unit, end).start()

    @pl.when(is_end)
    def _():
        for unit in late:
            with scope(f"scale{unit}"):
                scale(unit)
            send_over(0, unit)
            send_mate(0, unit)
        for i in range(n_cols):
            unit = (far_home + i) % n_cols

            @pl.when(unit != early)
            def _():
                send_over(1, unit)
                send_mate(1, unit)

    @pl.when(is_inner)
    def _():
        with scope("relay_0o"):
            relay(0, over, 0)
        with scope("scale2"):
            scale(2)
        send_over(0, 2)
        send_mate(0, 2)
        with scope("relay_1o"):
            relay(1, over, 1)
        with scope("scale3"):
            scale(3)
        send_over(0, 3)
        send_mate(0, 3)
        with scope("relay_01f"):
            relay(0, far, n_cols)
            relay(1, far, n_cols + 1)
        for i in range(n_cols):
            unit = (far_home + i) % n_cols

            @pl.when(unit != early)
            def _():
                send_over(1, unit)

        home = unit_of(end)

        @pl.when(home >= 2)
        def _():
            send_mate(1, home)

        for unit in late:
            with scope(f"relay_{unit}o"):
                relay(unit, over, unit)
            with scope(f"relay_{unit}f"):
                relay(unit, far, n_cols + unit)
        for i in range(n_cols):
            if i == 1:
                for unit in late:

                    @pl.when(unit != home)
                    def _():
                        send_mate(1, unit)

            unit = (home + i) % n_cols
            with scope(f"relay_h1_{i}"):
                arrived(gather.at[1, unit, 0:2], g_recv.at[second + unit])
            chunk_copy(1, unit, over, second + unit, end).start()
            chunk_copy(1, unit, far, second + unit, end).start()

    def ready(half, unit):
        @pl.when(is_end)
        def _():
            arrived(gather.at[half, unit, 0 : n_rows - 1], g_recv.at[second * half + unit])

    def multiply(half, unit, first):
        right = gather[half, unit].reshape(width, width)
        slot = peer(unit)
        for plane in range(2):
            value = jnp.dot(picks[slot, plane], right, preferred_element_type=F32)
            if first:
                acc[plane] = value
            else:
                acc[plane] += value

    @pl.when(is_inner)
    def _():
        for half in range(2):
            with scope(f"mate{half}"):
                arrived(gather.at[half, 0], g_recv.at[whole + half])

    home = unit_of(row)
    live = (jnp.full((1, width), table[col, row]) >= 0).astype(F32)
    named = jnp.full((1, lanes), table[col, row]) - row * row_blocks

    first = n_rows // 2 - 1

    def quad_copy(half, there, part, source):
        return remote(
            q_out.at[half, (there - first) * share + part], q_in.at[source, half, part],
            d_send.at[0], q_recv.at[half, part], {"prow": there},
        )

    def quad(half):
        real = acc[0, :, :lanes] - acc[1, :, lanes:]
        imag = acc[0, :, lanes:] + acc[1, :, :lanes]
        value = jnp.concatenate([real, imag], axis=1) * live
        low = value.astype(BF16)
        for there in (over, inner):
            top = there - first
            product = jnp.dot(z_t[top], low, preferred_element_type=F32)
            real = product[:lanes, :lanes] - product[lanes:, lanes:]
            imag = product[:lanes, lanes:] + product[lanes:, :lanes]
            both = jnp.concatenate([real, imag], axis=1)
            for part in range(share):
                block = both[part * band_rows : (part + 1) * band_rows]
                q_out[half, top * share + part] = block.astype(BF16)
                if there is inner:
                    q_own[half, part] = block

            @pl.when(row != there)
            def _():
                for part in range(share):
                    quad_copy(half, there, part, row).start()

        columns = slice(half * lanes, (half + 1) * lanes)
        for i in range(row_blocks):
            keep = -(named == i).astype(F32)
            for plane in range(2):
                block = value[:, plane * lanes : (plane + 1) * lanes]
                sel_out[plane, i * width : (i + 1) * width, columns] = block * keep

    for unit in range(n_cols):
        with scope(f"ready_h0_{unit}"):
            ready(0, unit)
        with scope(f"wpick_{unit}"):
            if unit > 0:
                pick_copy(unit, peer(unit)).wait_recv()
        multiply(0, unit, unit == 0)
    with scope("ready_home"):
        ready(1, home)
    for top in range(2):
        z_t[top] = gather[top, home].reshape(width, width).T
    with scope("quad0"):
        quad(0)
    for i in range(n_cols):
        unit = (home + i) % n_cols
        if i > 0:
            with scope(f"ready_h1_{i}"):
                ready(1, unit)
        multiply(1, unit, i == 0)
    with scope("quad1"):
        quad(1)
    copy_k.wait()

    def drain(view, sem):
        remote(view, view, sem, sem, {"prow": mate}).wait_send()

    drain(pr.at[0 : n_cols - 1], p_send.at[0])
    drain(pick_out, a_send.at[0])

    @pl.when(is_inner)
    def _():
        drain(gather, g_send.at[0])

    @pl.when(is_end)
    def _():
        drain(gather.at[0], g_send.at[0])
        drain(q_out, d_send.at[0])

    def total_copy(half, part, there):
        block = tot.at[half, (row - first) * share + part]
        return remote(block, block, d_send.at[0], t_recv.at[half, row - first], {"prow": there})

    def finish(half, group):
        columns = slice(half * lanes, (half + 1) * lanes)
        for part in range(share):
            band = group * share + part
            rows = pl.ds(pl.multiple_of(band * band_rows, band_rows), band_rows)
            for plane in range(2):
                block = tot[half, band, :, plane * lanes : (plane + 1) * lanes].astype(F32)
                diag_out[plane, 0, rows, columns] = kv[plane, 0, rows, columns] + block

    @pl.when(is_inner)
    def _():
        for half in range(2):
            for part in range(share):
                with scope(f"wq{half}_{part}"):
                    arrived(q_in.at[0 : n_rows - 1, half, part], q_recv.at[half, part])
                total = q_own[half, part]
                for source in (over, end, far):
                    total = total + q_in[source, half, part].astype(F32)
                tot[half, (row - first) * share + part] = total.astype(BF16)
                total_copy(half, part, far).start()
                total_copy(half, part, end).start()
        for half in range(2):
            for part in range(share):
                total_copy(half, part, over).start()
        for half in range(2):
            finish(half, row - first)

    for half in range(2):
        @pl.when(is_end)
        def _():
            with scope(f"wt_near{half}"):
                arrived(tot.at[half, 0:share], t_recv.at[half, inner - first])
            finish(half, inner - first)

        with scope(f"wt_over{half}"):
            arrived(tot.at[half, 0:share], t_recv.at[half, over - first])
        finish(half, over - first)

    @pl.when(is_inner)
    def _():
        drain(q_in, d_send.at[0])


def place(sel, diag, sel_out, diag_out, out_sem):
    copies = [
        pltpu.make_async_copy(sel, sel_out, out_sem.at[0]),
        pltpu.make_async_copy(diag, diag_out, out_sem.at[1]),
    ]
    for copy in copies:
        copy.start()
    for copy in copies:
        copy.wait()


def compact(ainv_anc, panel, u_inv, k_inv, structure):
    n_rows, n_cols = lax.axis_size("prow"), lax.axis_size("pcol")
    width, part = u_inv.shape[-1], panel.shape[2]
    row_blocks = ainv_anc.shape[1] // width
    bands = n_rows
    share = bands // 2
    hbm = pl.BlockSpec(memory_space=pltpu.HBM)
    vmem = pl.BlockSpec(memory_space=pltpu.VMEM)
    dma = pltpu.SemaphoreType.DMA
    shapes = (
        jax.ShapeDtypeStruct((2, row_blocks * width, width), F32),
        jax.ShapeDtypeStruct(k_inv.shape, F32),
    )
    piece = (width // bands, width)
    results = pl.pallas_call(
        functools.partial(kernel, n_rows, n_cols),
        out_shape=tuple(pltpu.VMEM(s.shape, s.dtype) for s in shapes),
        in_specs=[hbm, hbm, hbm, hbm, hbm],
        out_specs=(vmem, vmem),
        scratch_shapes=[
            pltpu.SMEM(structure.shape, jnp.int32),
            pltpu.VMEM(ainv_anc.shape, BF16),
            pltpu.VMEM(panel.shape, BF16),
            pltpu.VMEM((2, width, width), BF16),
            pltpu.VMEM((n_cols, 2, part, width), BF16),
            pltpu.VMEM((2, n_cols, n_rows, part, width), BF16),
            pltpu.VMEM((n_cols - 1, 2, width, width), BF16),
            pltpu.VMEM((n_cols, 2, width, width), BF16),
            pltpu.VMEM((2, width, width), F32),
            pltpu.VMEM(k_inv.shape, F32),
            pltpu.VMEM((2, width, width), BF16),
            pltpu.VMEM((2, share) + piece, F32),
            pltpu.VMEM((2, bands) + piece, BF16),
            pltpu.VMEM((n_rows, 2, share) + piece, BF16),
            pltpu.VMEM((2, bands) + piece, BF16),
            dma((4,)),
            dma((1,)),
            dma((n_cols - 1,)),
            dma((1,)),
            dma((n_cols - 1,)),
            dma((1,)),
            dma((3 * n_cols + 2,)),
            dma((1,)),
            dma((2, share)),
            dma((2, 2)),
        ],
        compiler_params=pltpu.CompilerParams(
            collective_id=0, has_side_effects=True
        ),
    )(ainv_anc, panel, u_inv, k_inv, structure)
    return pl.pallas_call(
        place,
        out_shape=shapes,
        in_specs=[vmem, vmem],
        out_specs=(hbm, hbm),
        scratch_shapes=[dma((2,))],
    )(*[pltpu.with_memory_space_constraint(x, pltpu.VMEM) for x in results])


def complex_quad(z_part, s_part):
    highest = lax.Precision.HIGHEST

    def single(left, right):
        return jnp.einsum("kra,rkb->kab", left, right, precision=highest)

    real = single(z_part[0], s_part[0]) - single(z_part[1], s_part[1])
    imag = single(z_part[0], s_part[1]) + single(z_part[1], s_part[0])
    return jnp.stack([real, imag])


def local(ainv_anc, panel, u_inv, k_inv, structure):
    block_width = u_inv.shape[-1]
    cols = lax.axis_size("pcol")
    if (
        structure.shape[1] == cols
        and lax.axis_size("prow") == cols
        and ainv_anc.shape[1] == ainv_anc.shape[2]
        and u_inv.shape[1] == cols
        and cols // 2 == 2
        and cols % 2 == 0
    ):
        return compact(ainv_anc, panel, u_inv, k_inv, structure)
    total_k = u_inv.shape[1]
    own_k = k_inv.shape[1]
    n_cols = lax.axis_size("pcol")
    row_here = lax.axis_index("prow")
    col_here = lax.axis_index("pcol")
    row_blocks = ainv_anc.shape[1] // block_width
    group_blocks = ainv_anc.shape[2] // block_width
    group_slots = structure.shape[1] // n_cols
    rows_all = row_blocks * block_width
    col_struct = lax.dynamic_slice_in_dim(structure, col_here * group_slots, group_slots, 1)
    slot_live = col_struct >= 0
    slot_pos = col_struct - col_here * group_blocks
    first_block = row_here * row_blocks
    target = first_block + jnp.arange(row_blocks, dtype=jnp.int32)
    rows_in = lax.all_gather(panel, "prow", axis=2, tiled=True)

    def single(left, right):
        return jnp.einsum("knb,kbc->knc", left, right, preferred_element_type=jnp.float32)

    real = single(rows_in[0], u_inv[0]) - single(rows_in[1], u_inv[1])
    imag = single(rows_in[0], u_inv[1]) + single(rows_in[1], u_inv[0])
    placed = jnp.stack([real, imag]).astype(jnp.bfloat16)
    placed = placed.reshape(2, total_k, group_slots, block_width, block_width)
    placed = jnp.where(slot_live[None, :, :, None, None], placed, jnp.zeros((), jnp.bfloat16))
    block_ids = jnp.arange(group_blocks, dtype=jnp.int32)
    pick_table = (slot_pos[:, :, None] == block_ids[None, None, :]).astype(jnp.bfloat16)
    ainv_blocks = ainv_anc.reshape(2, rows_all, group_blocks, block_width)

    def one_node(items):
        table_k, rows_k = items
        picked = jnp.einsum(
            "sg,cigw->cisw", table_k, ainv_blocks, preferred_element_type=jnp.float32
        )
        picked = picked.astype(jnp.bfloat16).reshape(2, rows_all, group_slots * block_width)
        right = rows_k.reshape(2, group_slots * block_width, block_width)
        real = jnp.dot(picked[0], right[0], preferred_element_type=jnp.float32) - jnp.dot(
            picked[1], right[1], preferred_element_type=jnp.float32
        )
        imag = jnp.dot(picked[0], right[1], preferred_element_type=jnp.float32) + jnp.dot(
            picked[1], right[0], preferred_element_type=jnp.float32
        )
        return jnp.stack([real, imag])

    per_node = lax.map(one_node, (pick_table, jnp.moveaxis(placed, 1, 0)))
    partial_value = jnp.transpose(per_node, (1, 2, 0, 3))
    row_table = (col_struct[:, None, :] == target[None, :, None]).astype(jnp.bfloat16)
    z_rows = jnp.einsum("kts,ckswb->cktwb", row_table, placed, preferred_element_type=jnp.float32)
    z_rows = z_rows.astype(jnp.bfloat16).reshape(2, total_k, rows_all, block_width)
    summed = lax.psum_scatter(
        partial_value.reshape(2, rows_all, total_k * block_width),
        "pcol",
        scatter_dimension=2,
        tiled=True,
    )
    own_struct = lax.dynamic_slice_in_dim(structure, col_here * own_k, own_k, 0)
    member = jnp.any(own_struct[:, :, None] == target[None, None, :], axis=1)
    selected = -summed.reshape(2, row_blocks, block_width, own_k, block_width)
    selected = jnp.where(member.T[None, :, None, :, None], selected, 0.0)
    sel_inv = selected.reshape(2, rows_all, own_k * block_width)
    received = lax.all_to_all(z_rows, "pcol", split_axis=1, concat_axis=1, tiled=True)
    z_own = (
        received.astype(jnp.float32).reshape(2, n_cols, own_k, rows_all, block_width).sum(axis=1)
    )
    quad_term = complex_quad(z_own, selected.reshape(2, rows_all, own_k, block_width))
    total_sum = lax.psum(quad_term, "prow")
    diag_inv = k_inv - total_sum
    return (sel_inv, diag_inv)


def solution(mesh):
    placed = (
        P(None, ("pole", "prow"), "pcol"),
        P(None, "pole", ("pcol", "prow"), None),
        P(None, "pole", None, None),
        P(None, ("pole", "pcol"), None, None),
        P(),
    )
    return jax.shard_map(
        local,
        mesh=mesh,
        in_specs=placed,
        out_specs=(P(None, ("pole", "prow"), "pcol"), P(None, ("pole", "pcol"), None, None)),
        check_vma=False,
    )
```

```python
import functools

import jax
import jax.numpy as jnp
from jax import lax
from jax.experimental import pallas as pl
from jax.experimental.pallas import tpu as pltpu
from jax.sharding import PartitionSpec as P

BF16 = jnp.bfloat16
F32 = jnp.float32
LANES = 128
scope = jax.named_scope


def cdot(left, right, dims=(((1,), (0,)), ((), ()))):
    def single(x, y):
        return lax.dot_general(x, y, dims, preferred_element_type=F32)

    real = single(left[0], right[0]) - single(left[1], right[1])
    imag = single(left[0], right[1]) + single(left[1], right[0])
    return real, imag


def remote(src, dst, send_sem, recv_sem, where):
    return pltpu.make_async_remote_copy(
        src_ref=src,
        dst_ref=dst,
        send_sem=send_sem,
        recv_sem=recv_sem,
        device_id=where,
        device_id_type=pl.DeviceIdType.MESH,
    )


def swap(x):
    return pltpu.roll(x, x.shape[1] // 2, 1)


def low_lanes():
    return lax.broadcasted_iota(jnp.int32, (1, LANES), 1) < LANES // 2


def tiles_of(x):
    return [x[:, at : at + LANES] for at in range(0, x.shape[1], LANES)]


def join(left, right):
    sign = jnp.where(low_lanes(), -1.0, 1.0)
    return jnp.concatenate([a + swap(b) * sign for a, b in zip(tiles_of(left), tiles_of(right))], axis=1)


def cross(a, b):
    low = low_lanes()
    return jnp.where(low, a, swap(b)), jnp.where(low, swap(a), b)


def kernel(
    n_rows, n_cols, spans, a_hbm, panel_hbm, u_hbm, k_hbm, table_hbm, sel_out, diag_out,
    table, av, pv, uv, pr, pick_out, picks, acc, kv, z_t,
    gather_0, gather_1, gather_2, own_0, own_1, own_2, out_0, out_1, out_2,
    in_0, in_1, in_2, tot_0, tot_1, tot_2,
    local_sem, p_send, p_recv, a_send, a_recv, g_send, g_recv, d_send, q_recv, t_recv,
):
    gather, own = (gather_0, gather_1, gather_2), (own_0, own_1, own_2)
    q_out, q_in, tot = (out_0, out_1, out_2), (in_0, in_1, in_2), (tot_0, tot_1, tot_2)
    groups = range(len(spans))
    row = lax.axis_index("prow")
    col = lax.axis_index("pcol")
    width = u_hbm.shape[-1]
    pairs = n_cols // 2
    row_blocks = a_hbm.shape[1] // width
    col_blocks = a_hbm.shape[2] // width
    band_rows = LANES // 2
    share = q_in[0].shape[1]
    first = n_rows // 2 - 1
    mate = row + 1 - 2 * (row % 2)
    is_end = (row == 0) | (row == n_rows - 1)
    is_inner = jnp.logical_not(is_end)
    end = jnp.where(is_end, row, mate)
    inner = jnp.where(is_end, mate, row)
    over = n_rows - 1 - inner
    far = n_rows - 1 - end

    def peer(unit):
        return ((col // 2 + unit // 2) % pairs) * 2 + (col + unit) % 2

    def unit_of(slot):
        return ((slot // 2 - col // 2 + pairs) % pairs) * 2 + (slot + col) % 2

    copy_p = pltpu.make_async_copy(panel_hbm, pv, local_sem.at[0])
    copy_u = pltpu.make_async_copy(u_hbm.at[:, col], uv, local_sem.at[1])
    copy_t = pltpu.make_async_copy(table_hbm, table, local_sem.at[2])
    copy_a = pltpu.make_async_copy(a_hbm, av, local_sem.at[3])
    copy_k = pltpu.make_async_copy(k_hbm, kv, local_sem.at[2])
    copy_p.start()
    copy_u.start()
    copy_t.start()
    copy_a.start()

    barrier = pltpu.get_barrier_semaphore()

    def greet(axis, there):
        pl.semaphore_signal(barrier, inc=1, device_id={axis: there}, device_id_type=pl.DeviceIdType.MESH)

    for unit in range(1, n_cols):
        greet("pcol", peer(unit))
    greet("prow", mate)
    greet("prow", jnp.where(is_end, over, far))

    @pl.when(is_inner)
    def _():
        greet("prow", over)

    def panel_copy(unit, source):
        return remote(
            pv.at[:, peer(unit)], pr.at[source], p_send.at[0], p_recv.at[unit - 1], {"pcol": peer(unit)}
        )

    def pick_copy(unit, source):
        return remote(
            pick_out.at[unit - 1], picks.at[source], a_send.at[0], a_recv.at[unit - 1], {"pcol": peer(unit)}
        )

    def base(group):
        return (group + 1) * n_cols if group else 0

    all_mate = 4 * n_cols

    def chunk_copy(group, unit, chunk, index, there):
        block = gather[group].at[unit, chunk]
        return remote(block, block, g_send.at[0], g_recv.at[index], {"prow": there})

    def arrived(view, sem):
        remote(view, view, sem, sem, {"prow": mate}).wait_recv()

    def drain(view, sem):
        remote(view, view, sem, sem, {"prow": mate}).wait_send()

    def scale(unit):
        slot = peer(unit)
        if unit == 0:
            left = (pv[0, col], pv[1, col])
        else:
            panel_copy(unit, slot).wait_recv()
            left = (pr[slot, 0], pr[slot, 1])
        real, imag = cdot(left, (uv[0], uv[1]))
        live = (jnp.full((1, width), table[col, slot]) >= 0).astype(F32)
        packed = []
        for a, b in zip(tiles_of(real * live), tiles_of(imag * live)):
            packed.extend(cross(a, b))
        for group in groups:
            lo, hi = spans[group]
            for tile in range(lo, hi):
                at = (tile - lo) * LANES
                gather[group][unit, row, :, at : at + LANES] = packed[tile].astype(BF16)

    def send_over(group, unit):
        index = base(group) + unit if group else unit + jnp.where(is_end, n_cols, 0)
        chunk_copy(group, unit, row, index, over).start()

    def send_mate(group, unit):
        chunk_copy(group, unit, row, jnp.where(is_end, all_mate, base(group) + unit), mate).start()

    def pick(unit):
        node = peer(unit)
        top = jnp.full((1, width), table[node, row]) - row * row_blocks
        side = jnp.full((1, width), table[node, col]) - col * col_blocks
        for plane in range(2):
            total = None
            for i in range(row_blocks):
                for j in range(col_blocks):
                    keep = ((top == i) & (side == j)).astype(F32).astype(BF16)
                    block = av[plane, i * width : (i + 1) * width, j * width : (j + 1) * width] * keep
                    total = block if total is None else total + block
            if unit == 0:
                picks[col, plane] = total
            else:
                pick_out[unit - 1, plane] = total

    with scope("copies"):
        copy_p.wait()
        copy_u.wait()
        copy_t.wait()
    copy_k.start()
    with scope("scale0"):
        scale(0)
    with scope("barrier"):
        pl.semaphore_wait(barrier, n_cols + 2 - is_end.astype(jnp.int32))
    for unit in range(1, n_cols):
        panel_copy(unit, col).start()
    send_over(0, 0)
    send_mate(0, 0)
    with scope("scale1"):
        scale(1)
    send_over(0, 1)
    send_mate(0, 1)
    far_home = unit_of(far)
    early = jnp.where(far_home < 2, far_home, 0)
    for group in groups[1:]:
        send_over(group, early)

    @pl.when(is_end)
    def _():
        for group in groups[1:]:
            send_mate(group, early)

    @pl.when(is_inner)
    def _():
        for unit in range(2):
            for group in groups[1:]:
                send_mate(group, unit)

    with scope("copy_a"):
        copy_a.wait()
    for unit in list(range(2, n_cols)) + [1]:
        with scope(f"pick{unit}"):
            pick(unit)
        pick_copy(unit, col).start()
    pick(0)
    late = range(2, n_cols)
    order = [(group, 0) for group in groups[1:]] + [(group, i) for group in groups[1:] for i in range(1, n_cols)]

    def relay(unit, chunk, index):
        arrived(gather[0].at[unit, chunk], g_recv.at[index])
        chunk_copy(0, unit, chunk, unit, end).start()

    def relay_both(group, unit):
        index = base(group) + unit
        arrived(gather[group].at[unit, 0:2], g_recv.at[index])
        chunk_copy(group, unit, over, index, end).start()
        chunk_copy(group, unit, far, index, end).start()

    @pl.when(is_end)
    def _():
        for unit in late:
            with scope(f"scale{unit}"):
                scale(unit)
            send_over(0, unit)
            send_mate(0, unit)
        for group, i in order:
            unit = (far_home + i) % n_cols

            @pl.when(unit != early)
            def _():
                send_over(group, unit)
                send_mate(group, unit)

    @pl.when(is_inner)
    def _():
        with scope("relay_0o"):
            relay(0, over, 0)
        with scope("scale2"):
            scale(2)
        send_over(0, 2)
        send_mate(0, 2)
        with scope("relay_1o"):
            relay(1, over, 1)
        with scope("scale3"):
            scale(3)
        send_over(0, 3)
        send_mate(0, 3)
        with scope("relay_01f"):
            relay(0, far, n_cols)
            relay(1, far, n_cols + 1)
        for group, i in order:
            unit = (far_home + i) % n_cols

            @pl.when(unit != early)
            def _():
                send_over(group, unit)

        home = unit_of(end)

        @pl.when(home >= 2)
        def _():
            for group in groups[1:]:
                send_mate(group, home)

        for unit in late:
            with scope(f"relay_{unit}o"):
                relay(unit, over, unit)
            with scope(f"relay_{unit}f"):
                relay(unit, far, n_cols + unit)
        for group, i in order:
            if i == 1:
                for unit in late:

                    @pl.when(unit != home)
                    def _():
                        send_mate(group, unit)

            with scope(f"relay_g{group}_{i}"):
                relay_both(group, (home + i) % n_cols)
        with scope("mate"):
            arrived(picks.at[0], g_recv.at[all_mate])

    def ready(group, unit):
        @pl.when(is_end)
        def _():
            arrived(gather[group].at[unit, 0 : n_rows - 1], g_recv.at[base(group) + unit])

    def span(group):
        lo, hi = spans[group]
        return slice(lo * LANES, hi * LANES)

    def multiply(group, unit, start):
        right = gather[group][unit].reshape(width, gather[group].shape[-1])
        slot = peer(unit)
        for plane in range(2):
            value = jnp.dot(picks[slot, plane], right, preferred_element_type=F32)
            if start:
                acc[plane, :, span(group)] = value
            else:
                acc[plane, :, span(group)] += value

    home = unit_of(row)
    live = (jnp.full((1, LANES), table[col, row]) >= 0).astype(F32)
    named = jnp.full((1, LANES), table[col, row]) - row * row_blocks

    def pieces(group):
        return [(part, 1) for part in range(share)] if group == 0 else [(0, share)]

    def quad_copy(group, there, piece, source):
        part, count = piece
        at = (there - first) * share + part
        return remote(
            q_out[group].at[pl.ds(at, count)], q_in[group].at[source, part : part + count],
            d_send.at[0], q_recv.at[group + share - 1 if group else part], {"prow": there},
        )

    def quad(group):
        value = join(acc[0, :, span(group)], acc[1, :, span(group)])
        value = jnp.concatenate([x * live for x in tiles_of(value)], axis=1)
        acc[0, :, span(group)] = value
        low = value.astype(BF16)
        for there in (over, inner):
            top = there - first
            product = jnp.dot(z_t[top], low, preferred_element_type=F32)
            for part in range(share):
                at = part * LANES
                block = join(product[at : at + band_rows], product[at + band_rows : at + LANES])
                q_out[group][top * share + part] = block.astype(BF16)
                if there is inner:
                    own[group][part] = block

            if there is over:
                quad_copy(group, over, pieces(group)[0], row).start()

        for number, piece in enumerate(pieces(group)):
            if number > 0:
                quad_copy(group, over, piece, row).start()

            @pl.when(is_end)
            def _():
                quad_copy(group, mate, piece, row).start()

    for unit in range(n_cols):
        with scope(f"ready_g0_{unit}"):
            ready(0, unit)
        if unit == n_cols - 1:
            with scope("ready_home"):
                for group in groups[1:]:
                    ready(group, home)
            for group in groups:
                turned = gather[group][home].reshape(width, gather[group].shape[-1]).T
                for tile in range(*spans[group]):
                    at = (tile - spans[group][0]) * LANES
                    to = (tile % share) * LANES
                    z_t[tile // share, to : to + LANES, :] = turned[at : at + LANES]
        with scope(f"wpick_{unit}"):
            if unit > 0:
                pick_copy(unit, peer(unit)).wait_recv()
        multiply(0, unit, unit == 0)
    with scope("quad0"):
        quad(0)
    for group in groups[1:]:
        for i in range(n_cols):
            unit = (home + i) % n_cols
            if i > 0:
                with scope(f"ready_g{group}_{i}"):
                    ready(group, unit)
            multiply(group, unit, i == 0)
        with scope(f"quad{group}"):
            quad(group)

    for pair in range(width // LANES):
        at = 2 * pair * LANES
        planes = cross(acc[0, :, at : at + LANES], acc[0, :, at + LANES : at + 2 * LANES])
        columns = slice(pair * LANES, (pair + 1) * LANES)
        for i in range(row_blocks):
            keep = -(named == i).astype(F32)
            for plane in range(2):
                sel_out[plane, i * width : (i + 1) * width, columns] = planes[plane] * keep
    copy_k.wait()
    drain(pr.at[0 : n_cols - 1], p_send.at[0])
    drain(pick_out, a_send.at[0])

    @pl.when(is_inner)
    def _():
        drain(picks, g_send.at[0])

    @pl.when(is_end)
    def _():
        drain(picks.at[0:2], g_send.at[0])
        drain(picks.at[0], d_send.at[0])

    def total_copy(group, piece, there):
        part, count = piece
        block = tot[group].at[pl.ds((row - first) * share + part, count)]
        return remote(block, block, d_send.at[0], t_recv.at[group * 2 + row - first], {"prow": there})

    where_tile = {tile: group for group in groups for tile in range(*spans[group])}

    def tile_of(tile, band):
        group = where_tile[tile]
        at = (tile - spans[group][0]) * LANES
        return tot[group][band, :, at : at + LANES].astype(F32)

    def finish(pair, owner):
        columns = slice(pair * LANES, (pair + 1) * LANES)
        for part in range(share):
            band = owner * share + part
            rows = pl.ds(pl.multiple_of(band * band_rows, band_rows), band_rows)
            planes = cross(tile_of(2 * pair, band), tile_of(2 * pair + 1, band))
            for plane in range(2):
                diag_out[plane, 0, rows, columns] = kv[plane, 0, rows, columns] + planes[plane]

    @pl.when(is_inner)
    def _():
        for group in groups:
            for piece in pieces(group):
                part, count = piece
                with scope(f"wq{group}_{part}"):
                    arrived(
                        q_in[group].at[0 : n_rows - 1, part : part + count],
                        q_recv.at[group + share - 1 if group else part],
                    )
                for at in range(part, part + count):
                    total = own[group][at]
                    for source in (over, end, far):
                        total = total + q_in[group][source, at].astype(F32)
                    tot[group][(row - first) * share + at] = total.astype(BF16)
                total_copy(group, piece, far).start()
                total_copy(group, piece, end).start()
        for group in groups:
            total_copy(group, (0, share), over).start()
        for pair in range(width // LANES):
            finish(pair, row - first)

    def total_wait(group, owner):
        arrived(tot[group].at[0:share], t_recv.at[group * 2 + owner])

    @pl.when(is_end)
    def _():
        for group in groups:
            for there in (inner, over):
                with scope(f"wt{group}"):
                    total_wait(group, there - first)
                if group != 1:
                    finish(1 if group else 0, there - first)

    @pl.when(is_inner)
    def _():
        for group in groups:
            with scope(f"wt{group}"):
                total_wait(group, over - first)
        for pair in range(width // LANES):
            finish(pair, over - first)
        drain(picks.at[0:2], d_send.at[0])


def place(sel, diag, sel_out, diag_out, out_sem):
    copies = [
        pltpu.make_async_copy(sel, sel_out, out_sem.at[0]),
        pltpu.make_async_copy(diag, diag_out, out_sem.at[1]),
    ]
    for copy in copies:
        copy.start()
    for copy in copies:
        copy.wait()


def compact(ainv_anc, panel, u_inv, k_inv, structure):
    n_rows, n_cols = lax.axis_size("prow"), lax.axis_size("pcol")
    width, part = u_inv.shape[-1], panel.shape[2]
    row_blocks = ainv_anc.shape[1] // width
    tiles = 2 * width // LANES
    share = tiles // 2
    spans = ((0, share), (share, share + share // 2), (share + share // 2, tiles))
    hbm = pl.BlockSpec(memory_space=pltpu.HBM)
    vmem = pl.BlockSpec(memory_space=pltpu.VMEM)
    dma = pltpu.SemaphoreType.DMA
    shapes = (
        jax.ShapeDtypeStruct((2, row_blocks * width, width), F32),
        jax.ShapeDtypeStruct(k_inv.shape, F32),
    )

    def per_group(lead, rows, kind):
        return [pltpu.VMEM(lead + (rows, (hi - lo) * LANES), kind) for lo, hi in spans]

    band_rows = LANES // 2
    results = pl.pallas_call(
        functools.partial(kernel, n_rows, n_cols, spans),
        out_shape=tuple(pltpu.VMEM(s.shape, s.dtype) for s in shapes),
        in_specs=[hbm, hbm, hbm, hbm, hbm],
        out_specs=(vmem, vmem),
        scratch_shapes=[
            pltpu.SMEM(structure.shape, jnp.int32),
            pltpu.VMEM(ainv_anc.shape, BF16),
            pltpu.VMEM(panel.shape, BF16),
            pltpu.VMEM((2, width, width), BF16),
            pltpu.VMEM((n_cols, 2, part, width), BF16),
            pltpu.VMEM((n_cols - 1, 2, width, width), BF16),
            pltpu.VMEM((n_cols, 2, width, width), BF16),
            pltpu.VMEM((2, width, 2 * width), F32),
            pltpu.VMEM(k_inv.shape, F32),
            pltpu.VMEM((2, width, width), BF16),
            *per_group((n_cols, n_rows), part, BF16),
            *per_group((share,), band_rows, F32),
            *per_group((tiles,), band_rows, BF16),
            *per_group((n_rows, share), band_rows, BF16),
            *per_group((tiles,), band_rows, BF16),
            dma((4,)),
            dma((1,)),
            dma((n_cols - 1,)),
            dma((1,)),
            dma((n_cols - 1,)),
            dma((1,)),
            dma((4 * n_cols + 1,)),
            dma((1,)),
            dma((share + 2,)),
            dma((6,)),
        ],
        compiler_params=pltpu.CompilerParams(
            collective_id=0, has_side_effects=True
        ),
    )(ainv_anc, panel, u_inv, k_inv, structure)
    return pl.pallas_call(
        place,
        out_shape=shapes,
        in_specs=[vmem, vmem],
        out_specs=(hbm, hbm),
        scratch_shapes=[dma((2,))],
    )(*[pltpu.with_memory_space_constraint(x, pltpu.VMEM) for x in results])


def complex_quad(z_part, s_part):
    highest = lax.Precision.HIGHEST

    def single(left, right):
        return jnp.einsum("kra,rkb->kab", left, right, precision=highest)

    real = single(z_part[0], s_part[0]) - single(z_part[1], s_part[1])
    imag = single(z_part[0], s_part[1]) + single(z_part[1], s_part[0])
    return jnp.stack([real, imag])


def local(ainv_anc, panel, u_inv, k_inv, structure):
    block_width = u_inv.shape[-1]
    cols = lax.axis_size("pcol")
    if (
        structure.shape[1] == cols
        and lax.axis_size("prow") == cols
        and ainv_anc.shape[1] == ainv_anc.shape[2]
        and u_inv.shape[1] == cols
        and cols // 2 == 2
        and cols % 2 == 0
        and block_width == 2 * LANES
    ):
        return compact(ainv_anc, panel, u_inv, k_inv, structure)
    total_k = u_inv.shape[1]
    own_k = k_inv.shape[1]
    n_cols = lax.axis_size("pcol")
    row_here = lax.axis_index("prow")
    col_here = lax.axis_index("pcol")
    row_blocks = ainv_anc.shape[1] // block_width
    group_blocks = ainv_anc.shape[2] // block_width
    group_slots = structure.shape[1] // n_cols
    rows_all = row_blocks * block_width
    col_struct = lax.dynamic_slice_in_dim(structure, col_here * group_slots, group_slots, 1)
    slot_live = col_struct >= 0
    slot_pos = col_struct - col_here * group_blocks
    first_block = row_here * row_blocks
    target = first_block + jnp.arange(row_blocks, dtype=jnp.int32)
    rows_in = lax.all_gather(panel, "prow", axis=2, tiled=True)

    def single(left, right):
        return jnp.einsum("knb,kbc->knc", left, right, preferred_element_type=jnp.float32)

    real = single(rows_in[0], u_inv[0]) - single(rows_in[1], u_inv[1])
    imag = single(rows_in[0], u_inv[1]) + single(rows_in[1], u_inv[0])
    placed = jnp.stack([real, imag]).astype(jnp.bfloat16)
    placed = placed.reshape(2, total_k, group_slots, block_width, block_width)
    placed = jnp.where(slot_live[None, :, :, None, None], placed, jnp.zeros((), jnp.bfloat16))
    block_ids = jnp.arange(group_blocks, dtype=jnp.int32)
    pick_table = (slot_pos[:, :, None] == block_ids[None, None, :]).astype(jnp.bfloat16)
    ainv_blocks = ainv_anc.reshape(2, rows_all, group_blocks, block_width)

    def one_node(items):
        table_k, rows_k = items
        picked = jnp.einsum(
            "sg,cigw->cisw", table_k, ainv_blocks, preferred_element_type=jnp.float32
        )
        picked = picked.astype(jnp.bfloat16).reshape(2, rows_all, group_slots * block_width)
        right = rows_k.reshape(2, group_slots * block_width, block_width)
        real = jnp.dot(picked[0], right[0], preferred_element_type=jnp.float32) - jnp.dot(
            picked[1], right[1], preferred_element_type=jnp.float32
        )
        imag = jnp.dot(picked[0], right[1], preferred_element_type=jnp.float32) + jnp.dot(
            picked[1], right[0], preferred_element_type=jnp.float32
        )
        return jnp.stack([real, imag])

    per_node = lax.map(one_node, (pick_table, jnp.moveaxis(placed, 1, 0)))
    partial_value = jnp.transpose(per_node, (1, 2, 0, 3))
    row_table = (col_struct[:, None, :] == target[None, :, None]).astype(jnp.bfloat16)
    z_rows = jnp.einsum("kts,ckswb->cktwb", row_table, placed, preferred_element_type=jnp.float32)
    z_rows = z_rows.astype(jnp.bfloat16).reshape(2, total_k, rows_all, block_width)
    summed = lax.psum_scatter(
        partial_value.reshape(2, rows_all, total_k * block_width),
        "pcol",
        scatter_dimension=2,
        tiled=True,
    )
    own_struct = lax.dynamic_slice_in_dim(structure, col_here * own_k, own_k, 0)
    member = jnp.any(own_struct[:, :, None] == target[None, None, :], axis=1)
    selected = -summed.reshape(2, row_blocks, block_width, own_k, block_width)
    selected = jnp.where(member.T[None, :, None, :, None], selected, 0.0)
    sel_inv = selected.reshape(2, rows_all, own_k * block_width)
    received = lax.all_to_all(z_rows, "pcol", split_axis=1, concat_axis=1, tiled=True)
    z_own = (
        received.astype(jnp.float32).reshape(2, n_cols, own_k, rows_all, block_width).sum(axis=1)
    )
    quad_term = complex_quad(z_own, selected.reshape(2, rows_all, own_k, block_width))
    total_sum = lax.psum(quad_term, "prow")
    diag_inv = k_inv - total_sum
    return (sel_inv, diag_inv)


def solution(mesh):
    placed = (
        P(None, ("pole", "prow"), "pcol"),
        P(None, "pole", ("pcol", "prow"), None),
        P(None, "pole", None, None),
        P(None, ("pole", "pcol"), None, None),
        P(),
    )
    return jax.shard_map(
        local,
        mesh=mesh,
        in_specs=placed,
        out_specs=(P(None, ("pole", "prow"), "pcol"), P(None, ("pole", "pcol"), None, None)),
        check_vma=False,
    )
```

```python
import functools

import jax
import jax.numpy as jnp
from jax import lax
from jax.experimental import pallas as pl
from jax.experimental.pallas import tpu as pltpu
from jax.sharding import PartitionSpec as P

BF16 = jnp.bfloat16
F32 = jnp.float32
LANES = 128
scope = jax.named_scope


def cdot(left, right, dims=(((1,), (0,)), ((), ()))):
    def single(x, y):
        return lax.dot_general(x, y, dims, preferred_element_type=F32)

    real = single(left[0], right[0]) - single(left[1], right[1])
    imag = single(left[0], right[1]) + single(left[1], right[0])
    return real, imag


def remote(src, dst, send_sem, recv_sem, where):
    return pltpu.make_async_remote_copy(
        src_ref=src,
        dst_ref=dst,
        send_sem=send_sem,
        recv_sem=recv_sem,
        device_id=where,
        device_id_type=pl.DeviceIdType.MESH,
    )


def swap(x):
    return pltpu.roll(x, x.shape[1] // 2, 1)


def low_lanes():
    return lax.broadcasted_iota(jnp.int32, (1, LANES), 1) < LANES // 2


def tiles_of(x):
    return [x[:, at : at + LANES] for at in range(0, x.shape[1], LANES)]


def join(left, right):
    sign = jnp.where(low_lanes(), -1.0, 1.0)
    return jnp.concatenate([a + swap(b) * sign for a, b in zip(tiles_of(left), tiles_of(right))], axis=1)


def cross(a, b):
    low = low_lanes()
    return jnp.where(low, a, swap(b)), jnp.where(low, swap(a), b)


def kernel(
    n_rows, n_cols, spans, a_hbm, panel_hbm, u_hbm, k_hbm, table_hbm, sel_out, diag_out,
    table, av, pv, uv, pr, pick_out, picks, acc, kv, z_t,
    gather_0, gather_1, gather_2, own_0, own_1, own_2, out_0, out_1, out_2,
    in_0, in_1, in_2, tot_0, tot_1, tot_2,
    local_sem, p_send, p_recv, a_send, a_recv, g_send, g_recv, d_send, q_recv, t_recv,
):
    gather, own = (gather_0, gather_1, gather_2), (own_0, own_1, own_2)
    q_out, q_in, tot = (out_0, out_1, out_2), (in_0, in_1, in_2), (tot_0, tot_1, tot_2)
    groups = range(len(spans))
    row = lax.axis_index("prow")
    col = lax.axis_index("pcol")
    width = u_hbm.shape[-1]
    pairs = n_cols // 2
    row_blocks = a_hbm.shape[1] // width
    col_blocks = a_hbm.shape[2] // width
    band_rows = LANES // 2
    share = q_in[0].shape[1]
    first = n_rows // 2 - 1
    mate = row + 1 - 2 * (row % 2)
    is_end = (row == 0) | (row == n_rows - 1)
    is_inner = jnp.logical_not(is_end)
    end = jnp.where(is_end, row, mate)
    inner = jnp.where(is_end, mate, row)
    over = n_rows - 1 - inner
    far = n_rows - 1 - end

    def peer(unit):
        return ((col // 2 + unit // 2) % pairs) * 2 + (col + unit) % 2

    def unit_of(slot):
        return ((slot // 2 - col // 2 + pairs) % pairs) * 2 + (slot + col) % 2

    copy_p = pltpu.make_async_copy(panel_hbm, pv, local_sem.at[0])
    copy_u = pltpu.make_async_copy(u_hbm.at[:, col], uv, local_sem.at[1])
    copy_t = pltpu.make_async_copy(table_hbm, table, local_sem.at[2])
    copy_a = pltpu.make_async_copy(a_hbm, av, local_sem.at[3])
    copy_k = pltpu.make_async_copy(k_hbm, kv, local_sem.at[2])
    copy_p.start()
    copy_u.start()
    copy_t.start()
    copy_a.start()

    barrier = pltpu.get_barrier_semaphore()

    def greet(axis, there):
        pl.semaphore_signal(barrier, inc=1, device_id={axis: there}, device_id_type=pl.DeviceIdType.MESH)

    for unit in range(1, n_cols):
        greet("pcol", peer(unit))
    greet("prow", mate)
    greet("prow", jnp.where(is_end, over, far))

    @pl.when(is_inner)
    def _():
        greet("prow", over)

    def panel_copy(unit, source):
        return remote(
            pv.at[:, peer(unit)], pr.at[source], p_send.at[0], p_recv.at[unit - 1], {"pcol": peer(unit)}
        )

    def pick_copy(unit, source):
        return remote(
            pick_out.at[unit - 1], picks.at[source], a_send.at[0], a_recv.at[unit - 1], {"pcol": peer(unit)}
        )

    def base(group):
        return (group + 1) * n_cols if group else 0

    all_mate = 4 * n_cols

    def chunk_copy(group, unit, chunk, index, there):
        block = gather[group].at[unit, chunk]
        return remote(block, block, g_send.at[0], g_recv.at[index], {"prow": there})

    def arrived(view, sem):
        remote(view, view, sem, sem, {"prow": mate}).wait_recv()

    def drain(view, sem):
        remote(view, view, sem, sem, {"prow": mate}).wait_send()

    def scale(unit):
        slot = peer(unit)
        if unit == 0:
            left = (pv[0, col], pv[1, col])
        else:
            panel_copy(unit, slot).wait_recv()
            left = (pr[slot, 0], pr[slot, 1])
        real, imag = cdot(left, (uv[0], uv[1]))
        live = (jnp.full((1, width), table[col, slot]) >= 0).astype(F32)
        packed = []
        for a, b in zip(tiles_of(real * live), tiles_of(imag * live)):
            packed.extend(cross(a, b))
        for group in groups:
            lo, hi = spans[group]
            for tile in range(lo, hi):
                at = (tile - lo) * LANES
                gather[group][unit, row, :, at : at + LANES] = packed[tile].astype(BF16)

    def send_over(group, unit):
        index = base(group) + unit if group else unit + jnp.where(is_end, n_cols, 0)
        chunk_copy(group, unit, row, index, over).start()

    def send_mate(group, unit):
        chunk_copy(group, unit, row, jnp.where(is_end, all_mate, base(group) + unit), mate).start()

    def pick(unit):
        node = peer(unit)
        top = jnp.full((1, width), table[node, row]) - row * row_blocks
        side = jnp.full((1, width), table[node, col]) - col * col_blocks
        for plane in range(2):
            total = None
            for i in range(row_blocks):
                for j in range(col_blocks):
                    keep = ((top == i) & (side == j)).astype(F32).astype(BF16)
                    block = av[plane, i * width : (i + 1) * width, j * width : (j + 1) * width] * keep
                    total = block if total is None else total + block
            if unit == 0:
                picks[col, plane] = total
            else:
                pick_out[unit - 1, plane] = total

    with scope("copies"):
        copy_p.wait()
        copy_u.wait()
        copy_t.wait()
    copy_k.start()
    with scope("scale0"):
        scale(0)
    with scope("barrier"):
        pl.semaphore_wait(barrier, n_cols + 2 - is_end.astype(jnp.int32))
    for unit in range(1, n_cols):
        panel_copy(unit, col).start()
    send_over(0, 0)
    send_mate(0, 0)
    with scope("scale1"):
        scale(1)
    send_over(0, 1)
    send_mate(0, 1)
    far_home = unit_of(far)
    early = jnp.where(far_home < 2, far_home, 0)
    for group in groups[1:]:
        send_over(group, early)

    @pl.when(is_end)
    def _():
        for group in groups[1:]:
            send_mate(group, early)

    @pl.when(is_inner)
    def _():
        for unit in range(2):
            for group in groups[1:]:
                send_mate(group, unit)

    with scope("copy_a"):
        copy_a.wait()
    for unit in list(range(2, n_cols)) + [1]:
        with scope(f"pick{unit}"):
            pick(unit)
        pick_copy(unit, col).start()
    pick(0)
    late = range(2, n_cols)
    order = [(group, 0) for group in groups[1:]] + [(group, i) for group in groups[1:] for i in range(1, n_cols)]

    def relay(unit, chunk, index):
        arrived(gather[0].at[unit, chunk], g_recv.at[index])
        chunk_copy(0, unit, chunk, unit, end).start()

    def relay_both(group, unit):
        index = base(group) + unit
        arrived(gather[group].at[unit, 0:2], g_recv.at[index])
        chunk_copy(group, unit, over, index, end).start()
        chunk_copy(group, unit, far, index, end).start()

    @pl.when(is_end)
    def _():
        for unit in late:
            with scope(f"scale{unit}"):
                scale(unit)
            send_over(0, unit)
            send_mate(0, unit)
        for group, i in order:
            unit = (far_home + i) % n_cols

            @pl.when(unit != early)
            def _():
                send_over(group, unit)
                send_mate(group, unit)

    @pl.when(is_inner)
    def _():
        with scope("relay_0o"):
            relay(0, over, 0)
        with scope("scale2"):
            scale(2)
        send_over(0, 2)
        send_mate(0, 2)
        with scope("relay_1o"):
            relay(1, over, 1)
        with scope("scale3"):
            scale(3)
        send_over(0, 3)
        send_mate(0, 3)
        with scope("relay_01f"):
            relay(0, far, n_cols)
            relay(1, far, n_cols + 1)
        for group, i in order:
            unit = (far_home + i) % n_cols

            @pl.when(unit != early)
            def _():
                send_over(group, unit)

        home = unit_of(end)

        @pl.when(home >= 2)
        def _():
            for group in groups[1:]:
                send_mate(group, home)

        for unit in late:
            with scope(f"relay_{unit}o"):
                relay(unit, over, unit)
            with scope(f"relay_{unit}f"):
                relay(unit, far, n_cols + unit)
        for group, i in order:
            if i == 1:
                for unit in late:

                    @pl.when(unit != home)
                    def _():
                        send_mate(group, unit)

            with scope(f"relay_g{group}_{i}"):
                relay_both(group, (home + i) % n_cols)
        with scope("mate"):
            arrived(picks.at[0], g_recv.at[all_mate])

    def ready(group, unit):
        @pl.when(is_end)
        def _():
            arrived(gather[group].at[unit, 0 : n_rows - 1], g_recv.at[base(group) + unit])

    def span(group):
        lo, hi = spans[group]
        return slice(lo * LANES, hi * LANES)

    def multiply(group, unit, start):
        right = gather[group][unit].reshape(width, gather[group].shape[-1])
        slot = peer(unit)
        for plane in range(2):
            value = jnp.dot(picks[slot, plane], right, preferred_element_type=F32)
            if start:
                acc[plane, :, span(group)] = value
            else:
                acc[plane, :, span(group)] += value

    home = unit_of(row)
    named = jnp.full((1, LANES), table[col, row]) - row * row_blocks

    def pieces(group):
        return [(0, share)] if group == 1 else [(part, 1) for part in range(share)]

    def slot_of(group, part):
        return (0, share, share + 1)[group] + part

    def quad_copy(group, there, piece):
        part, count = piece
        at = part if there is over else share + part
        return remote(
            q_out[group].at[at : at + count], q_in[group].at[row, part : part + count],
            d_send.at[0], q_recv.at[slot_of(group, part)], {"prow": there},
        )

    def quad(group, unit):
        right = gather[group][unit].reshape(width, gather[group].shape[-1])
        slot = peer(unit)
        sums = [
            acc[plane, :, span(group)] + jnp.dot(picks[slot, plane], right, preferred_element_type=F32)
            for plane in range(2)
        ]
        value = join(*sums)
        product = jnp.dot(z_t[...].reshape(2 * width, width), value.astype(BF16), preferred_element_type=F32)
        for piece in pieces(group):
            for half in range(2):
                for part in range(piece[0], piece[0] + piece[1]):
                    at = (half * share + part) * LANES
                    block = join(product[at : at + band_rows], product[at + band_rows : at + LANES])
                    q_out[group][half * share + part] = block.astype(BF16)
                    if half:
                        own[group][part] = block
                if half:

                    @pl.when(is_end)
                    def _():
                        quad_copy(group, mate, piece).start()

                else:
                    quad_copy(group, over, piece).start()

        acc[0, :, span(group)] = value

    for unit in range(n_cols):
        with scope(f"ready_g0_{unit}"):
            ready(0, unit)
        if unit == n_cols - 1:
            with scope("ready_home"):
                for group in groups[1:]:
                    ready(group, home)
            for group in groups:
                turned = gather[group][home].reshape(width, gather[group].shape[-1]).T
                for tile in range(*spans[group]):
                    at = (tile - spans[group][0]) * LANES
                    to = (tile % share) * LANES
                    part = jnp.where(over - first == tile // share, 0, 1)
                    z_t[part, to : to + LANES, :] = turned[at : at + LANES]
        with scope(f"wpick_{unit}"):
            if unit > 0:
                pick_copy(unit, peer(unit)).wait_recv()
        if unit < n_cols - 1:
            multiply(0, unit, unit == 0)
    with scope("quad0"):
        quad(0, n_cols - 1)
    for group in groups[1:]:
        for i in range(n_cols):
            unit = (home + i) % n_cols
            if i > 0:
                with scope(f"ready_g{group}_{i}"):
                    ready(group, unit)
            if i < n_cols - 1:
                multiply(group, unit, i == 0)
        with scope(f"quad{group}"):
            quad(group, unit)

    for pair in range(width // LANES):
        at = 2 * pair * LANES
        planes = cross(acc[0, :, at : at + LANES], acc[0, :, at + LANES : at + 2 * LANES])
        columns = slice(pair * LANES, (pair + 1) * LANES)
        for i in range(row_blocks):
            keep = -(named == i).astype(F32)
            for plane in range(2):
                sel_out[plane, i * width : (i + 1) * width, columns] = planes[plane] * keep
    copy_k.wait()
    drain(pr.at[0 : n_cols - 1], p_send.at[0])
    drain(pick_out, a_send.at[0])

    @pl.when(is_inner)
    def _():
        drain(picks, g_send.at[0])

    @pl.when(is_end)
    def _():
        drain(picks.at[0:2], g_send.at[0])
        drain(picks.at[0], d_send.at[0])

    def total_copy(group, piece, there):
        part, count = piece
        block = tot[group].at[pl.ds((row - first) * share + part, count)]
        return remote(block, block, d_send.at[0], t_recv.at[group * 2 + row - first], {"prow": there})

    where_tile = {tile: group for group in groups for tile in range(*spans[group])}

    def tile_of(tile, band):
        group = where_tile[tile]
        at = (tile - spans[group][0]) * LANES
        return tot[group][band, :, at : at + LANES].astype(F32)

    def finish(pair, owner):
        columns = slice(pair * LANES, (pair + 1) * LANES)
        for part in range(share):
            band = owner * share + part
            rows = pl.ds(pl.multiple_of(band * band_rows, band_rows), band_rows)
            planes = cross(tile_of(2 * pair, band), tile_of(2 * pair + 1, band))
            for plane in range(2):
                diag_out[plane, 0, rows, columns] = kv[plane, 0, rows, columns] + planes[plane]

    @pl.when(is_inner)
    def _():
        for group in groups:
            for piece in pieces(group):
                part, count = piece
                with scope(f"wq{group}_{part}"):
                    arrived(
                        q_in[group].at[0 : n_rows - 1, part : part + count],
                        q_recv.at[slot_of(group, part)],
                    )
                for at in range(part, part + count):
                    total = own[group][at]
                    for source in (over, end, far):
                        total = total + q_in[group][source, at].astype(F32)
                    tot[group][(row - first) * share + at] = total.astype(BF16)
                total_copy(group, piece, far).start()
                total_copy(group, piece, end).start()
        for group in groups:
            total_copy(group, (0, share), over).start()
        for pair in range(width // LANES):
            finish(pair, row - first)

    def total_wait(group, owner):
        arrived(tot[group].at[0:share], t_recv.at[group * 2 + owner])

    @pl.when(is_end)
    def _():
        for group in groups:
            for there in (inner, over):
                with scope(f"wt{group}"):
                    total_wait(group, there - first)
                if group != 1:
                    finish(1 if group else 0, there - first)

    @pl.when(is_inner)
    def _():
        for group in groups:
            with scope(f"wt{group}"):
                total_wait(group, over - first)
        for pair in range(width // LANES):
            finish(pair, over - first)
        drain(picks.at[0:2], d_send.at[0])


def place(sel, diag, sel_out, diag_out, out_sem):
    copies = [
        pltpu.make_async_copy(sel, sel_out, out_sem.at[0]),
        pltpu.make_async_copy(diag, diag_out, out_sem.at[1]),
    ]
    for copy in copies:
        copy.start()
    for copy in copies:
        copy.wait()


def compact(ainv_anc, panel, u_inv, k_inv, structure):
    n_rows, n_cols = lax.axis_size("prow"), lax.axis_size("pcol")
    width, part = u_inv.shape[-1], panel.shape[2]
    row_blocks = ainv_anc.shape[1] // width
    tiles = 2 * width // LANES
    share = tiles // 2
    spans = ((0, share), (share, share + share // 2), (share + share // 2, tiles))
    hbm = pl.BlockSpec(memory_space=pltpu.HBM)
    vmem = pl.BlockSpec(memory_space=pltpu.VMEM)
    dma = pltpu.SemaphoreType.DMA
    shapes = (
        jax.ShapeDtypeStruct((2, row_blocks * width, width), F32),
        jax.ShapeDtypeStruct(k_inv.shape, F32),
    )

    def per_group(lead, rows, kind):
        return [pltpu.VMEM(lead + (rows, (hi - lo) * LANES), kind) for lo, hi in spans]

    band_rows = LANES // 2
    results = pl.pallas_call(
        functools.partial(kernel, n_rows, n_cols, spans),
        out_shape=tuple(pltpu.VMEM(s.shape, s.dtype) for s in shapes),
        in_specs=[hbm, hbm, hbm, hbm, hbm],
        out_specs=(vmem, vmem),
        scratch_shapes=[
            pltpu.SMEM(structure.shape, jnp.int32),
            pltpu.VMEM(ainv_anc.shape, BF16),
            pltpu.VMEM(panel.shape, BF16),
            pltpu.VMEM((2, width, width), BF16),
            pltpu.VMEM((n_cols, 2, part, width), BF16),
            pltpu.VMEM((n_cols - 1, 2, width, width), BF16),
            pltpu.VMEM((n_cols, 2, width, width), BF16),
            pltpu.VMEM((2, width, 2 * width), F32),
            pltpu.VMEM(k_inv.shape, F32),
            pltpu.VMEM((2, width, width), BF16),
            *per_group((n_cols, n_rows), part, BF16),
            *per_group((share,), band_rows, F32),
            *per_group((tiles,), band_rows, BF16),
            *per_group((n_rows, share), band_rows, BF16),
            *per_group((tiles,), band_rows, BF16),
            dma((4,)),
            dma((1,)),
            dma((n_cols - 1,)),
            dma((1,)),
            dma((n_cols - 1,)),
            dma((1,)),
            dma((4 * n_cols + 1,)),
            dma((1,)),
            dma((2 * share + 1,)),
            dma((6,)),
        ],
        compiler_params=pltpu.CompilerParams(
            collective_id=0, has_side_effects=True
        ),
    )(ainv_anc, panel, u_inv, k_inv, structure)
    return pl.pallas_call(
        place,
        out_shape=shapes,
        in_specs=[vmem, vmem],
        out_specs=(hbm, hbm),
        scratch_shapes=[dma((2,))],
    )(*[pltpu.with_memory_space_constraint(x, pltpu.VMEM) for x in results])


def complex_quad(z_part, s_part):
    highest = lax.Precision.HIGHEST

    def single(left, right):
        return jnp.einsum("kra,rkb->kab", left, right, precision=highest)

    real = single(z_part[0], s_part[0]) - single(z_part[1], s_part[1])
    imag = single(z_part[0], s_part[1]) + single(z_part[1], s_part[0])
    return jnp.stack([real, imag])


def local(ainv_anc, panel, u_inv, k_inv, structure):
    block_width = u_inv.shape[-1]
    cols = lax.axis_size("pcol")
    if (
        structure.shape[1] == cols
        and lax.axis_size("prow") == cols
        and ainv_anc.shape[1] == ainv_anc.shape[2]
        and u_inv.shape[1] == cols
        and cols // 2 == 2
        and cols % 2 == 0
        and block_width == 2 * LANES
    ):
        return compact(ainv_anc, panel, u_inv, k_inv, structure)
    total_k = u_inv.shape[1]
    own_k = k_inv.shape[1]
    n_cols = lax.axis_size("pcol")
    row_here = lax.axis_index("prow")
    col_here = lax.axis_index("pcol")
    row_blocks = ainv_anc.shape[1] // block_width
    group_blocks = ainv_anc.shape[2] // block_width
    group_slots = structure.shape[1] // n_cols
    rows_all = row_blocks * block_width
    col_struct = lax.dynamic_slice_in_dim(structure, col_here * group_slots, group_slots, 1)
    slot_live = col_struct >= 0
    slot_pos = col_struct - col_here * group_blocks
    first_block = row_here * row_blocks
    target = first_block + jnp.arange(row_blocks, dtype=jnp.int32)
    rows_in = lax.all_gather(panel, "prow", axis=2, tiled=True)

    def single(left, right):
        return jnp.einsum("knb,kbc->knc", left, right, preferred_element_type=jnp.float32)

    real = single(rows_in[0], u_inv[0]) - single(rows_in[1], u_inv[1])
    imag = single(rows_in[0], u_inv[1]) + single(rows_in[1], u_inv[0])
    placed = jnp.stack([real, imag]).astype(jnp.bfloat16)
    placed = placed.reshape(2, total_k, group_slots, block_width, block_width)
    placed = jnp.where(slot_live[None, :, :, None, None], placed, jnp.zeros((), jnp.bfloat16))
    block_ids = jnp.arange(group_blocks, dtype=jnp.int32)
    pick_table = (slot_pos[:, :, None] == block_ids[None, None, :]).astype(jnp.bfloat16)
    ainv_blocks = ainv_anc.reshape(2, rows_all, group_blocks, block_width)

    def one_node(items):
        table_k, rows_k = items
        picked = jnp.einsum(
            "sg,cigw->cisw", table_k, ainv_blocks, preferred_element_type=jnp.float32
        )
        picked = picked.astype(jnp.bfloat16).reshape(2, rows_all, group_slots * block_width)
        right = rows_k.reshape(2, group_slots * block_width, block_width)
        real = jnp.dot(picked[0], right[0], preferred_element_type=jnp.float32) - jnp.dot(
            picked[1], right[1], preferred_element_type=jnp.float32
        )
        imag = jnp.dot(picked[0], right[1], preferred_element_type=jnp.float32) + jnp.dot(
            picked[1], right[0], preferred_element_type=jnp.float32
        )
        return jnp.stack([real, imag])

    per_node = lax.map(one_node, (pick_table, jnp.moveaxis(placed, 1, 0)))
    partial_value = jnp.transpose(per_node, (1, 2, 0, 3))
    row_table = (col_struct[:, None, :] == target[None, :, None]).astype(jnp.bfloat16)
    z_rows = jnp.einsum("kts,ckswb->cktwb", row_table, placed, preferred_element_type=jnp.float32)
    z_rows = z_rows.astype(jnp.bfloat16).reshape(2, total_k, rows_all, block_width)
    summed = lax.psum_scatter(
        partial_value.reshape(2, rows_all, total_k * block_width),
        "pcol",
        scatter_dimension=2,
        tiled=True,
    )
    own_struct = lax.dynamic_slice_in_dim(structure, col_here * own_k, own_k, 0)
    member = jnp.any(own_struct[:, :, None] == target[None, None, :], axis=1)
    selected = -summed.reshape(2, row_blocks, block_width, own_k, block_width)
    selected = jnp.where(member.T[None, :, None, :, None], selected, 0.0)
    sel_inv = selected.reshape(2, rows_all, own_k * block_width)
    received = lax.all_to_all(z_rows, "pcol", split_axis=1, concat_axis=1, tiled=True)
    z_own = (
        received.astype(jnp.float32).reshape(2, n_cols, own_k, rows_all, block_width).sum(axis=1)
    )
    quad_term = complex_quad(z_own, selected.reshape(2, rows_all, own_k, block_width))
    total_sum = lax.psum(quad_term, "prow")
    diag_inv = k_inv - total_sum
    return (sel_inv, diag_inv)


def solution(mesh):
    placed = (
        P(None, ("pole", "prow"), "pcol"),
        P(None, "pole", ("pcol", "prow"), None),
        P(None, "pole", None, None),
        P(None, ("pole", "pcol"), None, None),
        P(),
    )
    return jax.shard_map(
        local,
        mesh=mesh,
        in_specs=placed,
        out_specs=(P(None, ("pole", "prow"), "pcol"), P(None, ("pole", "pcol"), None, None)),
        check_vma=False,
    )
```

```python
import functools

import jax
import jax.numpy as jnp
from jax import lax
from jax.experimental import pallas as pl
from jax.experimental.pallas import tpu as pltpu
from jax.sharding import PartitionSpec as P

BF16 = jnp.bfloat16
F32 = jnp.float32
LANES = 128
scope = jax.named_scope


def cdot(left, right, dims=(((1,), (0,)), ((), ()))):
    def single(x, y):
        return lax.dot_general(x, y, dims, preferred_element_type=F32)

    real = single(left[0], right[0]) - single(left[1], right[1])
    imag = single(left[0], right[1]) + single(left[1], right[0])
    return real, imag


def remote(src, dst, send_sem, recv_sem, where):
    return pltpu.make_async_remote_copy(
        src_ref=src,
        dst_ref=dst,
        send_sem=send_sem,
        recv_sem=recv_sem,
        device_id=where,
        device_id_type=pl.DeviceIdType.MESH,
    )


def swap(x):
    return pltpu.roll(x, x.shape[1] // 2, 1)


def low_lanes():
    return lax.broadcasted_iota(jnp.int32, (1, LANES), 1) < LANES // 2


def tiles_of(x):
    return [x[:, at : at + LANES] for at in range(0, x.shape[1], LANES)]


def join(left, right):
    sign = jnp.where(low_lanes(), -1.0, 1.0)
    return jnp.concatenate([a + swap(b) * sign for a, b in zip(tiles_of(left), tiles_of(right))], axis=1)


def cross(a, b):
    low = low_lanes()
    return jnp.where(low, a, swap(b)), jnp.where(low, swap(a), b)


def kernel(
    n_rows, n_cols, spans, a_hbm, panel_hbm, u_hbm, k_hbm, table_hbm, sel_out, diag_out,
    table, av, pv, uv, pr, pick_out, picks, acc, kv, z_t,
    gather_0, gather_1, gather_2, own_0, own_1, own_2, out_0, out_1, out_2,
    in_0, in_1, in_2, tot_0, tot_1, tot_2,
    d_send, q_recv, t_recv,
):
    gather, own = (gather_0, gather_1, gather_2), (own_0, own_1, own_2)
    q_out, q_in, tot = (out_0, out_1, out_2), (in_0, in_1, in_2), (tot_0, tot_1, tot_2)
    groups = range(len(spans))
    row = lax.axis_index("prow")
    col = lax.axis_index("pcol")
    width = u_hbm.shape[-1]
    pairs = n_cols // 2
    row_blocks = a_hbm.shape[1] // width
    col_blocks = a_hbm.shape[2] // width
    band_rows = LANES // 2
    share = q_in[0].shape[1]
    first = n_rows // 2 - 1
    mate = row + 1 - 2 * (row % 2)
    is_end = (row == 0) | (row == n_rows - 1)
    is_inner = jnp.logical_not(is_end)
    end = jnp.where(is_end, row, mate)
    inner = jnp.where(is_end, mate, row)
    over = n_rows - 1 - inner
    far = n_rows - 1 - end

    def peer(unit):
        return ((col // 2 + unit // 2) % pairs) * 2 + (col + unit) % 2

    def unit_of(slot):
        return ((slot // 2 - col // 2 + pairs) % pairs) * 2 + (slot + col) % 2

    def arrived(view, sem):
        remote(view, view, sem, sem, {"prow": mate}).wait_recv()

    def drain(view, sem):
        remote(view, view, sem, sem, {"prow": mate}).wait_send()

    def pieces(group):
        cuts = 1 if group else 2
        rows = band_rows // cuts
        return [(part, slice(cut * rows, (cut + 1) * rows)) for part in range(share) for cut in range(cuts)]

    def slot_of(group, piece):
        before = sum(len(pieces(other)) for other in range(group))
        return before + pieces(group).index(piece)

    def gathering(local_sem, p_send, p_recv, a_send, a_recv, g_send, g_recv):
        copy_p = pltpu.make_async_copy(panel_hbm, pv, local_sem.at[0])
        copy_u = pltpu.make_async_copy(u_hbm.at[:, col], uv, local_sem.at[1])
        copy_t = pltpu.make_async_copy(table_hbm, table, local_sem.at[2])
        copy_a = pltpu.make_async_copy(a_hbm, av, local_sem.at[3])
        copy_k = pltpu.make_async_copy(k_hbm, kv, local_sem.at[2])
        copy_p.start()
        copy_u.start()
        copy_t.start()
        copy_a.start()

        barrier = pltpu.get_barrier_semaphore()

        def greet(axis, there):
            pl.semaphore_signal(barrier, inc=1, device_id={axis: there}, device_id_type=pl.DeviceIdType.MESH)

        for unit in range(1, n_cols):
            greet("pcol", peer(unit))
        greet("prow", mate)
        greet("prow", jnp.where(is_end, over, far))

        @pl.when(is_inner)
        def _():
            greet("prow", over)

        def panel_copy(unit, source):
            return remote(
                pv.at[:, peer(unit)], pr.at[source], p_send.at[0], p_recv.at[unit - 1], {"pcol": peer(unit)}
            )

        def pick_copy(unit, source):
            return remote(
                pick_out.at[unit - 1], picks.at[source], a_send.at[0], a_recv.at[unit - 1], {"pcol": peer(unit)}
            )

        def base(group):
            return (group + 1) * n_cols if group else 0

        all_mate = 4 * n_cols

        def chunk_copy(group, unit, chunk, index, there):
            block = gather[group].at[unit, chunk]
            return remote(block, block, g_send.at[0], g_recv.at[index], {"prow": there})

        def scale(unit):
            slot = peer(unit)
            if unit == 0:
                left = (pv[0, col], pv[1, col])
            else:
                panel_copy(unit, slot).wait_recv()
                left = (pr[slot, 0], pr[slot, 1])
            real, imag = cdot(left, (uv[0], uv[1]))
            live = (jnp.full((1, width), table[col, slot]) >= 0).astype(F32)
            packed = []
            for a, b in zip(tiles_of(real * live), tiles_of(imag * live)):
                packed.extend(cross(a, b))
            for group in groups:
                lo, hi = spans[group]
                for tile in range(lo, hi):
                    at = (tile - lo) * LANES
                    gather[group][unit, row, :, at : at + LANES] = packed[tile].astype(BF16)

        def send_over(group, unit):
            index = base(group) + unit if group else unit + jnp.where(is_end, n_cols, 0)
            chunk_copy(group, unit, row, index, over).start()

        def send_mate(group, unit):
            chunk_copy(group, unit, row, jnp.where(is_end, all_mate, base(group) + unit), mate).start()

        def pick(unit):
            node = peer(unit)
            top = jnp.full((1, width), table[node, row]) - row * row_blocks
            side = jnp.full((1, width), table[node, col]) - col * col_blocks
            for plane in range(2):
                total = None
                for i in range(row_blocks):
                    for j in range(col_blocks):
                        keep = ((top == i) & (side == j)).astype(F32).astype(BF16)
                        block = av[plane, i * width : (i + 1) * width, j * width : (j + 1) * width] * keep
                        total = block if total is None else total + block
                if unit == 0:
                    picks[col, plane] = total
                else:
                    pick_out[unit - 1, plane] = total

        with scope("copies"):
            copy_p.wait()
            copy_u.wait()
            copy_t.wait()
        copy_k.start()
        with scope("scale0"):
            scale(0)
        with scope("barrier"):
            pl.semaphore_wait(barrier, n_cols + 2 - is_end.astype(jnp.int32))
        for unit in range(1, n_cols):
            panel_copy(unit, col).start()
        send_over(0, 0)
        send_mate(0, 0)
        with scope("scale1"):
            scale(1)
        send_over(0, 1)
        send_mate(0, 1)
        far_home = unit_of(far)
        early = jnp.where(far_home < 2, far_home, 0)
        for group in groups[1:]:
            send_over(group, early)

        @pl.when(is_end)
        def _():
            for group in groups[1:]:
                send_mate(group, early)

        @pl.when(is_inner)
        def _():
            for unit in range(2):
                for group in groups[1:]:
                    send_mate(group, unit)

        with scope("copy_a"):
            copy_a.wait()
        for unit in list(range(2, n_cols)) + [1]:
            with scope(f"pick{unit}"):
                pick(unit)
            pick_copy(unit, col).start()
        pick(0)
        late = range(2, n_cols)
        order = [(group, 0) for group in groups[1:]] + [(group, i) for group in groups[1:] for i in range(1, n_cols)]

        def relay(unit, chunk, index):
            arrived(gather[0].at[unit, chunk], g_recv.at[index])
            chunk_copy(0, unit, chunk, unit, end).start()

        def relay_both(group, unit):
            index = base(group) + unit
            arrived(gather[group].at[unit, 0:2], g_recv.at[index])
            chunk_copy(group, unit, over, index, end).start()
            chunk_copy(group, unit, far, index, end).start()

        @pl.when(is_end)
        def _():
            for unit in late:
                with scope(f"scale{unit}"):
                    scale(unit)
                send_over(0, unit)
                send_mate(0, unit)
            for group, i in order:
                unit = (far_home + i) % n_cols

                @pl.when(unit != early)
                def _():
                    send_over(group, unit)
                    send_mate(group, unit)

        @pl.when(is_inner)
        def _():
            with scope("relay_0o"):
                relay(0, over, 0)
            with scope("scale2"):
                scale(2)
            send_over(0, 2)
            send_mate(0, 2)
            with scope("relay_1o"):
                relay(1, over, 1)
            with scope("scale3"):
                scale(3)
            send_over(0, 3)
            send_mate(0, 3)
            with scope("relay_01f"):
                relay(0, far, n_cols)
                relay(1, far, n_cols + 1)
            for group, i in order:
                unit = (far_home + i) % n_cols

                @pl.when(unit != early)
                def _():
                    send_over(group, unit)

            home = unit_of(end)

            @pl.when(home >= 2)
            def _():
                for group in groups[1:]:
                    send_mate(group, home)

            for unit in late:
                with scope(f"relay_{unit}o"):
                    relay(unit, over, unit)
                with scope(f"relay_{unit}f"):
                    relay(unit, far, n_cols + unit)
            for group, i in order:
                if i == 1:
                    for unit in late:

                        @pl.when(unit != home)
                        def _():
                            send_mate(group, unit)

                with scope(f"relay_g{group}_{i}"):
                    relay_both(group, (home + i) % n_cols)
            with scope("mate"):
                arrived(picks.at[0], g_recv.at[all_mate])

        def ready(group, unit):
            @pl.when(is_end)
            def _():
                arrived(gather[group].at[unit, 0 : n_rows - 1], g_recv.at[base(group) + unit])

        def span(group):
            lo, hi = spans[group]
            return slice(lo * LANES, hi * LANES)

        def multiply(group, unit, start):
            right = gather[group][unit].reshape(width, gather[group].shape[-1])
            slot = peer(unit)
            for plane in range(2):
                value = jnp.dot(picks[slot, plane], right, preferred_element_type=F32)
                if start:
                    acc[plane, :, span(group)] = value
                else:
                    acc[plane, :, span(group)] += value

        home = unit_of(row)
        named = jnp.full((1, LANES), table[col, row]) - row * row_blocks

        def quad_copy(group, there, piece):
            part, rows = piece
            at = part if there is over else share + part
            return remote(
                q_out[group].at[at, rows], q_in[group].at[row, part, rows],
                d_send.at[0], q_recv.at[slot_of(group, piece)], {"prow": there},
            )

        def quad(group, unit):
            right = gather[group][unit].reshape(width, gather[group].shape[-1])
            slot = peer(unit)
            sums = [
                acc[plane, :, span(group)] + jnp.dot(picks[slot, plane], right, preferred_element_type=F32)
                for plane in range(2)
            ]
            value = join(*sums)
            product = jnp.dot(z_t[...].reshape(2 * width, width), value.astype(BF16), preferred_element_type=F32)
            for piece in pieces(group):
                for half in range(2):
                    part, rows = piece
                    at = (half * share + part) * LANES
                    upper = product[at + rows.start : at + rows.stop]
                    lower = product[at + band_rows + rows.start : at + band_rows + rows.stop]
                    block = join(upper, lower)
                    q_out[group][half * share + part, rows] = block.astype(BF16)
                    if half:
                        own[group][part, rows] = block
                    if half:

                        @pl.when(is_end)
                        def _():
                            quad_copy(group, mate, piece).start()

                    else:
                        quad_copy(group, over, piece).start()

            acc[0, :, span(group)] = value

        for unit in range(n_cols):
            with scope(f"ready_g0_{unit}"):
                ready(0, unit)
            if unit == n_cols - 1:
                with scope("ready_home"):
                    for group in groups[1:]:
                        ready(group, home)
                for group in groups:
                    turned = gather[group][home].reshape(width, gather[group].shape[-1]).T
                    for tile in range(*spans[group]):
                        at = (tile - spans[group][0]) * LANES
                        to = (tile % share) * LANES
                        part = jnp.where(over - first == tile // share, 0, 1)
                        z_t[part, to : to + LANES, :] = turned[at : at + LANES]
            with scope(f"wpick_{unit}"):
                if unit > 0:
                    pick_copy(unit, peer(unit)).wait_recv()
            if unit < n_cols - 1:
                multiply(0, unit, unit == 0)
        with scope("quad0"):
            quad(0, n_cols - 1)
        for group in groups[1:]:
            for i in range(n_cols):
                unit = (home + i) % n_cols
                if i > 0:
                    with scope(f"ready_g{group}_{i}"):
                        ready(group, unit)
                if i < n_cols - 1:
                    multiply(group, unit, i == 0)
            with scope(f"quad{group}"):
                quad(group, unit)

        for pair in range(width // LANES):
            at = 2 * pair * LANES
            planes = cross(acc[0, :, at : at + LANES], acc[0, :, at + LANES : at + 2 * LANES])
            columns = slice(pair * LANES, (pair + 1) * LANES)
            for i in range(row_blocks):
                keep = -(named == i).astype(F32)
                for plane in range(2):
                    sel_out[plane, i * width : (i + 1) * width, columns] = planes[plane] * keep
        copy_k.wait()
        drain(pr.at[0 : n_cols - 1], p_send.at[0])
        drain(pick_out, a_send.at[0])

        @pl.when(is_inner)
        def _():
            drain(picks, g_send.at[0])

        @pl.when(is_end)
        def _():
            drain(picks.at[0:2], g_send.at[0])
            drain(picks.at[0], d_send.at[0])

    dma = pltpu.SemaphoreType.DMA
    pl.run_scoped(
        gathering, dma((4,)), dma((1,)), dma((n_cols - 1,)), dma((1,)), dma((n_cols - 1,)), dma((1,)), dma((4 * n_cols + 1,))
    )

    def total_copy(group, piece, there):
        part, rows = piece
        block = tot[group].at[(row - first) * share + part, rows]
        return remote(block, block, d_send.at[0], t_recv.at[group * 2 + row - first], {"prow": there})

    where_tile = {tile: group for group in groups for tile in range(*spans[group])}

    def tile_of(tile, band):
        group = where_tile[tile]
        at = (tile - spans[group][0]) * LANES
        return tot[group][band, :, at : at + LANES].astype(F32)

    def finish(pair, owner):
        columns = slice(pair * LANES, (pair + 1) * LANES)
        for part in range(share):
            band = owner * share + part
            rows = pl.ds(pl.multiple_of(band * band_rows, band_rows), band_rows)
            planes = cross(tile_of(2 * pair, band), tile_of(2 * pair + 1, band))
            for plane in range(2):
                diag_out[plane, 0, rows, columns] = kv[plane, 0, rows, columns] + planes[plane]

    @pl.when(is_inner)
    def _():
        for group in groups:
            for piece in pieces(group):
                part, rows = piece
                with scope(f"wq{slot_of(group, piece)}"):
                    arrived(q_in[group].at[0 : n_rows - 1, part, rows], q_recv.at[slot_of(group, piece)])
                total = own[group][part, rows]
                for source in (over, end, far):
                    total = total + q_in[group][source, part, rows].astype(F32)
                tot[group][(row - first) * share + part, rows] = total.astype(BF16)
                total_copy(group, piece, far).start()
                total_copy(group, piece, end).start()
        for group in groups:
            for part in range(share):
                total_copy(group, (part, slice(0, band_rows)), over).start()
        for pair in range(width // LANES):
            finish(pair, row - first)

    def total_wait(group, owner):
        arrived(tot[group].at[0:share], t_recv.at[group * 2 + owner])

    @pl.when(is_end)
    def _():
        for group in groups:
            for there in (inner, over):
                with scope(f"wt{group}"):
                    total_wait(group, there - first)
                if group != 1:
                    finish(1 if group else 0, there - first)

    @pl.when(is_inner)
    def _():
        for group in groups:
            with scope(f"wt{group}"):
                total_wait(group, over - first)
        for pair in range(width // LANES):
            finish(pair, over - first)
        drain(picks.at[0:2], d_send.at[0])


def place(sel, diag, sel_out, diag_out, out_sem):
    copies = [
        pltpu.make_async_copy(sel, sel_out, out_sem.at[0]),
        pltpu.make_async_copy(diag, diag_out, out_sem.at[1]),
    ]
    for copy in copies:
        copy.start()
    for copy in copies:
        copy.wait()


def compact(ainv_anc, panel, u_inv, k_inv, structure):
    n_rows, n_cols = lax.axis_size("prow"), lax.axis_size("pcol")
    width, part = u_inv.shape[-1], panel.shape[2]
    row_blocks = ainv_anc.shape[1] // width
    tiles = 2 * width // LANES
    share = tiles // 2
    spans = ((0, share), (share, share + share // 2), (share + share // 2, tiles))
    hbm = pl.BlockSpec(memory_space=pltpu.HBM)
    vmem = pl.BlockSpec(memory_space=pltpu.VMEM)
    dma = pltpu.SemaphoreType.DMA
    shapes = (
        jax.ShapeDtypeStruct((2, row_blocks * width, width), F32),
        jax.ShapeDtypeStruct(k_inv.shape, F32),
    )

    def per_group(lead, rows, kind):
        return [pltpu.VMEM(lead + (rows, (hi - lo) * LANES), kind) for lo, hi in spans]

    band_rows = LANES // 2
    results = pl.pallas_call(
        functools.partial(kernel, n_rows, n_cols, spans),
        out_shape=tuple(pltpu.VMEM(s.shape, s.dtype) for s in shapes),
        in_specs=[hbm, hbm, hbm, hbm, hbm],
        out_specs=(vmem, vmem),
        scratch_shapes=[
            pltpu.SMEM(structure.shape, jnp.int32),
            pltpu.VMEM(ainv_anc.shape, BF16),
            pltpu.VMEM(panel.shape, BF16),
            pltpu.VMEM((2, width, width), BF16),
            pltpu.VMEM((n_cols, 2, part, width), BF16),
            pltpu.VMEM((n_cols - 1, 2, width, width), BF16),
            pltpu.VMEM((n_cols, 2, width, width), BF16),
            pltpu.VMEM((2, width, 2 * width), F32),
            pltpu.VMEM(k_inv.shape, F32),
            pltpu.VMEM((2, width, width), BF16),
            *per_group((n_cols, n_rows), part, BF16),
            *per_group((share,), band_rows, F32),
            *per_group((tiles,), band_rows, BF16),
            *per_group((n_rows, share), band_rows, BF16),
            *per_group((tiles,), band_rows, BF16),
            dma((1,)),
            dma((4 * share,)),
            dma((6,)),
        ],
        compiler_params=pltpu.CompilerParams(
            collective_id=0, has_side_effects=True
        ),
    )(ainv_anc, panel, u_inv, k_inv, structure)
    return pl.pallas_call(
        place,
        out_shape=shapes,
        in_specs=[vmem, vmem],
        out_specs=(hbm, hbm),
        scratch_shapes=[dma((2,))],
    )(*[pltpu.with_memory_space_constraint(x, pltpu.VMEM) for x in results])


def complex_quad(z_part, s_part):
    highest = lax.Precision.HIGHEST

    def single(left, right):
        return jnp.einsum("kra,rkb->kab", left, right, precision=highest)

    real = single(z_part[0], s_part[0]) - single(z_part[1], s_part[1])
    imag = single(z_part[0], s_part[1]) + single(z_part[1], s_part[0])
    return jnp.stack([real, imag])


def local(ainv_anc, panel, u_inv, k_inv, structure):
    block_width = u_inv.shape[-1]
    cols = lax.axis_size("pcol")
    if (
        structure.shape[1] == cols
        and lax.axis_size("prow") == cols
        and ainv_anc.shape[1] == ainv_anc.shape[2]
        and u_inv.shape[1] == cols
        and cols // 2 == 2
        and cols % 2 == 0
        and block_width == 2 * LANES
    ):
        return compact(ainv_anc, panel, u_inv, k_inv, structure)
    total_k = u_inv.shape[1]
    own_k = k_inv.shape[1]
    n_cols = lax.axis_size("pcol")
    row_here = lax.axis_index("prow")
    col_here = lax.axis_index("pcol")
    row_blocks = ainv_anc.shape[1] // block_width
    group_blocks = ainv_anc.shape[2] // block_width
    group_slots = structure.shape[1] // n_cols
    rows_all = row_blocks * block_width
    col_struct = lax.dynamic_slice_in_dim(structure, col_here * group_slots, group_slots, 1)
    slot_live = col_struct >= 0
    slot_pos = col_struct - col_here * group_blocks
    first_block = row_here * row_blocks
    target = first_block + jnp.arange(row_blocks, dtype=jnp.int32)
    rows_in = lax.all_gather(panel, "prow", axis=2, tiled=True)

    def single(left, right):
        return jnp.einsum("knb,kbc->knc", left, right, preferred_element_type=jnp.float32)

    real = single(rows_in[0], u_inv[0]) - single(rows_in[1], u_inv[1])
    imag = single(rows_in[0], u_inv[1]) + single(rows_in[1], u_inv[0])
    placed = jnp.stack([real, imag]).astype(jnp.bfloat16)
    placed = placed.reshape(2, total_k, group_slots, block_width, block_width)
    placed = jnp.where(slot_live[None, :, :, None, None], placed, jnp.zeros((), jnp.bfloat16))
    block_ids = jnp.arange(group_blocks, dtype=jnp.int32)
    pick_table = (slot_pos[:, :, None] == block_ids[None, None, :]).astype(jnp.bfloat16)
    ainv_blocks = ainv_anc.reshape(2, rows_all, group_blocks, block_width)

    def one_node(items):
        table_k, rows_k = items
        picked = jnp.einsum(
            "sg,cigw->cisw", table_k, ainv_blocks, preferred_element_type=jnp.float32
        )
        picked = picked.astype(jnp.bfloat16).reshape(2, rows_all, group_slots * block_width)
        right = rows_k.reshape(2, group_slots * block_width, block_width)
        real = jnp.dot(picked[0], right[0], preferred_element_type=jnp.float32) - jnp.dot(
            picked[1], right[1], preferred_element_type=jnp.float32
        )
        imag = jnp.dot(picked[0], right[1], preferred_element_type=jnp.float32) + jnp.dot(
            picked[1], right[0], preferred_element_type=jnp.float32
        )
        return jnp.stack([real, imag])

    per_node = lax.map(one_node, (pick_table, jnp.moveaxis(placed, 1, 0)))
    partial_value = jnp.transpose(per_node, (1, 2, 0, 3))
    row_table = (col_struct[:, None, :] == target[None, :, None]).astype(jnp.bfloat16)
    z_rows = jnp.einsum("kts,ckswb->cktwb", row_table, placed, preferred_element_type=jnp.float32)
    z_rows = z_rows.astype(jnp.bfloat16).reshape(2, total_k, rows_all, block_width)
    summed = lax.psum_scatter(
        partial_value.reshape(2, rows_all, total_k * block_width),
        "pcol",
        scatter_dimension=2,
        tiled=True,
    )
    own_struct = lax.dynamic_slice_in_dim(structure, col_here * own_k, own_k, 0)
    member = jnp.any(own_struct[:, :, None] == target[None, None, :], axis=1)
    selected = -summed.reshape(2, row_blocks, block_width, own_k, block_width)
    selected = jnp.where(member.T[None, :, None, :, None], selected, 0.0)
    sel_inv = selected.reshape(2, rows_all, own_k * block_width)
    received = lax.all_to_all(z_rows, "pcol", split_axis=1, concat_axis=1, tiled=True)
    z_own = (
        received.astype(jnp.float32).reshape(2, n_cols, own_k, rows_all, block_width).sum(axis=1)
    )
    quad_term = complex_quad(z_own, selected.reshape(2, rows_all, own_k, block_width))
    total_sum = lax.psum(quad_term, "prow")
    diag_inv = k_inv - total_sum
    return (sel_inv, diag_inv)


def solution(mesh):
    placed = (
        P(None, ("pole", "prow"), "pcol"),
        P(None, "pole", ("pcol", "prow"), None),
        P(None, "pole", None, None),
        P(None, ("pole", "pcol"), None, None),
        P(),
    )
    return jax.shard_map(
        local,
        mesh=mesh,
        in_specs=placed,
        out_specs=(P(None, ("pole", "prow"), "pcol"), P(None, ("pole", "pcol"), None, None)),
        check_vma=False,
    )
```

```python
import functools

import jax
import jax.numpy as jnp
from jax import lax
from jax.experimental import pallas as pl
from jax.experimental.pallas import tpu as pltpu
from jax.sharding import PartitionSpec as P

BF16 = jnp.bfloat16
F32 = jnp.float32
LANES = 128
scope = jax.named_scope


def cdot(left, right, dims=(((1,), (0,)), ((), ()))):
    def single(x, y):
        return lax.dot_general(x, y, dims, preferred_element_type=F32)

    real = single(left[0], right[0]) - single(left[1], right[1])
    imag = single(left[0], right[1]) + single(left[1], right[0])
    return real, imag


def remote(src, dst, send_sem, recv_sem, where):
    return pltpu.make_async_remote_copy(
        src_ref=src,
        dst_ref=dst,
        send_sem=send_sem,
        recv_sem=recv_sem,
        device_id=where,
        device_id_type=pl.DeviceIdType.MESH,
    )


def swap(x):
    return pltpu.roll(x, x.shape[1] // 2, 1)


def low_lanes():
    return lax.broadcasted_iota(jnp.int32, (1, LANES), 1) < LANES // 2


def tiles_of(x):
    return [x[:, at : at + LANES] for at in range(0, x.shape[1], LANES)]


def join(left, right):
    sign = jnp.where(low_lanes(), -1.0, 1.0)
    return jnp.concatenate([a + swap(b) * sign for a, b in zip(tiles_of(left), tiles_of(right))], axis=1)


def cross(a, b):
    low = low_lanes()
    return jnp.where(low, a, swap(b)), jnp.where(low, swap(a), b)


def kernel(
    n_rows, n_cols, spans, a_hbm, panel_hbm, u_hbm, k_hbm, table_hbm, sel_out, diag_out,
    table, av, pv, uv, pr, pick_out, picks, acc, kv, z_t,
    gather_0, gather_1, gather_2, own_0, own_1, own_2, out_0, out_1, out_2,
    in_0, in_1, in_2, tot_0, tot_1, tot_2, some,
    d_send, q_recv, t_recv,
):
    gather, own = (gather_0, gather_1, gather_2), (own_0, own_1, own_2)
    q_out, q_in, tot = (out_0, out_1, out_2), (in_0, in_1, in_2), (tot_0, tot_1, tot_2)
    groups = range(len(spans))
    row = lax.axis_index("prow")
    col = lax.axis_index("pcol")
    width = u_hbm.shape[-1]
    pairs = n_cols // 2
    row_blocks = a_hbm.shape[1] // width
    col_blocks = a_hbm.shape[2] // width
    band_rows = LANES // 2
    share = q_in[0].shape[1]
    first = n_rows // 2 - 1
    mate = row + 1 - 2 * (row % 2)
    is_end = (row == 0) | (row == n_rows - 1)
    is_inner = jnp.logical_not(is_end)
    end = jnp.where(is_end, row, mate)
    inner = jnp.where(is_end, mate, row)
    over = n_rows - 1 - inner
    far = n_rows - 1 - end

    def peer(unit):
        return ((col // 2 + unit // 2) % pairs) * 2 + (col + unit) % 2

    def unit_of(slot):
        return ((slot // 2 - col // 2 + pairs) % pairs) * 2 + (slot + col) % 2

    def arrived(view, sem):
        remote(view, view, sem, sem, {"prow": mate}).wait_recv()

    def drain(view, sem):
        remote(view, view, sem, sem, {"prow": mate}).wait_send()

    def pieces(group):
        cuts = 1 if group else 2
        rows = band_rows // cuts
        return [(part, slice(cut * rows, (cut + 1) * rows)) for part in range(share) for cut in range(cuts)]

    last = len(spans) - 1
    slots = sum(len(pieces(group)) for group in groups)

    def slot_of(group, piece):
        before = sum(len(pieces(other)) for other in range(group))
        return before + pieces(group).index(piece)

    def gathering(local_sem, p_send, p_recv, a_send, a_recv, g_send, g_recv):
        copy_p = pltpu.make_async_copy(panel_hbm, pv, local_sem.at[0])
        copy_u = pltpu.make_async_copy(u_hbm.at[:, col], uv, local_sem.at[1])
        copy_t = pltpu.make_async_copy(table_hbm, table, local_sem.at[2])
        copy_a = pltpu.make_async_copy(a_hbm, av, local_sem.at[3])
        copy_k = pltpu.make_async_copy(k_hbm, kv, local_sem.at[2])
        copy_p.start()
        copy_u.start()
        copy_t.start()
        copy_a.start()

        barrier = pltpu.get_barrier_semaphore()

        def greet(axis, there):
            pl.semaphore_signal(barrier, inc=1, device_id={axis: there}, device_id_type=pl.DeviceIdType.MESH)

        for unit in range(1, n_cols):
            greet("pcol", peer(unit))
        greet("prow", mate)
        greet("prow", jnp.where(is_end, over, far))

        @pl.when(is_inner)
        def _():
            greet("prow", over)

        def panel_copy(unit, source):
            return remote(
                pv.at[:, peer(unit)], pr.at[source], p_send.at[0], p_recv.at[unit - 1], {"pcol": peer(unit)}
            )

        def pick_copy(unit, source):
            return remote(
                pick_out.at[unit - 1], picks.at[source], a_send.at[0], a_recv.at[unit - 1], {"pcol": peer(unit)}
            )

        def base(group):
            return (group + 1) * n_cols if group else 0

        all_mate = 4 * n_cols

        def chunk_copy(group, unit, chunk, index, there):
            block = gather[group].at[unit, chunk]
            return remote(block, block, g_send.at[0], g_recv.at[index], {"prow": there})

        def scale(unit):
            slot = peer(unit)
            if unit == 0:
                left = (pv[0, col], pv[1, col])
            else:
                panel_copy(unit, slot).wait_recv()
                left = (pr[slot, 0], pr[slot, 1])
            real, imag = cdot(left, (uv[0], uv[1]))
            live = (jnp.full((1, width), table[col, slot]) >= 0).astype(F32)
            packed = []
            for a, b in zip(tiles_of(real * live), tiles_of(imag * live)):
                packed.extend(cross(a, b))
            for group in groups:
                lo, hi = spans[group]
                for tile in range(lo, hi):
                    at = (tile - lo) * LANES
                    gather[group][unit, row, :, at : at + LANES] = packed[tile].astype(BF16)

        def send_over(group, unit):
            index = base(group) + unit if group else unit + jnp.where(is_end, n_cols, 0)
            chunk_copy(group, unit, row, index, over).start()

        def send_mate(group, unit):
            chunk_copy(group, unit, row, jnp.where(is_end, all_mate, base(group) + unit), mate).start()

        def pick(unit):
            node = peer(unit)
            top = jnp.full((1, width), table[node, row]) - row * row_blocks
            side = jnp.full((1, width), table[node, col]) - col * col_blocks
            for plane in range(2):
                total = None
                for i in range(row_blocks):
                    for j in range(col_blocks):
                        keep = ((top == i) & (side == j)).astype(F32).astype(BF16)
                        block = av[plane, i * width : (i + 1) * width, j * width : (j + 1) * width] * keep
                        total = block if total is None else total + block
                if unit == 0:
                    picks[col, plane] = total
                else:
                    pick_out[unit - 1, plane] = total

        def meet():
            with scope("barrier"):
                pl.semaphore_wait(barrier, n_cols + 2 - is_end.astype(jnp.int32))
            for unit in range(1, n_cols):
                panel_copy(unit, col).start()

        with scope("copy_p"):
            copy_p.wait()

        @pl.when(is_end)
        def _():
            meet()

        with scope("copies"):
            copy_u.wait()
            copy_t.wait()
        copy_k.start()
        with scope("scale0"):
            scale(0)

        @pl.when(is_inner)
        def _():
            meet()

        send_over(0, 0)
        send_mate(0, 0)
        with scope("scale1"):
            scale(1)
        send_over(0, 1)
        send_mate(0, 1)
        far_home = unit_of(far)
        early = jnp.where(far_home < 2, far_home, 0)
        for group in groups[1:]:
            send_over(group, early)

        @pl.when(is_end)
        def _():
            for group in groups[1:]:
                send_mate(group, early)

        @pl.when(is_inner)
        def _():
            for unit in range(2):
                for group in groups[1:]:
                    send_mate(group, unit)

        with scope("copy_a"):
            copy_a.wait()
        for unit in list(range(2, n_cols)) + [1]:
            with scope(f"pick{unit}"):
                pick(unit)
            pick_copy(unit, col).start()
        pick(0)
        late = range(2, n_cols)
        order = [(group, 0) for group in groups[1:]] + [(group, i) for group in groups[1:] for i in range(1, n_cols)]

        def relay(unit, chunk, index):
            arrived(gather[0].at[unit, chunk], g_recv.at[index])
            chunk_copy(0, unit, chunk, unit, end).start()

        def relay_both(group, unit):
            index = base(group) + unit
            arrived(gather[group].at[unit, 0:2], g_recv.at[index])
            chunk_copy(group, unit, over, index, end).start()
            chunk_copy(group, unit, far, index, end).start()

        @pl.when(is_end)
        def _():
            for unit in late:
                with scope(f"scale{unit}"):
                    scale(unit)
                send_over(0, unit)
                send_mate(0, unit)
            for group, i in order:
                unit = (far_home + i) % n_cols

                @pl.when(unit != early)
                def _():
                    send_over(group, unit)
                    send_mate(group, unit)

        @pl.when(is_inner)
        def _():
            with scope("relay_0o"):
                relay(0, over, 0)
            with scope("scale2"):
                scale(2)
            send_over(0, 2)
            send_mate(0, 2)
            with scope("relay_1o"):
                relay(1, over, 1)
            with scope("scale3"):
                scale(3)
            send_over(0, 3)
            send_mate(0, 3)
            with scope("relay_01f"):
                relay(0, far, n_cols)
                relay(1, far, n_cols + 1)
            for group, i in order:
                unit = (far_home + i) % n_cols

                @pl.when(unit != early)
                def _():
                    send_over(group, unit)

            home = unit_of(end)

            @pl.when(home >= 2)
            def _():
                for group in groups[1:]:
                    send_mate(group, home)

            for unit in late:
                with scope(f"relay_{unit}o"):
                    relay(unit, over, unit)
                with scope(f"relay_{unit}f"):
                    relay(unit, far, n_cols + unit)
            for group, i in order:
                if i == 1:
                    for unit in late:

                        @pl.when(unit != home)
                        def _():
                            send_mate(group, unit)

                with scope(f"relay_g{group}_{i}"):
                    relay_both(group, (home + i) % n_cols)
            with scope("mate"):
                arrived(picks.at[0], g_recv.at[all_mate])

        def ready(group, unit):
            @pl.when(is_end)
            def _():
                arrived(gather[group].at[unit, 0 : n_rows - 1], g_recv.at[base(group) + unit])

        def span(group):
            lo, hi = spans[group]
            return slice(lo * LANES, hi * LANES)

        def multiply(group, unit, start):
            right = gather[group][unit].reshape(width, gather[group].shape[-1])
            slot = peer(unit)
            for plane in range(2):
                value = jnp.dot(picks[slot, plane], right, preferred_element_type=F32)
                if start:
                    acc[plane, :, span(group)] = value
                else:
                    acc[plane, :, span(group)] += value

        home = unit_of(row)
        named = jnp.full((1, LANES), table[col, row]) - row * row_blocks

        def quad_copy(group, there, piece):
            part, rows = piece
            at = part if there is over else share + part
            slot = slot_of(group, piece)
            if group == last and there is over:
                slot = jnp.where(is_end, slots + part, slot)
            return remote(
                q_out[group].at[at, rows], q_in[group].at[row, part, rows],
                d_send.at[0], q_recv.at[slot], {"prow": there},
            )

        def quad(group, unit):
            right = gather[group][unit].reshape(width, gather[group].shape[-1])
            slot = peer(unit)
            sums = [
                acc[plane, :, span(group)] + jnp.dot(picks[slot, plane], right, preferred_element_type=F32)
                for plane in range(2)
            ]
            value = join(*sums)
            product = jnp.dot(z_t[...].reshape(2 * width, width), value.astype(BF16), preferred_element_type=F32)
            turns = [(piece, half) for piece in pieces(group) for half in range(2)]
            if group == last:
                turns = [(piece, half) for piece in pieces(group) for half in (1, 0)]
            for piece, half in turns:
                part, rows = piece
                at = (half * share + part) * LANES
                upper = product[at + rows.start : at + rows.stop]
                lower = product[at + band_rows + rows.start : at + band_rows + rows.stop]
                block = join(upper, lower)
                q_out[group][half * share + part, rows] = block.astype(BF16)
                if half:
                    own[group][part, rows] = block
                if half:

                    @pl.when(is_end)
                    def _():
                        quad_copy(group, mate, piece).start()

                else:
                    quad_copy(group, over, piece).start()

            acc[0, :, span(group)] = value

        for unit in range(n_cols):
            with scope(f"ready_g0_{unit}"):
                ready(0, unit)
            if unit == n_cols - 1:
                with scope("ready_home"):
                    for group in groups[1:]:
                        ready(group, home)
                for group in groups:
                    turned = gather[group][home].reshape(width, gather[group].shape[-1]).T
                    for tile in range(*spans[group]):
                        at = (tile - spans[group][0]) * LANES
                        to = (tile % share) * LANES
                        part = jnp.where(over - first == tile // share, 0, 1)
                        z_t[part, to : to + LANES, :] = turned[at : at + LANES]
            with scope(f"wpick_{unit}"):
                if unit > 0:
                    pick_copy(unit, peer(unit)).wait_recv()
            if unit < n_cols - 1:
                multiply(0, unit, unit == 0)
        with scope("quad0"):
            quad(0, n_cols - 1)
        for group in groups[1:]:
            for i in range(n_cols):
                unit = (home + i) % n_cols
                if i > 0:
                    with scope(f"ready_g{group}_{i}"):
                        ready(group, unit)
                if i < n_cols - 1:
                    multiply(group, unit, i == 0)
            with scope(f"quad{group}"):
                quad(group, unit)

        for pair in range(width // LANES):
            at = 2 * pair * LANES
            planes = cross(acc[0, :, at : at + LANES], acc[0, :, at + LANES : at + 2 * LANES])
            columns = slice(pair * LANES, (pair + 1) * LANES)
            for i in range(row_blocks):
                keep = -(named == i).astype(F32)
                for plane in range(2):
                    sel_out[plane, i * width : (i + 1) * width, columns] = planes[plane] * keep
        copy_k.wait()
        drain(pr.at[0 : n_cols - 1], p_send.at[0])
        drain(pick_out, a_send.at[0])

        @pl.when(is_inner)
        def _():
            drain(picks, g_send.at[0])

        @pl.when(is_end)
        def _():
            drain(picks.at[0:2], g_send.at[0])
            drain(picks.at[0], d_send.at[0])

    dma = pltpu.SemaphoreType.DMA
    pl.run_scoped(
        gathering, dma((4,)), dma((1,)), dma((n_cols - 1,)), dma((1,)), dma((n_cols - 1,)), dma((1,)), dma((4 * n_cols + 1,))
    )

    def total_copy(group, piece, there):
        part, rows = piece
        block = tot[group].at[(row - first) * share + part, rows]
        return remote(block, block, d_send.at[0], t_recv.at[group * 2 + row - first], {"prow": there})

    where_tile = {tile: group for group in groups for tile in range(*spans[group])}

    def tile_of(tile, band):
        group = where_tile[tile]
        at = (tile - spans[group][0]) * LANES
        return tot[group][band, :, at : at + LANES].astype(F32)

    def finish(pair, owner):
        columns = slice(pair * LANES, (pair + 1) * LANES)
        for part in range(share):
            band = owner * share + part
            rows = pl.ds(pl.multiple_of(band * band_rows, band_rows), band_rows)
            planes = cross(tile_of(2 * pair, band), tile_of(2 * pair + 1, band))
            for plane in range(2):
                diag_out[plane, 0, rows, columns] = kv[plane, 0, rows, columns] + planes[plane]

    @pl.when(is_inner)
    def _():
        for group in groups[:last]:
            for piece in pieces(group):
                part, rows = piece
                with scope(f"wq{slot_of(group, piece)}"):
                    arrived(q_in[group].at[0 : n_rows - 1, part, rows], q_recv.at[slot_of(group, piece)])
                total = own[group][part, rows]
                for source in (over, end, far):
                    total = total + q_in[group][source, part, rows].astype(F32)
                tot[group][(row - first) * share + part, rows] = total.astype(BF16)
                total_copy(group, piece, far).start()
                total_copy(group, piece, end).start()
        for piece in pieces(last):
            part, rows = piece
            slot = slot_of(last, piece)
            with scope(f"wq{slot}"):
                arrived(q_in[last].at[0:2, part, rows], q_recv.at[slot])
            total = own[last][part] + q_in[last][over, part].astype(F32) + q_in[last][end, part].astype(F32)
            some[part] = total.astype(BF16)
            band = (row - first) * share + part
            remote(
                some.at[part], tot[last].at[band], d_send.at[0], t_recv.at[2 * last + row - first], {"prow": far}
            ).start()
        for piece in pieces(last):
            part, rows = piece
            with scope(f"wf{part}"):
                arrived(q_in[last].at[0, part, rows], q_recv.at[slots + part])
            total = some[part].astype(F32) + q_in[last][far, part].astype(F32)
            tot[last][(row - first) * share + part] = total.astype(BF16)
            total_copy(last, piece, end).start()
        for group in groups:
            for part in range(share):
                total_copy(group, (part, slice(0, band_rows)), over).start()
        for pair in range(width // LANES):
            finish(pair, row - first)

    def total_wait(group, owner):
        arrived(tot[group].at[0:share], t_recv.at[group * 2 + owner])

    @pl.when(is_end)
    def _():
        for group in groups:
            for there in (inner, over):
                with scope(f"wt{group}"):
                    total_wait(group, there - first)
                if group == last and there is over:
                    for part in range(share):
                        band = (over - first) * share + part
                        total = tot[last][band].astype(F32) + q_out[last][part].astype(F32)
                        tot[last][band] = total.astype(BF16)
                if group != 1:
                    finish(1 if group else 0, there - first)

    @pl.when(is_inner)
    def _():
        for group in groups:
            with scope(f"wt{group}"):
                total_wait(group, over - first)
        for pair in range(width // LANES):
            finish(pair, over - first)
        drain(picks.at[0:2], d_send.at[0])


def place(sel, diag, sel_out, diag_out, out_sem):
    copies = [
        pltpu.make_async_copy(sel, sel_out, out_sem.at[0]),
        pltpu.make_async_copy(diag, diag_out, out_sem.at[1]),
    ]
    for copy in copies:
        copy.start()
    for copy in copies:
        copy.wait()


def compact(ainv_anc, panel, u_inv, k_inv, structure):
    n_rows, n_cols = lax.axis_size("prow"), lax.axis_size("pcol")
    width, part = u_inv.shape[-1], panel.shape[2]
    row_blocks = ainv_anc.shape[1] // width
    tiles = 2 * width // LANES
    share = tiles // 2
    spans = ((0, share), (share, share + share // 2), (share + share // 2, tiles))
    hbm = pl.BlockSpec(memory_space=pltpu.HBM)
    vmem = pl.BlockSpec(memory_space=pltpu.VMEM)
    dma = pltpu.SemaphoreType.DMA
    shapes = (
        jax.ShapeDtypeStruct((2, row_blocks * width, width), F32),
        jax.ShapeDtypeStruct(k_inv.shape, F32),
    )

    def per_group(lead, rows, kind):
        return [pltpu.VMEM(lead + (rows, (hi - lo) * LANES), kind) for lo, hi in spans]

    band_rows = LANES // 2
    results = pl.pallas_call(
        functools.partial(kernel, n_rows, n_cols, spans),
        out_shape=tuple(pltpu.VMEM(s.shape, s.dtype) for s in shapes),
        in_specs=[hbm, hbm, hbm, hbm, hbm],
        out_specs=(vmem, vmem),
        scratch_shapes=[
            pltpu.SMEM(structure.shape, jnp.int32),
            pltpu.VMEM(ainv_anc.shape, BF16),
            pltpu.VMEM(panel.shape, BF16),
            pltpu.VMEM((2, width, width), BF16),
            pltpu.VMEM((n_cols, 2, part, width), BF16),
            pltpu.VMEM((n_cols - 1, 2, width, width), BF16),
            pltpu.VMEM((n_cols, 2, width, width), BF16),
            pltpu.VMEM((2, width, 2 * width), F32),
            pltpu.VMEM(k_inv.shape, F32),
            pltpu.VMEM((2, width, width), BF16),
            *per_group((n_cols, n_rows), part, BF16),
            *per_group((share,), band_rows, F32),
            *per_group((tiles,), band_rows, BF16),
            *per_group((n_rows, share), band_rows, BF16),
            *per_group((tiles,), band_rows, BF16),
            pltpu.VMEM((share, band_rows, LANES), BF16),
            dma((1,)),
            dma((5 * share,)),
            dma((6,)),
        ],
        compiler_params=pltpu.CompilerParams(
            collective_id=0, has_side_effects=True
        ),
    )(ainv_anc, panel, u_inv, k_inv, structure)
    return pl.pallas_call(
        place,
        out_shape=shapes,
        in_specs=[vmem, vmem],
        out_specs=(hbm, hbm),
        scratch_shapes=[dma((2,))],
    )(*[pltpu.with_memory_space_constraint(x, pltpu.VMEM) for x in results])


def complex_quad(z_part, s_part):
    highest = lax.Precision.HIGHEST

    def single(left, right):
        return jnp.einsum("kra,rkb->kab", left, right, precision=highest)

    real = single(z_part[0], s_part[0]) - single(z_part[1], s_part[1])
    imag = single(z_part[0], s_part[1]) + single(z_part[1], s_part[0])
    return jnp.stack([real, imag])


def local(ainv_anc, panel, u_inv, k_inv, structure):
    block_width = u_inv.shape[-1]
    cols = lax.axis_size("pcol")
    if (
        structure.shape[1] == cols
        and lax.axis_size("prow") == cols
        and ainv_anc.shape[1] == ainv_anc.shape[2]
        and u_inv.shape[1] == cols
        and cols // 2 == 2
        and cols % 2 == 0
        and block_width == 2 * LANES
    ):
        return compact(ainv_anc, panel, u_inv, k_inv, structure)
    total_k = u_inv.shape[1]
    own_k = k_inv.shape[1]
    n_cols = lax.axis_size("pcol")
    row_here = lax.axis_index("prow")
    col_here = lax.axis_index("pcol")
    row_blocks = ainv_anc.shape[1] // block_width
    group_blocks = ainv_anc.shape[2] // block_width
    group_slots = structure.shape[1] // n_cols
    rows_all = row_blocks * block_width
    col_struct = lax.dynamic_slice_in_dim(structure, col_here * group_slots, group_slots, 1)
    slot_live = col_struct >= 0
    slot_pos = col_struct - col_here * group_blocks
    first_block = row_here * row_blocks
    target = first_block + jnp.arange(row_blocks, dtype=jnp.int32)
    rows_in = lax.all_gather(panel, "prow", axis=2, tiled=True)

    def single(left, right):
        return jnp.einsum("knb,kbc->knc", left, right, preferred_element_type=jnp.float32)

    real = single(rows_in[0], u_inv[0]) - single(rows_in[1], u_inv[1])
    imag = single(rows_in[0], u_inv[1]) + single(rows_in[1], u_inv[0])
    placed = jnp.stack([real, imag]).astype(jnp.bfloat16)
    placed = placed.reshape(2, total_k, group_slots, block_width, block_width)
    placed = jnp.where(slot_live[None, :, :, None, None], placed, jnp.zeros((), jnp.bfloat16))
    block_ids = jnp.arange(group_blocks, dtype=jnp.int32)
    pick_table = (slot_pos[:, :, None] == block_ids[None, None, :]).astype(jnp.bfloat16)
    ainv_blocks = ainv_anc.reshape(2, rows_all, group_blocks, block_width)

    def one_node(items):
        table_k, rows_k = items
        picked = jnp.einsum(
            "sg,cigw->cisw", table_k, ainv_blocks, preferred_element_type=jnp.float32
        )
        picked = picked.astype(jnp.bfloat16).reshape(2, rows_all, group_slots * block_width)
        right = rows_k.reshape(2, group_slots * block_width, block_width)
        real = jnp.dot(picked[0], right[0], preferred_element_type=jnp.float32) - jnp.dot(
            picked[1], right[1], preferred_element_type=jnp.float32
        )
        imag = jnp.dot(picked[0], right[1], preferred_element_type=jnp.float32) + jnp.dot(
            picked[1], right[0], preferred_element_type=jnp.float32
        )
        return jnp.stack([real, imag])

    per_node = lax.map(one_node, (pick_table, jnp.moveaxis(placed, 1, 0)))
    partial_value = jnp.transpose(per_node, (1, 2, 0, 3))
    row_table = (col_struct[:, None, :] == target[None, :, None]).astype(jnp.bfloat16)
    z_rows = jnp.einsum("kts,ckswb->cktwb", row_table, placed, preferred_element_type=jnp.float32)
    z_rows = z_rows.astype(jnp.bfloat16).reshape(2, total_k, rows_all, block_width)
    summed = lax.psum_scatter(
        partial_value.reshape(2, rows_all, total_k * block_width),
        "pcol",
        scatter_dimension=2,
        tiled=True,
    )
    own_struct = lax.dynamic_slice_in_dim(structure, col_here * own_k, own_k, 0)
    member = jnp.any(own_struct[:, :, None] == target[None, None, :], axis=1)
    selected = -summed.reshape(2, row_blocks, block_width, own_k, block_width)
    selected = jnp.where(member.T[None, :, None, :, None], selected, 0.0)
    sel_inv = selected.reshape(2, rows_all, own_k * block_width)
    received = lax.all_to_all(z_rows, "pcol", split_axis=1, concat_axis=1, tiled=True)
    z_own = (
        received.astype(jnp.float32).reshape(2, n_cols, own_k, rows_all, block_width).sum(axis=1)
    )
    quad_term = complex_quad(z_own, selected.reshape(2, rows_all, own_k, block_width))
    total_sum = lax.psum(quad_term, "prow")
    diag_inv = k_inv - total_sum
    return (sel_inv, diag_inv)


def solution(mesh):
    placed = (
        P(None, ("pole", "prow"), "pcol"),
        P(None, "pole", ("pcol", "prow"), None),
        P(None, "pole", None, None),
        P(None, ("pole", "pcol"), None, None),
        P(),
    )
    return jax.shard_map(
        local,
        mesh=mesh,
        in_specs=placed,
        out_specs=(P(None, ("pole", "prow"), "pcol"), P(None, ("pole", "pcol"), None, None)),
        check_vma=False,
    )
```

```python
import functools

import jax
import jax.numpy as jnp
from jax import lax
from jax.experimental import pallas as pl
from jax.experimental.pallas import tpu as pltpu
from jax.sharding import PartitionSpec as P

BF16 = jnp.bfloat16
F32 = jnp.float32
LANES = 128
scope = jax.named_scope


def cdot(left, right, dims=(((1,), (0,)), ((), ()))):
    def single(x, y):
        return lax.dot_general(x, y, dims, preferred_element_type=F32)

    real = single(left[0], right[0]) - single(left[1], right[1])
    imag = single(left[0], right[1]) + single(left[1], right[0])
    return real, imag


def remote(src, dst, send_sem, recv_sem, where):
    return pltpu.make_async_remote_copy(
        src_ref=src,
        dst_ref=dst,
        send_sem=send_sem,
        recv_sem=recv_sem,
        device_id=where,
        device_id_type=pl.DeviceIdType.MESH,
    )


def swap(x):
    return pltpu.roll(x, x.shape[1] // 2, 1)


def low_lanes():
    return lax.broadcasted_iota(jnp.int32, (1, LANES), 1) < LANES // 2


def tiles_of(x):
    return [x[:, at : at + LANES] for at in range(0, x.shape[1], LANES)]


def join(left, right):
    sign = jnp.where(low_lanes(), -1.0, 1.0)
    return jnp.concatenate([a + swap(b) * sign for a, b in zip(tiles_of(left), tiles_of(right))], axis=1)


def cross(a, b):
    low = low_lanes()
    return jnp.where(low, a, swap(b)), jnp.where(low, swap(a), b)


def kernel(
    n_rows, n_cols, spans, a_hbm, panel_hbm, u_hbm, k_hbm, table_hbm, sel_out, diag_out,
    table, av, pv, uv, pr, pick_out, picks, acc, kv, z_t,
    gather_0, gather_1, gather_2, own_0, own_1, own_2, out_0, out_1, out_2,
    in_0, in_1, in_2, tot_0, tot_1, tot_2, some,
    d_send, t_recv,
):
    gather, own = (gather_0, gather_1, gather_2), (own_0, own_1, own_2)
    q_out, q_in, tot = (out_0, out_1, out_2), (in_0, in_1, in_2), (tot_0, tot_1, tot_2)
    groups = range(len(spans))
    row = lax.axis_index("prow")
    col = lax.axis_index("pcol")
    width = u_hbm.shape[-1]
    pairs = n_cols // 2
    row_blocks = a_hbm.shape[1] // width
    col_blocks = a_hbm.shape[2] // width
    band_rows = LANES // 2
    share = q_in[0].shape[1]
    first = n_rows // 2 - 1
    mate = row + 1 - 2 * (row % 2)
    is_end = (row == 0) | (row == n_rows - 1)
    is_inner = jnp.logical_not(is_end)
    end = jnp.where(is_end, row, mate)
    inner = jnp.where(is_end, mate, row)
    over = n_rows - 1 - inner
    far = n_rows - 1 - end

    def peer(unit):
        return ((col // 2 + unit // 2) % pairs) * 2 + (col + unit) % 2

    def unit_of(slot):
        return ((slot // 2 - col // 2 + pairs) % pairs) * 2 + (slot + col) % 2

    def arrived(view, sem):
        remote(view, view, sem, sem, {"prow": mate}).wait_recv()

    def drain(view, sem):
        remote(view, view, sem, sem, {"prow": mate}).wait_send()

    def pieces(group):
        cuts = 1 if group else 2
        rows = band_rows // cuts
        return [(part, slice(cut * rows, (cut + 1) * rows)) for part in range(share) for cut in range(cuts)]

    last = len(spans) - 1
    slots = sum(len(pieces(group)) for group in groups)

    def slot_of(group, piece):
        before = sum(len(pieces(other)) for other in range(group))
        return before + pieces(group).index(piece)

    def total_copy(group, piece, there):
        part, rows = piece
        block = tot[group].at[(row - first) * share + part, rows]
        return remote(block, block, d_send.at[0], t_recv.at[group * 2 + row - first], {"prow": there})

    where_tile = {tile: group for group in groups for tile in range(*spans[group])}

    def tile_of(tile, band):
        group = where_tile[tile]
        at = (tile - spans[group][0]) * LANES
        return tot[group][band, :, at : at + LANES].astype(F32)

    def finish(pair, owner):
        columns = slice(pair * LANES, (pair + 1) * LANES)
        for part in range(share):
            band = owner * share + part
            rows = pl.ds(pl.multiple_of(band * band_rows, band_rows), band_rows)
            planes = cross(tile_of(2 * pair, band), tile_of(2 * pair + 1, band))
            for plane in range(2):
                diag_out[plane, 0, rows, columns] = kv[plane, 0, rows, columns] + planes[plane]

    dma = pltpu.SemaphoreType.DMA

    def adding(q_recv):
        def gathering(local_sem, p_send, p_recv, a_send, a_recv, g_send, g_recv):
            copy_p = pltpu.make_async_copy(panel_hbm, pv, local_sem.at[0])
            copy_u = pltpu.make_async_copy(u_hbm.at[:, col], uv, local_sem.at[1])
            copy_t = pltpu.make_async_copy(table_hbm, table, local_sem.at[2])
            copy_a = pltpu.make_async_copy(a_hbm, av, local_sem.at[3])
            copy_k = pltpu.make_async_copy(k_hbm, kv, local_sem.at[2])
            copy_p.start()
            copy_u.start()
            copy_t.start()
            copy_a.start()

            barrier = pltpu.get_barrier_semaphore()

            def greet(axis, there):
                pl.semaphore_signal(barrier, inc=1, device_id={axis: there}, device_id_type=pl.DeviceIdType.MESH)

            for unit in range(1, n_cols):
                greet("pcol", peer(unit))
            greet("prow", mate)
            greet("prow", jnp.where(is_end, over, far))

            @pl.when(is_inner)
            def _():
                greet("prow", over)

            def panel_copy(unit, source):
                return remote(
                    pv.at[:, peer(unit)], pr.at[source], p_send.at[0], p_recv.at[unit - 1], {"pcol": peer(unit)}
                )

            def pick_copy(unit, source):
                return remote(
                    pick_out.at[unit - 1], picks.at[source], a_send.at[0], a_recv.at[unit - 1], {"pcol": peer(unit)}
                )

            def base(group):
                return (group + 1) * n_cols if group else 0

            all_mate = 4 * n_cols

            def chunk_copy(group, unit, chunk, index, there):
                block = gather[group].at[unit, chunk]
                return remote(block, block, g_send.at[0], g_recv.at[index], {"prow": there})

            def scale(unit):
                slot = peer(unit)
                if unit == 0:
                    left = (pv[0, col], pv[1, col])
                else:
                    panel_copy(unit, slot).wait_recv()
                    left = (pr[slot, 0], pr[slot, 1])
                real, imag = cdot(left, (uv[0], uv[1]))
                live = (jnp.full((1, width), table[col, slot]) >= 0).astype(F32)
                packed = []
                for a, b in zip(tiles_of(real * live), tiles_of(imag * live)):
                    packed.extend(cross(a, b))
                for group in groups:
                    lo, hi = spans[group]
                    for tile in range(lo, hi):
                        at = (tile - lo) * LANES
                        gather[group][unit, row, :, at : at + LANES] = packed[tile].astype(BF16)

            def send_over(group, unit):
                index = base(group) + unit if group else unit + jnp.where(is_end, n_cols, 0)
                chunk_copy(group, unit, row, index, over).start()

            def send_mate(group, unit):
                chunk_copy(group, unit, row, jnp.where(is_end, all_mate, base(group) + unit), mate).start()

            def pick(unit):
                node = peer(unit)
                top = jnp.full((1, width), table[node, row]) - row * row_blocks
                side = jnp.full((1, width), table[node, col]) - col * col_blocks
                for plane in range(2):
                    total = None
                    for i in range(row_blocks):
                        for j in range(col_blocks):
                            keep = ((top == i) & (side == j)).astype(F32).astype(BF16)
                            block = av[plane, i * width : (i + 1) * width, j * width : (j + 1) * width] * keep
                            total = block if total is None else total + block
                    if unit == 0:
                        picks[col, plane] = total
                    else:
                        pick_out[unit - 1, plane] = total

            def meet():
                with scope("barrier"):
                    pl.semaphore_wait(barrier, n_cols + 2 - is_end.astype(jnp.int32))
                for unit in range(1, n_cols):
                    panel_copy(unit, col).start()

            with scope("copy_p"):
                copy_p.wait()

            @pl.when(is_end)
            def _():
                meet()

            with scope("copies"):
                copy_u.wait()
                copy_t.wait()
            copy_k.start()
            with scope("scale0"):
                scale(0)

            @pl.when(is_inner)
            def _():
                meet()

            send_over(0, 0)
            send_mate(0, 0)
            with scope("scale1"):
                scale(1)
            send_over(0, 1)
            send_mate(0, 1)
            far_home = unit_of(far)
            early = jnp.where(far_home < 2, far_home, 0)
            for group in groups[1:]:
                send_over(group, early)

            @pl.when(is_end)
            def _():
                for group in groups[1:]:
                    send_mate(group, early)

            @pl.when(is_inner)
            def _():
                for unit in range(2):
                    for group in groups[1:]:
                        send_mate(group, unit)

            with scope("copy_a"):
                copy_a.wait()
            for unit in list(range(2, n_cols)) + [1]:
                with scope(f"pick{unit}"):
                    pick(unit)
                pick_copy(unit, col).start()
            pick(0)
            late = range(2, n_cols)
            order = [(group, 0) for group in groups[1:]] + [(group, i) for group in groups[1:] for i in range(1, n_cols)]

            def relay(unit, chunk, index):
                arrived(gather[0].at[unit, chunk], g_recv.at[index])
                chunk_copy(0, unit, chunk, unit, end).start()

            def relay_both(group, unit):
                index = base(group) + unit
                arrived(gather[group].at[unit, 0:2], g_recv.at[index])
                chunk_copy(group, unit, over, index, end).start()
                chunk_copy(group, unit, far, index, end).start()

            @pl.when(is_end)
            def _():
                for unit in late:
                    with scope(f"scale{unit}"):
                        scale(unit)
                    send_over(0, unit)
                    send_mate(0, unit)
                for group, i in order:
                    unit = (far_home + i) % n_cols

                    @pl.when(unit != early)
                    def _():
                        send_over(group, unit)
                        send_mate(group, unit)

            @pl.when(is_inner)
            def _():
                with scope("relay_0o"):
                    relay(0, over, 0)
                with scope("scale2"):
                    scale(2)
                send_over(0, 2)
                send_mate(0, 2)
                with scope("relay_1o"):
                    relay(1, over, 1)
                with scope("scale3"):
                    scale(3)
                send_over(0, 3)
                send_mate(0, 3)
                with scope("relay_01f"):
                    relay(0, far, n_cols)
                    relay(1, far, n_cols + 1)
                for group, i in order:
                    unit = (far_home + i) % n_cols

                    @pl.when(unit != early)
                    def _():
                        send_over(group, unit)

                home = unit_of(end)

                @pl.when(home >= 2)
                def _():
                    for group in groups[1:]:
                        send_mate(group, home)

                for unit in late:
                    with scope(f"relay_{unit}o"):
                        relay(unit, over, unit)
                    with scope(f"relay_{unit}f"):
                        relay(unit, far, n_cols + unit)
                for group, i in order:
                    if i == 1:
                        for unit in late:

                            @pl.when(unit != home)
                            def _():
                                send_mate(group, unit)

                    with scope(f"relay_g{group}_{i}"):
                        relay_both(group, (home + i) % n_cols)
                with scope("mate"):
                    arrived(picks.at[0], g_recv.at[all_mate])

            def ready(group, unit):
                @pl.when(is_end)
                def _():
                    arrived(gather[group].at[unit, 0 : n_rows - 1], g_recv.at[base(group) + unit])

            def span(group):
                lo, hi = spans[group]
                return slice(lo * LANES, hi * LANES)

            def multiply(group, unit, start):
                right = gather[group][unit].reshape(width, gather[group].shape[-1])
                slot = peer(unit)
                for plane in range(2):
                    value = jnp.dot(picks[slot, plane], right, preferred_element_type=F32)
                    if start:
                        acc[plane, :, span(group)] = value
                    else:
                        acc[plane, :, span(group)] += value

            home = unit_of(row)
            named = jnp.full((1, LANES), table[col, row]) - row * row_blocks

            def quad_copy(group, there, piece):
                part, rows = piece
                at = part if there is over else share + part
                slot = slot_of(group, piece)
                if group == last and there is over:
                    slot = jnp.where(is_end, slots + part, slot)
                return remote(
                    q_out[group].at[at, rows], q_in[group].at[row, part, rows],
                    d_send.at[0], q_recv.at[slot], {"prow": there},
                )

            def quad(group, unit):
                right = gather[group][unit].reshape(width, gather[group].shape[-1])
                slot = peer(unit)
                sums = [
                    acc[plane, :, span(group)] + jnp.dot(picks[slot, plane], right, preferred_element_type=F32)
                    for plane in range(2)
                ]
                value = join(*sums)
                product = jnp.dot(z_t[...].reshape(2 * width, width), value.astype(BF16), preferred_element_type=F32)
                turns = [(piece, half) for piece in pieces(group) for half in range(2)]
                if group == last:
                    turns = [(piece, half) for piece in pieces(group) for half in (1, 0)]
                for piece, half in turns:
                    part, rows = piece
                    at = (half * share + part) * LANES
                    upper = product[at + rows.start : at + rows.stop]
                    lower = product[at + band_rows + rows.start : at + band_rows + rows.stop]
                    block = join(upper, lower)
                    q_out[group][half * share + part, rows] = block.astype(BF16)
                    if half:
                        own[group][part, rows] = block
                    if half:

                        @pl.when(is_end)
                        def _():
                            quad_copy(group, mate, piece).start()

                    else:
                        quad_copy(group, over, piece).start()

                acc[0, :, span(group)] = value

            for unit in range(n_cols):
                with scope(f"ready_g0_{unit}"):
                    ready(0, unit)
                if unit == n_cols - 1:
                    with scope("ready_home"):
                        for group in groups[1:]:
                            ready(group, home)
                    for group in groups:
                        turned = gather[group][home].reshape(width, gather[group].shape[-1]).T
                        for tile in range(*spans[group]):
                            at = (tile - spans[group][0]) * LANES
                            to = (tile % share) * LANES
                            part = jnp.where(over - first == tile // share, 0, 1)
                            z_t[part, to : to + LANES, :] = turned[at : at + LANES]
                with scope(f"wpick_{unit}"):
                    if unit > 0:
                        pick_copy(unit, peer(unit)).wait_recv()
                if unit < n_cols - 1:
                    multiply(0, unit, unit == 0)
            with scope("quad0"):
                quad(0, n_cols - 1)
            for group in groups[1:]:
                for i in range(n_cols):
                    unit = (home + i) % n_cols
                    if i > 0:
                        with scope(f"ready_g{group}_{i}"):
                            ready(group, unit)
                    if i < n_cols - 1:
                        multiply(group, unit, i == 0)
                with scope(f"quad{group}"):
                    quad(group, unit)

            for pair in range(width // LANES):
                at = 2 * pair * LANES
                planes = cross(acc[0, :, at : at + LANES], acc[0, :, at + LANES : at + 2 * LANES])
                columns = slice(pair * LANES, (pair + 1) * LANES)
                for i in range(row_blocks):
                    keep = -(named == i).astype(F32)
                    for plane in range(2):
                        sel_out[plane, i * width : (i + 1) * width, columns] = planes[plane] * keep
            copy_k.wait()
            drain(pr.at[0 : n_cols - 1], p_send.at[0])
            drain(pick_out, a_send.at[0])

            @pl.when(is_inner)
            def _():
                drain(picks, g_send.at[0])

            @pl.when(is_end)
            def _():
                drain(picks.at[0:2], g_send.at[0])
                drain(picks.at[0], d_send.at[0])

        pl.run_scoped(
            gathering, dma((4,)), dma((1,)), dma((n_cols - 1,)), dma((1,)), dma((n_cols - 1,)), dma((1,)), dma((4 * n_cols + 1,))
        )

        @pl.when(is_inner)
        def _():
            for group in groups[:last]:
                for piece in pieces(group):
                    part, rows = piece
                    with scope(f"wq{slot_of(group, piece)}"):
                        arrived(q_in[group].at[0 : n_rows - 1, part, rows], q_recv.at[slot_of(group, piece)])
                    total = own[group][part, rows]
                    for source in (over, end, far):
                        total = total + q_in[group][source, part, rows].astype(F32)
                    tot[group][(row - first) * share + part, rows] = total.astype(BF16)
                    total_copy(group, piece, far).start()
                    total_copy(group, piece, end).start()
            for piece in pieces(last):
                part, rows = piece
                slot = slot_of(last, piece)
                with scope(f"wq{slot}"):
                    arrived(q_in[last].at[0:2, part, rows], q_recv.at[slot])
                total = own[last][part] + q_in[last][over, part].astype(F32) + q_in[last][end, part].astype(F32)
                some[part] = total.astype(BF16)
                band = (row - first) * share + part
                remote(
                    some.at[part], tot[last].at[band], d_send.at[0], t_recv.at[2 * last + row - first], {"prow": far}
                ).start()
            for piece in pieces(last):
                part, rows = piece
                with scope(f"wf{part}"):
                    arrived(q_in[last].at[0, part, rows], q_recv.at[slots + part])
                total = some[part].astype(F32) + q_in[last][far, part].astype(F32)
                tot[last][(row - first) * share + part] = total.astype(BF16)
                total_copy(last, piece, end).start()
            for group in groups:
                for part in range(share):
                    total_copy(group, (part, slice(0, band_rows)), over).start()
            for pair in range(width // LANES):
                finish(pair, row - first)

    pl.run_scoped(adding, dma((5 * share,)))

    def total_wait(group, owner):
        arrived(tot[group].at[0:share], t_recv.at[group * 2 + owner])

    @pl.when(is_end)
    def _():
        for group in groups:
            for there in (inner, over):
                with scope(f"wt{group}"):
                    total_wait(group, there - first)
                if group == last and there is over:
                    for part in range(share):
                        band = (over - first) * share + part
                        total = tot[last][band].astype(F32) + q_out[last][part].astype(F32)
                        tot[last][band] = total.astype(BF16)
                if group != 1:
                    finish(1 if group else 0, there - first)

    @pl.when(is_inner)
    def _():
        for group in groups:
            with scope(f"wt{group}"):
                total_wait(group, over - first)
        for pair in range(width // LANES):
            finish(pair, over - first)
        drain(picks.at[0:2], d_send.at[0])


def place(sel, diag, sel_out, diag_out, out_sem):
    copies = [
        pltpu.make_async_copy(sel, sel_out, out_sem.at[0]),
        pltpu.make_async_copy(diag, diag_out, out_sem.at[1]),
    ]
    for copy in copies:
        copy.start()
    for copy in copies:
        copy.wait()


def compact(ainv_anc, panel, u_inv, k_inv, structure):
    n_rows, n_cols = lax.axis_size("prow"), lax.axis_size("pcol")
    width, part = u_inv.shape[-1], panel.shape[2]
    row_blocks = ainv_anc.shape[1] // width
    tiles = 2 * width // LANES
    share = tiles // 2
    spans = ((0, share), (share, share + share // 2), (share + share // 2, tiles))
    hbm = pl.BlockSpec(memory_space=pltpu.HBM)
    vmem = pl.BlockSpec(memory_space=pltpu.VMEM)
    dma = pltpu.SemaphoreType.DMA
    shapes = (
        jax.ShapeDtypeStruct((2, row_blocks * width, width), F32),
        jax.ShapeDtypeStruct(k_inv.shape, F32),
    )

    def per_group(lead, rows, kind):
        return [pltpu.VMEM(lead + (rows, (hi - lo) * LANES), kind) for lo, hi in spans]

    band_rows = LANES // 2
    results = pl.pallas_call(
        functools.partial(kernel, n_rows, n_cols, spans),
        out_shape=tuple(pltpu.VMEM(s.shape, s.dtype) for s in shapes),
        in_specs=[hbm, hbm, hbm, hbm, hbm],
        out_specs=(vmem, vmem),
        scratch_shapes=[
            pltpu.SMEM(structure.shape, jnp.int32),
            pltpu.VMEM(ainv_anc.shape, BF16),
            pltpu.VMEM(panel.shape, BF16),
            pltpu.VMEM((2, width, width), BF16),
            pltpu.VMEM((n_cols, 2, part, width), BF16),
            pltpu.VMEM((n_cols - 1, 2, width, width), BF16),
            pltpu.VMEM((n_cols, 2, width, width), BF16),
            pltpu.VMEM((2, width, 2 * width), F32),
            pltpu.VMEM(k_inv.shape, F32),
            pltpu.VMEM((2, width, width), BF16),
            *per_group((n_cols, n_rows), part, BF16),
            *per_group((share,), band_rows, F32),
            *per_group((tiles,), band_rows, BF16),
            *per_group((n_rows, share), band_rows, BF16),
            *per_group((tiles,), band_rows, BF16),
            pltpu.VMEM((share, band_rows, LANES), BF16),
            dma((1,)),
            dma((6,)),
        ],
        compiler_params=pltpu.CompilerParams(
            collective_id=0, has_side_effects=True
        ),
    )(ainv_anc, panel, u_inv, k_inv, structure)
    return pl.pallas_call(
        place,
        out_shape=shapes,
        in_specs=[vmem, vmem],
        out_specs=(hbm, hbm),
        scratch_shapes=[dma((2,))],
    )(*[pltpu.with_memory_space_constraint(x, pltpu.VMEM) for x in results])


def complex_quad(z_part, s_part):
    highest = lax.Precision.HIGHEST

    def single(left, right):
        return jnp.einsum("kra,rkb->kab", left, right, precision=highest)

    real = single(z_part[0], s_part[0]) - single(z_part[1], s_part[1])
    imag = single(z_part[0], s_part[1]) + single(z_part[1], s_part[0])
    return jnp.stack([real, imag])


def local(ainv_anc, panel, u_inv, k_inv, structure):
    block_width = u_inv.shape[-1]
    cols = lax.axis_size("pcol")
    if (
        structure.shape[1] == cols
        and lax.axis_size("prow") == cols
        and ainv_anc.shape[1] == ainv_anc.shape[2]
        and u_inv.shape[1] == cols
        and cols // 2 == 2
        and cols % 2 == 0
        and block_width == 2 * LANES
    ):
        return compact(ainv_anc, panel, u_inv, k_inv, structure)
    total_k = u_inv.shape[1]
    own_k = k_inv.shape[1]
    n_cols = lax.axis_size("pcol")
    row_here = lax.axis_index("prow")
    col_here = lax.axis_index("pcol")
    row_blocks = ainv_anc.shape[1] // block_width
    group_blocks = ainv_anc.shape[2] // block_width
    group_slots = structure.shape[1] // n_cols
    rows_all = row_blocks * block_width
    col_struct = lax.dynamic_slice_in_dim(structure, col_here * group_slots, group_slots, 1)
    slot_live = col_struct >= 0
    slot_pos = col_struct - col_here * group_blocks
    first_block = row_here * row_blocks
    target = first_block + jnp.arange(row_blocks, dtype=jnp.int32)
    rows_in = lax.all_gather(panel, "prow", axis=2, tiled=True)

    def single(left, right):
        return jnp.einsum("knb,kbc->knc", left, right, preferred_element_type=jnp.float32)

    real = single(rows_in[0], u_inv[0]) - single(rows_in[1], u_inv[1])
    imag = single(rows_in[0], u_inv[1]) + single(rows_in[1], u_inv[0])
    placed = jnp.stack([real, imag]).astype(jnp.bfloat16)
    placed = placed.reshape(2, total_k, group_slots, block_width, block_width)
    placed = jnp.where(slot_live[None, :, :, None, None], placed, jnp.zeros((), jnp.bfloat16))
    block_ids = jnp.arange(group_blocks, dtype=jnp.int32)
    pick_table = (slot_pos[:, :, None] == block_ids[None, None, :]).astype(jnp.bfloat16)
    ainv_blocks = ainv_anc.reshape(2, rows_all, group_blocks, block_width)

    def one_node(items):
        table_k, rows_k = items
        picked = jnp.einsum(
            "sg,cigw->cisw", table_k, ainv_blocks, preferred_element_type=jnp.float32
        )
        picked = picked.astype(jnp.bfloat16).reshape(2, rows_all, group_slots * block_width)
        right = rows_k.reshape(2, group_slots * block_width, block_width)
        real = jnp.dot(picked[0], right[0], preferred_element_type=jnp.float32) - jnp.dot(
            picked[1], right[1], preferred_element_type=jnp.float32
        )
        imag = jnp.dot(picked[0], right[1], preferred_element_type=jnp.float32) + jnp.dot(
            picked[1], right[0], preferred_element_type=jnp.float32
        )
        return jnp.stack([real, imag])

    per_node = lax.map(one_node, (pick_table, jnp.moveaxis(placed, 1, 0)))
    partial_value = jnp.transpose(per_node, (1, 2, 0, 3))
    row_table = (col_struct[:, None, :] == target[None, :, None]).astype(jnp.bfloat16)
    z_rows = jnp.einsum("kts,ckswb->cktwb", row_table, placed, preferred_element_type=jnp.float32)
    z_rows = z_rows.astype(jnp.bfloat16).reshape(2, total_k, rows_all, block_width)
    summed = lax.psum_scatter(
        partial_value.reshape(2, rows_all, total_k * block_width),
        "pcol",
        scatter_dimension=2,
        tiled=True,
    )
    own_struct = lax.dynamic_slice_in_dim(structure, col_here * own_k, own_k, 0)
    member = jnp.any(own_struct[:, :, None] == target[None, None, :], axis=1)
    selected = -summed.reshape(2, row_blocks, block_width, own_k, block_width)
    selected = jnp.where(member.T[None, :, None, :, None], selected, 0.0)
    sel_inv = selected.reshape(2, rows_all, own_k * block_width)
    received = lax.all_to_all(z_rows, "pcol", split_axis=1, concat_axis=1, tiled=True)
    z_own = (
        received.astype(jnp.float32).reshape(2, n_cols, own_k, rows_all, block_width).sum(axis=1)
    )
    quad_term = complex_quad(z_own, selected.reshape(2, rows_all, own_k, block_width))
    total_sum = lax.psum(quad_term, "prow")
    diag_inv = k_inv - total_sum
    return (sel_inv, diag_inv)


def solution(mesh):
    placed = (
        P(None, ("pole", "prow"), "pcol"),
        P(None, "pole", ("pcol", "prow"), None),
        P(None, "pole", None, None),
        P(None, ("pole", "pcol"), None, None),
        P(),
    )
    return jax.shard_map(
        local,
        mesh=mesh,
        in_specs=placed,
        out_specs=(P(None, ("pole", "prow"), "pcol"), P(None, ("pole", "pcol"), None, None)),
        check_vma=False,
    )
```

```python
import functools

import jax
import jax.numpy as jnp
from jax import lax
from jax.experimental import pallas as pl
from jax.experimental.pallas import tpu as pltpu
from jax.sharding import PartitionSpec as P

BF16 = jnp.bfloat16
F32 = jnp.float32
LANES = 128
scope = jax.named_scope


def cdot(left, right, dims=(((1,), (0,)), ((), ()))):
    def single(x, y):
        return lax.dot_general(x, y, dims, preferred_element_type=F32)

    real = single(left[0], right[0]) - single(left[1], right[1])
    imag = single(left[0], right[1]) + single(left[1], right[0])
    return real, imag


def remote(src, dst, send_sem, recv_sem, where):
    return pltpu.make_async_remote_copy(
        src_ref=src,
        dst_ref=dst,
        send_sem=send_sem,
        recv_sem=recv_sem,
        device_id=where,
        device_id_type=pl.DeviceIdType.MESH,
    )


def swap(x):
    return pltpu.roll(x, x.shape[1] // 2, 1)


def low_lanes():
    return lax.broadcasted_iota(jnp.int32, (1, LANES), 1) < LANES // 2


def tiles_of(x):
    return [x[:, at : at + LANES] for at in range(0, x.shape[1], LANES)]


def join(left, right):
    sign = jnp.where(low_lanes(), -1.0, 1.0)
    return jnp.concatenate([a + swap(b) * sign for a, b in zip(tiles_of(left), tiles_of(right))], axis=1)


def cross(a, b):
    low = low_lanes()
    return jnp.where(low, a, swap(b)), jnp.where(low, swap(a), b)


def kernel(
    n_rows, n_cols, spans, a_hbm, panel_hbm, u_hbm, k_hbm, table_hbm, sel_out, diag_out,
    table, av, pv, uv, pr, pick_out, picks, acc, kv, z_t,
    gather_0, gather_1, gather_2, own_0, own_1, own_2, out_0, out_1, out_2,
    in_0, in_1, in_2, tot_0, tot_1, tot_2, some,
    d_send, t_recv,
):
    gather, own = (gather_0, gather_1, gather_2), (own_0, own_1, own_2)
    q_out, q_in, tot = (out_0, out_1, out_2), (in_0, in_1, in_2), (tot_0, tot_1, tot_2)
    groups = range(len(spans))
    row = lax.axis_index("prow")
    col = lax.axis_index("pcol")
    width = u_hbm.shape[-1]
    pairs = n_cols // 2
    row_blocks = a_hbm.shape[1] // width
    col_blocks = a_hbm.shape[2] // width
    band_rows = LANES // 2
    share = q_in[0].shape[1]
    first = n_rows // 2 - 1
    mate = row + 1 - 2 * (row % 2)
    is_end = (row == 0) | (row == n_rows - 1)
    is_inner = jnp.logical_not(is_end)
    end = jnp.where(is_end, row, mate)
    inner = jnp.where(is_end, mate, row)
    over = n_rows - 1 - inner
    far = n_rows - 1 - end

    def peer(unit):
        return ((col // 2 + unit // 2) % pairs) * 2 + (col + unit) % 2

    def unit_of(slot):
        return ((slot // 2 - col // 2 + pairs) % pairs) * 2 + (slot + col) % 2

    def arrived(view, sem):
        remote(view, view, sem, sem, {"prow": mate}).wait_recv()

    def drain(view, sem):
        remote(view, view, sem, sem, {"prow": mate}).wait_send()

    def pieces(group):
        cuts = 1 if group else 2
        rows = band_rows // cuts
        return [(part, slice(cut * rows, (cut + 1) * rows)) for part in range(share) for cut in range(cuts)]

    last = len(spans) - 1
    slots = sum(len(pieces(group)) for group in groups)

    def slot_of(group, piece):
        before = sum(len(pieces(other)) for other in range(group))
        return before + pieces(group).index(piece)

    def total_copy(group, piece, there):
        part, rows = piece
        block = tot[group].at[(row - first) * share + part, rows]
        return remote(block, block, d_send.at[0], t_recv.at[group * 2 + row - first], {"prow": there})

    where_tile = {tile: group for group in groups for tile in range(*spans[group])}

    def tile_of(tile, band):
        group = where_tile[tile]
        at = (tile - spans[group][0]) * LANES
        return tot[group][band, :, at : at + LANES].astype(F32)

    def finish(pair, owner):
        columns = slice(pair * LANES, (pair + 1) * LANES)
        for part in range(share):
            band = owner * share + part
            rows = pl.ds(pl.multiple_of(band * band_rows, band_rows), band_rows)
            planes = cross(tile_of(2 * pair, band), tile_of(2 * pair + 1, band))
            for plane in range(2):
                diag_out[plane, 0, rows, columns] = kv[plane, 0, rows, columns] + planes[plane]

    dma = pltpu.SemaphoreType.DMA

    def put_sel():
        named = jnp.full((1, LANES), table[col, row]) - row * row_blocks
        for pair in range(width // LANES):
            at = 2 * pair * LANES
            planes = cross(acc[0, :, at : at + LANES], acc[0, :, at + LANES : at + 2 * LANES])
            columns = slice(pair * LANES, (pair + 1) * LANES)
            for i in range(row_blocks):
                keep = -(named == i).astype(F32)
                for plane in range(2):
                    sel_out[plane, i * width : (i + 1) * width, columns] = planes[plane] * keep

    def adding(q_recv):
        def gathering(local_sem, p_send, p_recv, a_send, a_recv, g_send, g_recv):
            copy_p = pltpu.make_async_copy(panel_hbm, pv, local_sem.at[0])
            copy_u = pltpu.make_async_copy(u_hbm.at[:, col], uv, local_sem.at[1])
            copy_t = pltpu.make_async_copy(table_hbm, table, local_sem.at[2])
            copy_a = pltpu.make_async_copy(a_hbm, av, local_sem.at[3])
            copy_k = pltpu.make_async_copy(k_hbm, kv, local_sem.at[2])
            copy_p.start()
            copy_u.start()
            copy_t.start()
            copy_a.start()

            barrier = pltpu.get_barrier_semaphore()

            def greet(axis, there):
                pl.semaphore_signal(barrier, inc=1, device_id={axis: there}, device_id_type=pl.DeviceIdType.MESH)

            for unit in range(1, n_cols):
                greet("pcol", peer(unit))
            greet("prow", mate)
            greet("prow", jnp.where(is_end, over, far))

            @pl.when(is_inner)
            def _():
                greet("prow", over)

            def panel_copy(unit, source):
                return remote(
                    pv.at[:, peer(unit)], pr.at[source], p_send.at[0], p_recv.at[unit - 1], {"pcol": peer(unit)}
                )

            def pick_copy(unit, source):
                return remote(
                    pick_out.at[unit - 1], picks.at[source], a_send.at[0], a_recv.at[unit - 1], {"pcol": peer(unit)}
                )

            def base(group):
                return (group + 1) * n_cols if group else 0

            all_mate = 4 * n_cols

            def chunk_copy(group, unit, chunk, index, there):
                block = gather[group].at[unit, chunk]
                return remote(block, block, g_send.at[0], g_recv.at[index], {"prow": there})

            def scale(unit):
                slot = peer(unit)
                if unit == 0:
                    left = (pv[0, col], pv[1, col])
                else:
                    panel_copy(unit, slot).wait_recv()
                    left = (pr[slot, 0], pr[slot, 1])
                real, imag = cdot(left, (uv[0], uv[1]))
                live = (jnp.full((1, width), table[col, slot]) >= 0).astype(F32)
                packed = []
                for a, b in zip(tiles_of(real * live), tiles_of(imag * live)):
                    packed.extend(cross(a, b))
                for group in groups:
                    lo, hi = spans[group]
                    for tile in range(lo, hi):
                        at = (tile - lo) * LANES
                        gather[group][unit, row, :, at : at + LANES] = packed[tile].astype(BF16)

            def send_over(group, unit):
                index = base(group) + unit if group else unit + jnp.where(is_end, n_cols, 0)
                chunk_copy(group, unit, row, index, over).start()

            def send_mate(group, unit):
                chunk_copy(group, unit, row, jnp.where(is_end, all_mate, base(group) + unit), mate).start()

            def pick(unit):
                node = peer(unit)
                top = jnp.full((1, width), table[node, row]) - row * row_blocks
                side = jnp.full((1, width), table[node, col]) - col * col_blocks
                for plane in range(2):
                    total = None
                    for i in range(row_blocks):
                        for j in range(col_blocks):
                            keep = ((top == i) & (side == j)).astype(F32).astype(BF16)
                            block = av[plane, i * width : (i + 1) * width, j * width : (j + 1) * width] * keep
                            total = block if total is None else total + block
                    if unit == 0:
                        picks[col, plane] = total
                    else:
                        pick_out[unit - 1, plane] = total

            def meet():
                with scope("barrier"):
                    pl.semaphore_wait(barrier, n_cols + 2 - is_end.astype(jnp.int32))
                for unit in range(1, n_cols):
                    panel_copy(unit, col).start()

            with scope("copy_p"):
                copy_p.wait()

            @pl.when(is_end)
            def _():
                meet()

            with scope("copies"):
                copy_u.wait()
                copy_t.wait()
            copy_k.start()
            with scope("scale0"):
                scale(0)

            @pl.when(is_inner)
            def _():
                meet()

            send_over(0, 0)
            send_mate(0, 0)
            with scope("scale1"):
                scale(1)
            send_over(0, 1)
            send_mate(0, 1)
            far_home = unit_of(far)
            early = jnp.where(far_home < 2, far_home, 0)
            for group in groups[1:]:
                send_over(group, early)

            @pl.when(is_end)
            def _():
                for group in groups[1:]:
                    send_mate(group, early)

            @pl.when(is_inner)
            def _():
                for unit in range(2):
                    for group in groups[1:]:
                        send_mate(group, unit)

            with scope("copy_a"):
                copy_a.wait()
            for unit in list(range(2, n_cols)) + [1]:
                with scope(f"pick{unit}"):
                    pick(unit)
                pick_copy(unit, col).start()
            pick(0)
            late = range(2, n_cols)
            order = [(group, 0) for group in groups[1:]] + [(group, i) for group in groups[1:] for i in range(1, n_cols)]

            def relay(unit, chunk, index):
                arrived(gather[0].at[unit, chunk], g_recv.at[index])
                chunk_copy(0, unit, chunk, unit, end).start()

            def relay_both(group, unit):
                index = base(group) + unit
                arrived(gather[group].at[unit, 0:2], g_recv.at[index])
                chunk_copy(group, unit, over, index, end).start()
                chunk_copy(group, unit, far, index, end).start()

            @pl.when(is_end)
            def _():
                for unit in late:
                    with scope(f"scale{unit}"):
                        scale(unit)
                    send_over(0, unit)
                    send_mate(0, unit)
                for group, i in order:
                    unit = (far_home + i) % n_cols

                    @pl.when(unit != early)
                    def _():
                        send_over(group, unit)
                        send_mate(group, unit)

            @pl.when(is_inner)
            def _():
                with scope("relay_0o"):
                    relay(0, over, 0)
                with scope("scale2"):
                    scale(2)
                send_over(0, 2)
                send_mate(0, 2)
                with scope("relay_1o"):
                    relay(1, over, 1)
                with scope("scale3"):
                    scale(3)
                send_over(0, 3)
                send_mate(0, 3)
                with scope("relay_01f"):
                    relay(0, far, n_cols)
                    relay(1, far, n_cols + 1)
                for group, i in order:
                    unit = (far_home + i) % n_cols

                    @pl.when(unit != early)
                    def _():
                        send_over(group, unit)

                home = unit_of(end)

                @pl.when(home >= 2)
                def _():
                    for group in groups[1:]:
                        send_mate(group, home)

                for unit in late:
                    with scope(f"relay_{unit}o"):
                        relay(unit, over, unit)
                    with scope(f"relay_{unit}f"):
                        relay(unit, far, n_cols + unit)
                for group, i in order:
                    if i == 1:
                        for unit in late:

                            @pl.when(unit != home)
                            def _():
                                send_mate(group, unit)

                    with scope(f"relay_g{group}_{i}"):
                        relay_both(group, (home + i) % n_cols)
                with scope("mate"):
                    arrived(picks.at[0], g_recv.at[all_mate])

            def ready(group, unit):
                @pl.when(is_end)
                def _():
                    arrived(gather[group].at[unit, 0 : n_rows - 1], g_recv.at[base(group) + unit])

            def span(group):
                lo, hi = spans[group]
                return slice(lo * LANES, hi * LANES)

            def multiply(group, unit, start):
                right = gather[group][unit].reshape(width, gather[group].shape[-1])
                slot = peer(unit)
                for plane in range(2):
                    value = jnp.dot(picks[slot, plane], right, preferred_element_type=F32)
                    if start:
                        acc[plane, :, span(group)] = value
                    else:
                        acc[plane, :, span(group)] += value

            home = unit_of(row)
            named = jnp.full((1, LANES), table[col, row]) - row * row_blocks

            def quad_copy(group, there, piece):
                part, rows = piece
                at = part if there is over else share + part
                slot = slot_of(group, piece)
                if group == last and there is over:
                    slot = jnp.where(is_end, slots + part, slot)
                return remote(
                    q_out[group].at[at, rows], q_in[group].at[row, part, rows],
                    d_send.at[0], q_recv.at[slot], {"prow": there},
                )

            def quad(group, unit):
                right = gather[group][unit].reshape(width, gather[group].shape[-1])
                slot = peer(unit)
                sums = [
                    acc[plane, :, span(group)] + jnp.dot(picks[slot, plane], right, preferred_element_type=F32)
                    for plane in range(2)
                ]
                value = join(*sums)
                product = jnp.dot(z_t[...].reshape(2 * width, width), value.astype(BF16), preferred_element_type=F32)
                turns = [(piece, half) for piece in pieces(group) for half in range(2)]
                if group == last:
                    turns = [(piece, half) for piece in pieces(group) for half in (1, 0)]
                for piece, half in turns:
                    part, rows = piece
                    at = (half * share + part) * LANES
                    upper = product[at + rows.start : at + rows.stop]
                    lower = product[at + band_rows + rows.start : at + band_rows + rows.stop]
                    block = join(upper, lower)
                    q_out[group][half * share + part, rows] = block.astype(BF16)
                    if half:
                        own[group][part, rows] = block
                    if half:

                        @pl.when(is_end)
                        def _():
                            quad_copy(group, mate, piece).start()

                    else:
                        quad_copy(group, over, piece).start()

                acc[0, :, span(group)] = value

            for unit in range(n_cols):
                with scope(f"ready_g0_{unit}"):
                    ready(0, unit)
                if unit == n_cols - 1:
                    with scope("ready_home"):
                        for group in groups[1:]:
                            ready(group, home)
                    for group in groups:
                        turned = gather[group][home].reshape(width, gather[group].shape[-1]).T
                        for tile in range(*spans[group]):
                            at = (tile - spans[group][0]) * LANES
                            to = (tile % share) * LANES
                            part = jnp.where(over - first == tile // share, 0, 1)
                            z_t[part, to : to + LANES, :] = turned[at : at + LANES]
                with scope(f"wpick_{unit}"):
                    if unit > 0:
                        pick_copy(unit, peer(unit)).wait_recv()
                if unit < n_cols - 1:
                    multiply(0, unit, unit == 0)
            with scope("quad0"):
                quad(0, n_cols - 1)
            for group in groups[1:]:
                for i in range(n_cols):
                    unit = (home + i) % n_cols
                    if i > 0:
                        with scope(f"ready_g{group}_{i}"):
                            ready(group, unit)
                    if i < n_cols - 1:
                        multiply(group, unit, i == 0)
                with scope(f"quad{group}"):
                    quad(group, unit)

            @pl.when(is_end)
            def _():
                put_sel()

            copy_k.wait()
            drain(pr.at[0 : n_cols - 1], p_send.at[0])
            drain(pick_out, a_send.at[0])

            @pl.when(is_inner)
            def _():
                drain(picks, g_send.at[0])

            @pl.when(is_end)
            def _():
                drain(picks.at[0:2], g_send.at[0])
                drain(picks.at[0], d_send.at[0])

        pl.run_scoped(
            gathering, dma((4,)), dma((1,)), dma((n_cols - 1,)), dma((1,)), dma((n_cols - 1,)), dma((1,)), dma((4 * n_cols + 1,))
        )

        @pl.when(is_inner)
        def _():
            for group in groups[:last]:
                for piece in pieces(group):
                    part, rows = piece
                    with scope(f"wq{slot_of(group, piece)}"):
                        arrived(q_in[group].at[0 : n_rows - 1, part, rows], q_recv.at[slot_of(group, piece)])
                    total = own[group][part, rows]
                    for source in (over, end, far):
                        total = total + q_in[group][source, part, rows].astype(F32)
                    tot[group][(row - first) * share + part, rows] = total.astype(BF16)
                    total_copy(group, piece, far).start()
                    total_copy(group, piece, end).start()
            for piece in pieces(last):
                part, rows = piece
                slot = slot_of(last, piece)
                with scope(f"wq{slot}"):
                    arrived(q_in[last].at[0:2, part, rows], q_recv.at[slot])
                total = own[last][part] + q_in[last][over, part].astype(F32) + q_in[last][end, part].astype(F32)
                some[part] = total.astype(BF16)
                band = (row - first) * share + part
                remote(
                    some.at[part], tot[last].at[band], d_send.at[0], t_recv.at[2 * last + row - first], {"prow": far}
                ).start()
            for piece in pieces(last):
                part, rows = piece
                with scope(f"wf{part}"):
                    arrived(q_in[last].at[0, part, rows], q_recv.at[slots + part])
                total = some[part].astype(F32) + q_in[last][far, part].astype(F32)
                tot[last][(row - first) * share + part] = total.astype(BF16)
                total_copy(last, piece, end).start()
            for group in groups:
                for part in range(share):
                    total_copy(group, (part, slice(0, band_rows)), over).start()
            put_sel()
            for pair in range(width // LANES):
                finish(pair, row - first)

    pl.run_scoped(adding, dma((5 * share,)))

    def total_wait(group, owner):
        arrived(tot[group].at[0:share], t_recv.at[group * 2 + owner])

    @pl.when(is_end)
    def _():
        for group in groups:
            for there in (inner, over):
                with scope(f"wt{group}"):
                    total_wait(group, there - first)
                if group == last and there is over:
                    for part in range(share):
                        band = (over - first) * share + part
                        total = tot[last][band].astype(F32) + q_out[last][part].astype(F32)
                        tot[last][band] = total.astype(BF16)
                if group != 1:
                    finish(1 if group else 0, there - first)

    @pl.when(is_inner)
    def _():
        for group in groups:
            with scope(f"wt{group}"):
                total_wait(group, over - first)
        for pair in range(width // LANES):
            finish(pair, over - first)
        drain(picks.at[0:2], d_send.at[0])


def place(sel, diag, sel_out, diag_out, out_sem):
    copies = [
        pltpu.make_async_copy(sel, sel_out, out_sem.at[0]),
        pltpu.make_async_copy(diag, diag_out, out_sem.at[1]),
    ]
    for copy in copies:
        copy.start()
    for copy in copies:
        copy.wait()


def compact(ainv_anc, panel, u_inv, k_inv, structure):
    n_rows, n_cols = lax.axis_size("prow"), lax.axis_size("pcol")
    width, part = u_inv.shape[-1], panel.shape[2]
    row_blocks = ainv_anc.shape[1] // width
    tiles = 2 * width // LANES
    share = tiles // 2
    spans = ((0, share), (share, share + share // 2), (share + share // 2, tiles))
    hbm = pl.BlockSpec(memory_space=pltpu.HBM)
    vmem = pl.BlockSpec(memory_space=pltpu.VMEM)
    dma = pltpu.SemaphoreType.DMA
    shapes = (
        jax.ShapeDtypeStruct((2, row_blocks * width, width), F32),
        jax.ShapeDtypeStruct(k_inv.shape, F32),
    )

    def per_group(lead, rows, kind):
        return [pltpu.VMEM(lead + (rows, (hi - lo) * LANES), kind) for lo, hi in spans]

    band_rows = LANES // 2
    results = pl.pallas_call(
        functools.partial(kernel, n_rows, n_cols, spans),
        out_shape=tuple(pltpu.VMEM(s.shape, s.dtype) for s in shapes),
        in_specs=[hbm, hbm, hbm, hbm, hbm],
        out_specs=(vmem, vmem),
        scratch_shapes=[
            pltpu.SMEM(structure.shape, jnp.int32),
            pltpu.VMEM(ainv_anc.shape, BF16),
            pltpu.VMEM(panel.shape, BF16),
            pltpu.VMEM((2, width, width), BF16),
            pltpu.VMEM((n_cols, 2, part, width), BF16),
            pltpu.VMEM((n_cols - 1, 2, width, width), BF16),
            pltpu.VMEM((n_cols, 2, width, width), BF16),
            pltpu.VMEM((2, width, 2 * width), F32),
            pltpu.VMEM(k_inv.shape, F32),
            pltpu.VMEM((2, width, width), BF16),
            *per_group((n_cols, n_rows), part, BF16),
            *per_group((share,), band_rows, F32),
            *per_group((tiles,), band_rows, BF16),
            *per_group((n_rows, share), band_rows, BF16),
            *per_group((tiles,), band_rows, BF16),
            pltpu.VMEM((share, band_rows, LANES), BF16),
            dma((1,)),
            dma((6,)),
        ],
        compiler_params=pltpu.CompilerParams(
            collective_id=0, has_side_effects=True
        ),
    )(ainv_anc, panel, u_inv, k_inv, structure)
    return pl.pallas_call(
        place,
        out_shape=shapes,
        in_specs=[vmem, vmem],
        out_specs=(hbm, hbm),
        scratch_shapes=[dma((2,))],
    )(*[pltpu.with_memory_space_constraint(x, pltpu.VMEM) for x in results])


def complex_quad(z_part, s_part):
    highest = lax.Precision.HIGHEST

    def single(left, right):
        return jnp.einsum("kra,rkb->kab", left, right, precision=highest)

    real = single(z_part[0], s_part[0]) - single(z_part[1], s_part[1])
    imag = single(z_part[0], s_part[1]) + single(z_part[1], s_part[0])
    return jnp.stack([real, imag])


def local(ainv_anc, panel, u_inv, k_inv, structure):
    block_width = u_inv.shape[-1]
    cols = lax.axis_size("pcol")
    if (
        structure.shape[1] == cols
        and lax.axis_size("prow") == cols
        and ainv_anc.shape[1] == ainv_anc.shape[2]
        and u_inv.shape[1] == cols
        and cols // 2 == 2
        and cols % 2 == 0
        and block_width == 2 * LANES
    ):
        return compact(ainv_anc, panel, u_inv, k_inv, structure)
    total_k = u_inv.shape[1]
    own_k = k_inv.shape[1]
    n_cols = lax.axis_size("pcol")
    row_here = lax.axis_index("prow")
    col_here = lax.axis_index("pcol")
    row_blocks = ainv_anc.shape[1] // block_width
    group_blocks = ainv_anc.shape[2] // block_width
    group_slots = structure.shape[1] // n_cols
    rows_all = row_blocks * block_width
    col_struct = lax.dynamic_slice_in_dim(structure, col_here * group_slots, group_slots, 1)
    slot_live = col_struct >= 0
    slot_pos = col_struct - col_here * group_blocks
    first_block = row_here * row_blocks
    target = first_block + jnp.arange(row_blocks, dtype=jnp.int32)
    rows_in = lax.all_gather(panel, "prow", axis=2, tiled=True)

    def single(left, right):
        return jnp.einsum("knb,kbc->knc", left, right, preferred_element_type=jnp.float32)

    real = single(rows_in[0], u_inv[0]) - single(rows_in[1], u_inv[1])
    imag = single(rows_in[0], u_inv[1]) + single(rows_in[1], u_inv[0])
    placed = jnp.stack([real, imag]).astype(jnp.bfloat16)
    placed = placed.reshape(2, total_k, group_slots, block_width, block_width)
    placed = jnp.where(slot_live[None, :, :, None, None], placed, jnp.zeros((), jnp.bfloat16))
    block_ids = jnp.arange(group_blocks, dtype=jnp.int32)
    pick_table = (slot_pos[:, :, None] == block_ids[None, None, :]).astype(jnp.bfloat16)
    ainv_blocks = ainv_anc.reshape(2, rows_all, group_blocks, block_width)

    def one_node(items):
        table_k, rows_k = items
        picked = jnp.einsum(
            "sg,cigw->cisw", table_k, ainv_blocks, preferred_element_type=jnp.float32
        )
        picked = picked.astype(jnp.bfloat16).reshape(2, rows_all, group_slots * block_width)
        right = rows_k.reshape(2, group_slots * block_width, block_width)
        real = jnp.dot(picked[0], right[0], preferred_element_type=jnp.float32) - jnp.dot(
            picked[1], right[1], preferred_element_type=jnp.float32
        )
        imag = jnp.dot(picked[0], right[1], preferred_element_type=jnp.float32) + jnp.dot(
            picked[1], right[0], preferred_element_type=jnp.float32
        )
        return jnp.stack([real, imag])

    per_node = lax.map(one_node, (pick_table, jnp.moveaxis(placed, 1, 0)))
    partial_value = jnp.transpose(per_node, (1, 2, 0, 3))
    row_table = (col_struct[:, None, :] == target[None, :, None]).astype(jnp.bfloat16)
    z_rows = jnp.einsum("kts,ckswb->cktwb", row_table, placed, preferred_element_type=jnp.float32)
    z_rows = z_rows.astype(jnp.bfloat16).reshape(2, total_k, rows_all, block_width)
    summed = lax.psum_scatter(
        partial_value.reshape(2, rows_all, total_k * block_width),
        "pcol",
        scatter_dimension=2,
        tiled=True,
    )
    own_struct = lax.dynamic_slice_in_dim(structure, col_here * own_k, own_k, 0)
    member = jnp.any(own_struct[:, :, None] == target[None, None, :], axis=1)
    selected = -summed.reshape(2, row_blocks, block_width, own_k, block_width)
    selected = jnp.where(member.T[None, :, None, :, None], selected, 0.0)
    sel_inv = selected.reshape(2, rows_all, own_k * block_width)
    received = lax.all_to_all(z_rows, "pcol", split_axis=1, concat_axis=1, tiled=True)
    z_own = (
        received.astype(jnp.float32).reshape(2, n_cols, own_k, rows_all, block_width).sum(axis=1)
    )
    quad_term = complex_quad(z_own, selected.reshape(2, rows_all, own_k, block_width))
    total_sum = lax.psum(quad_term, "prow")
    diag_inv = k_inv - total_sum
    return (sel_inv, diag_inv)


def solution(mesh):
    placed = (
        P(None, ("pole", "prow"), "pcol"),
        P(None, "pole", ("pcol", "prow"), None),
        P(None, "pole", None, None),
        P(None, ("pole", "pcol"), None, None),
        P(),
    )
    return jax.shard_map(
        local,
        mesh=mesh,
        in_specs=placed,
        out_specs=(P(None, ("pole", "prow"), "pcol"), P(None, ("pole", "pcol"), None, None)),
        check_vma=False,
    )
```
